128 devices in a mesh: days: 8 (over x, y_hi), assets: 16 (over z, y_lo, core).
Axes of the slice: x: 4, y: 4 (y_hi: 2, y_lo: 2; y = y_hi * 2 + y_lo), z: 4, core: 2. Of those that a mesh axis runs over, the one named last changes fastest.
Arguments:
- factors: bfloat16 [1536, 256], P('days'), may hold values from -6 to 6
- returns: bfloat16 [1536, 16384], P('days', 'assets'), may hold values from -6 to 6
Outputs:
- loadings: float32 [256, 16384], P(None, 'assets')
- covariance: float32 [16384, 16384], P('assets', 'days')
The draws below stay inside these ranges and needn't reach their ends.
All inputs are finite; a program needn't handle non-finite values.
Results may differ from the reference program's by a relative error of at most 0.0036.
Values may be sent and summed in bfloat16 or wider, within the bound.
A program may use at most 64 MiB of HBM per device.

```python
import jax
import jax.numpy as jnp
from jax import lax

K = 256
ASSETS = 16384
DAYS = 1536


def block_scale(rng, dims, cuts, least, high):
    level, own = 1.0, jax.random.fold_in(rng, 6)
    for axis_at, shards_of in cuts:
        draws = jnp.exp(jax.random.uniform(jax.random.fold_in(own, axis_at), (shards_of,), jnp.float32, least / len(cuts), high / len(cuts)))
        level = level * jnp.repeat(draws, dims[axis_at] // shards_of).reshape([-1 if axis == axis_at else 1 for axis in range(len(dims))])
    return level


def centred(stream_key, dims, scale, limit, pieces=(), kind=jnp.bfloat16):
    entries = jax.random.normal(stream_key, dims, jnp.float32) * scale
    if len(pieces) > 0:
        entries = block_scale(stream_key, dims, pieces, -0.22, 0.18) * entries
    return jnp.clip(entries, min=-limit, max=limit).astype(kind)


def setup_inputs(seed: int = 0) -> dict:
    key_of = jax.random.split(jax.random.key(seed), 3)
    factors = centred(key_of[0], (DAYS, K), 1.0, 6.0, ((0, 8),))
    returns = centred(key_of[1], (DAYS, ASSETS), 1.0, 6.0, ((0, 8), (1, 16)))
    return dict(factors=factors, returns=returns)


def reference(factors, returns):
    gram = lax.dot_general(factors.astype(jnp.float32), factors.astype(jnp.float32), (((0,), (0,)), ((), ())), preferred_element_type=jnp.float32)
    cross = lax.dot_general(factors.astype(jnp.float32), returns.astype(jnp.float32), (((0,), (0,)), ((), ())), preferred_element_type=jnp.float32)
    lower = jnp.linalg.cholesky(gram)
    middle = lax.linalg.triangular_solve(lower, cross, left_side=True, lower=True)
    loadings = lax.linalg.triangular_solve(lower, middle, left_side=True, lower=True, transpose_a=True)
    fitted = jnp.dot(factors.astype(jnp.float32), loadings.astype(jnp.bfloat16).astype(jnp.float32), preferred_element_type=jnp.float32)
    residual = (returns.astype(jnp.float32) - fitted).astype(jnp.bfloat16)

    def block_rows(start):
        rows = lax.dynamic_slice_in_dim(residual, start, 1024, 1)
        return lax.dot_general(rows.astype(jnp.float32), residual.astype(jnp.float32), (((0,), (0,)), ((), ())), preferred_element_type=jnp.float32)
    width = residual.shape[1]
    step = min(1024, width)
    if step == 1024:
        starts = jnp.arange(0, width, 1024).astype(jnp.int32)
        covariance = lax.map(block_rows, starts).reshape(width, width)
    else:
        covariance = lax.dot_general(residual.astype(jnp.float32), residual.astype(jnp.float32), (((0,), (0,)), ((), ())), preferred_element_type=jnp.float32)
    covariance = covariance / residual.shape[0]
    return (loadings, covariance)
```

```python
import functools

import jax
import jax.numpy as jnp
from jax import lax
from jax.experimental import pallas as pl
from jax.experimental.pallas import tpu as pltpu
from jax.sharding import PartitionSpec as P

MESH = pl.DeviceIdType.MESH
DAY_BLOCK = 192
ASSET_BLOCK = 1024
PART = 64
HALF = 96

TREES = (
    (("z+", ((0, 0), (0, 1), (0, 2), (1, 2))), ("y", ((0, 1), (0, 2))), ("z-", ((1, 1),))),
    (("z-", ((0, 0), (0, 3), (0, 2), (1, 3), (1, 2))), ("y", ((0, 3),)), ("z+", ((1, 3),))),
    (("y", ((0, 0), (1, 1), (1, 2), (1, 3))), ("z+", ((1, 0), (1, 1))), ("z-", ((1, 0),))),
)


def events():
    mine = {}
    for dx in (1, -1):
        for p in range(3):
            mine[dx, 0, p] = 5.0 + 2.7 * p
            mine[dx, 1, p] = 17.0 + 2.8 * p
    for p in range(3):
        mine[0, 1, p] = 5.5 + 3.5 * p
        mine[2, 0, p] = (14.0, 17.0, 14.1)[p]
        mine[2, 1, p] = (27.0, 26.0, 27.1)[p]
    order = [(t, "mine", key) for key, t in mine.items()]
    mine.update({(0, 0, p): 0.0 for p in range(3)})
    order += [(t + 7.0, "cols", key) for key, t in mine.items()]
    return sorted(order)


def gather_kernel(f_hbm, x_hbm, mine, cols, fall, load_sem, f_send, f_recv, f_pair, m_send, m_recv,
                  c_send, c_recv, c_pair, fp_send, cp_send):
    day, asset = lax.axis_index("days"), lax.axis_index("assets")
    x, h = day // 2, day % 2
    z, l, c = asset // 4, (asset // 2) % 2, asset % 2
    dl, dz = (l + h) % 2, (z - x + 4) % 4
    is_root = jnp.logical_and(dl == 0, dz == 0)

    def day_of(dx, dh):
        return lax.rem(x + dx + 4, 4) * 2 + lax.rem(h + dh, 2)

    def asset_of(link):
        if link == "z+":
            return lax.rem(z + 1, 4) * 4 + l * 2 + c
        if link == "z-":
            return lax.rem(z + 3, 4) * 4 + l * 2 + c
        return z * 4 + (1 - l) * 2 + c

    sibling = z * 4 + l * 2 + 1 - c

    load_x = pltpu.make_async_copy(
        x_hbm, mine.at[pl.ds(pl.multiple_of(day * DAY_BLOCK, DAY_BLOCK), DAY_BLOCK)], load_sem.at[0])
    load_f = pltpu.make_async_copy(
        f_hbm, fall.at[pl.ds(pl.multiple_of(day * DAY_BLOCK, DAY_BLOCK), DAY_BLOCK)], load_sem.at[1])
    load_f.start()
    load_x.start()

    barrier = pltpu.get_barrier_semaphore()
    greeted = [(day_of(dx, dh), asset) for dx in (0, 1, -1) for dh in (0, 1) if (dx, dh) != (0, 0) and (dh == 0 or dx == 0)]
    greeted += [(day, asset_of("z+")), (day, asset_of("z-")), (day, asset_of("y")), (day, sibling)]
    for d, a in greeted:
        pl.semaphore_signal(barrier, inc=1, device_id={"days": d, "assets": a}, device_id_type=MESH)
    pl.semaphore_wait(barrier, len(greeted))
    load_f.wait()
    load_x.wait()

    pending = []

    def send(src, dst, ssem, rsem, d, a, when=None):
        copy = pltpu.make_async_remote_copy(
            src_ref=src, dst_ref=dst, send_sem=ssem, recv_sem=rsem,
            device_id={"days": d, "assets": a}, device_id_type=MESH)
        if when is None:
            copy.start()
        else:
            pl.when(when)(copy.start)
        pending.append((when, copy))

    def arrived(ref, rsem, when=None):
        copy = pltpu.make_async_remote_copy(
            src_ref=ref, dst_ref=ref, send_sem=load_sem.at[0], recv_sem=rsem,
            device_id={"days": day, "assets": sibling}, device_id_type=MESH)
        if when is None:
            copy.wait_recv()
        else:
            pl.when(when)(copy.wait_recv)

    def f_rows(dx, dh, core):
        return fall.at[pl.ds(pl.multiple_of(day_of(dx, dh) * DAY_BLOCK + core * HALF, 32), HALF)]

    def part_rows(dx, dh, p):
        return pl.ds(pl.multiple_of(day_of(dx, dh) * DAY_BLOCK + p * PART, PART), PART)

    def m_part(dx, dh, p):
        return mine.at[part_rows(dx, dh, p)]

    def c_part(dx, dh, p, core):
        return cols.at[part_rows(dx, dh, p), pl.ds(pl.multiple_of(core * ASSET_BLOCK, ASSET_BLOCK), ASSET_BLOCK)]

    n_f, n_m, n_c = [0], [0], [0]

    def send_f(dx, dh, to):
        ref = f_rows(dx, dh, c)
        send(ref, ref, f_send.at[n_f[0]], f_recv.at[day_of(dx, dh)], day_of(*to), asset)
        n_f[0] += 1

    def send_m(dx, dh, p, to):
        ref = m_part(dx, dh, p)
        send(ref, ref, m_send.at[n_m[0]], m_recv.at[day_of(dx, dh), p], day_of(*to), asset)
        n_m[0] += 1

    def pair_f(dx, dh):
        ref = f_rows(dx, dh, c)
        arrived(ref, f_recv.at[day_of(dx, dh)])
        send(ref, ref, fp_send.at[day_of(dx, dh)], f_pair.at[day_of(dx, dh)], day, sibling)

    def root_sends(dx, dh, p):
        link = TREES[p][0][0]
        src, dst = m_part(dx, dh, p), c_part(dx, dh, p, c)
        send(src, dst, c_send.at[n_c[0]], c_recv.at[day_of(dx, dh), p], day, asset_of(link), is_root)
        n_c[0] += 1
        send(src, dst, cp_send.at[day_of(dx, dh), p], c_pair.at[day_of(dx, dh), p], day, sibling, is_root)

    def cols_relay(dx, dh, p):
        ref = c_part(dx, dh, p, c)
        other = jnp.logical_not(is_root)
        arrived(ref, c_recv.at[day_of(dx, dh), p], other)
        for link, roles in TREES[p]:
            roles = [role for role in roles if role != (0, 0)]
            if not roles:
                continue
            here = functools.reduce(jnp.logical_or, [jnp.logical_and(dl == i, dz == j) for i, j in roles])
            send(ref, ref, c_send.at[n_c[0]], c_recv.at[day_of(dx, dh), p], day, asset_of(link), here)
            n_c[0] += 1
        send(ref, ref, cp_send.at[day_of(dx, dh), p], c_pair.at[day_of(dx, dh), p], day, sibling, other)

    send_f(0, 0, (0, 1))
    send_f(0, 0, (1, 0))
    send_f(0, 0, (-1, 0))
    for p in range(3):
        send_m(0, 0, p, (0, 1))
        if p == 0:
            send_m(0, 0, p, (1, 0))
            send_m(0, 0, p, (-1, 0))
        root_sends(0, 0, p)
    pair_f(0, 1)
    send_f(0, 1, (1, 0))
    send_f(0, 1, (-1, 0))
    pair_f(1, 0)
    pair_f(-1, 0)
    send_f(-1, 0, (1, 0))
    for p in (1, 2):
        send_m(0, 0, p, (1, 0))
        send_m(0, 0, p, (-1, 0))
    pair_f(1, 1)
    send_f(1, 1, (-1, 0))
    pair_f(-1, 1)
    pair_f(2, 0)
    pair_f(2, 1)

    for _, kind, (dx, dh, p) in events():
        if kind == "mine":
            arrived(m_part(dx, dh, p), m_recv.at[day_of(dx, dh), p])
            if (dx, dh) == (0, 1):
                send_m(dx, dh, p, (1, 0))
                send_m(dx, dh, p, (-1, 0))
            if (dx, dh, p) in ((-1, 0, 0), (-1, 0, 1), (-1, 1, 0)):
                send_m(dx, dh, p, (1, 0))
            if (dx, dh, p) in ((1, 0, 2), (1, 1, 1), (1, 1, 2)):
                send_m(dx, dh, p, (-1, 0))
            root_sends(dx, dh, p)
        else:
            cols_relay(dx, dh, p)

    @pl.when(is_root)
    def _():
        @pl.loop(0, 8 * DAY_BLOCK // PART)
        def _(i):
            rows = pl.ds(pl.multiple_of(i * PART, PART), PART)
            cols[rows, pl.ds(pl.multiple_of(c * ASSET_BLOCK, ASSET_BLOCK), ASSET_BLOCK)] = mine[rows, :]

    keys = [(dx, dh) for dx in (0, 1, -1, 2) for dh in (0, 1)]
    for dx, dh in keys:
        if (dx, dh) != (0, 0):
            arrived(f_rows(dx, dh, 1 - c), f_pair.at[day_of(dx, dh)])
        for p in range(3):
            arrived(c_part(dx, dh, p, 1 - c), c_pair.at[day_of(dx, dh), p])
    for when, copy in pending:
        if when is None:
            copy.wait_send()
        else:
            pl.when(when)(copy.wait_send)


def gather(factors, returns):
    dma = pltpu.SemaphoreType.DMA
    days = 8 * DAY_BLOCK
    return pl.pallas_call(
        gather_kernel,
        out_shape=(
            jax.ShapeDtypeStruct((days, ASSET_BLOCK), jnp.bfloat16),
            jax.ShapeDtypeStruct((days, 2 * ASSET_BLOCK), jnp.bfloat16),
            jax.ShapeDtypeStruct((days, factors.shape[1]), jnp.bfloat16),
        ),
        in_specs=[pl.BlockSpec(memory_space=pl.ANY)] * 2,
        out_specs=(pl.BlockSpec(memory_space=pltpu.VMEM),) * 3,
        scratch_shapes=[
            dma((2,)), dma((7,)), dma((8,)), dma((8,)), dma((21,)), dma((8, 3)),
            dma((12 * 8,)), dma((8, 3)), dma((8, 3)), dma((8,)), dma((8, 3)),
        ],
        compiler_params=pltpu.CompilerParams(collective_id=0, has_side_effects=True),
    )(factors, returns)


def per_device(factors, returns):
    mine, columns, factors = gather(factors, returns)
    gram = lax.dot_general(
        factors, factors, (((0,), (0,)), ((), ())), preferred_element_type=jnp.float32
    )
    both = jnp.concatenate((mine, columns), axis=1)
    cross = lax.dot_general(
        factors, both, (((0,), (0,)), ((), ())), preferred_element_type=jnp.float32
    )
    lower = jnp.linalg.cholesky(gram)
    middle = lax.linalg.triangular_solve(lower, cross, left_side=True, lower=True)
    loadings = lax.linalg.triangular_solve(
        lower, middle, left_side=True, lower=True, transpose_a=True
    )
    fitted = jnp.dot(factors, loadings.astype(jnp.bfloat16), preferred_element_type=jnp.float32)
    residual = (both.astype(jnp.float32) - fitted).astype(jnp.bfloat16)
    covariance = lax.dot_general(
        residual[:, :ASSET_BLOCK], residual[:, ASSET_BLOCK:], (((0,), (0,)), ((), ())),
        preferred_element_type=jnp.float32
    )
    covariance = covariance / mine.shape[0]
    return (loadings[:, :ASSET_BLOCK], covariance)


def solution(mesh):
    in_specs = (P("days", None), P("days", "assets"))
    out_specs = (P(None, "assets"), P("assets", "days"))
    return jax.shard_map(
        per_device, mesh=mesh, in_specs=in_specs, out_specs=out_specs, check_vma=False
    )
```

```python
import functools

import jax
import jax.numpy as jnp
from jax import lax
from jax.experimental import pallas as pl
from jax.experimental.pallas import tpu as pltpu
from jax.sharding import PartitionSpec as P

MESH = pl.DeviceIdType.MESH
DAY_BLOCK = 192
DAYS = 8 * DAY_BLOCK
ASSET_BLOCK = 1024
FACTORS = 256
HALF = 96
PARTS = 3
PART = DAY_BLOCK // PARTS
PIVOTS = 4
TILE = 256

TREES = (
    (("z+", ((0, 0), (0, 1), (0, 2), (1, 2))), ("y", ((0, 1), (0, 2))), ("z-", ((1, 1),))),
    (("z-", ((0, 0), (0, 3), (0, 2), (1, 3), (1, 2))), ("y", ((0, 3),)), ("z+", ((1, 3),))),
    (("y", ((0, 0), (1, 1), (1, 2), (1, 3))), ("z+", ((1, 0), (1, 1))), ("z-", ((1, 0),))),
)
DEPTHS = (
    (((0, 1),), ((0, 2), (1, 1)), ((0, 3), (1, 2), (1, 0)), ((1, 3),)),
    (((0, 3),), ((0, 2), (1, 3)), ((0, 1), (1, 2), (1, 0)), ((1, 1),)),
    (((1, 0),), ((1, 1), (1, 3)), ((0, 1), (1, 2), (0, 3)), ((0, 2),)),
)
CHUNKS = ((0, 0), (0, 1), (1, 0), (1, 1), (-1, 0), (-1, 1), (2, 0), (2, 1))

LINKS = ("h", "x+", "x-", "root")
ORDER = (
    (0, 2, 2), (0, 2, 0), (0, 1, 1), (0, 0, 1), (0, 0, 0), (0, 3, 1), (0, 2, 1), (0, 1, 2),
    (0, 1, 0), (0, 3, 2), (2, 0, 2, 1), (2, 0, 0, 1), (2, 4, 1, 1), (0, 3, 0), (1, 4, 1), (2, 2, 0, 1),
    (1, 2, 0), (2, 0, 1, 1), (0, 0, 2), (1, 2, 2), (1, 4, 0), (1, 1, 1), (2, 2, 2, 1), (2, 4, 1, 2),
    (1, 1, 0), (2, 6, 1, 1), (2, 0, 1, 2), (2, 0, 2, 2), (1, 6, 1), (2, 0, 0, 2), (1, 3, 1), (2, 4, 2, 1),
    (1, 2, 1), (1, 6, 0), (2, 2, 0, 2), (1, 4, 2), (1, 1, 2), (2, 2, 2, 2), (2, 2, 1, 1), (1, 6, 2),
    (2, 6, 1, 2), (1, 3, 0), (2, 3, 1, 1), (2, 1, 2, 1), (2, 6, 0, 2), (2, 4, 1, 3), (2, 6, 0, 1), (2, 0, 0, 3),
    (1, 5, 0), (2, 6, 2, 1), (2, 2, 1, 2), (2, 0, 2, 3), (2, 4, 0, 1), (2, 4, 2, 2), (2, 4, 0, 2), (2, 3, 1, 2),
    (2, 1, 0, 2), (2, 1, 2, 2), (2, 4, 1, 4), (1, 5, 1), (2, 6, 1, 3), (1, 3, 2), (2, 7, 1, 1), (2, 7, 1, 2),
    (2, 1, 0, 1), (2, 5, 0, 2), (2, 5, 1, 1), (2, 6, 0, 3), (2, 3, 2, 2), (2, 6, 2, 2), (2, 0, 1, 3), (2, 1, 1, 1),
    (2, 5, 0, 1), (2, 3, 2, 1), (2, 5, 2, 2), (2, 5, 2, 1), (2, 2, 2, 3), (2, 3, 0, 1), (2, 4, 0, 3), (1, 5, 2),
    (2, 7, 0, 1), (2, 7, 2, 1), (2, 3, 0, 2), (2, 5, 1, 2), (2, 1, 2, 4), (2, 4, 2, 3), (2, 7, 2, 2), (2, 2, 1, 3),
    (2, 7, 0, 2), (2, 3, 1, 3), (2, 1, 2, 3), (2, 4, 2, 4), (2, 1, 0, 3), (2, 7, 1, 3), (2, 1, 1, 2), (2, 0, 1, 4),
    (2, 6, 2, 4), (2, 2, 0, 3), (2, 6, 1, 4), (2, 3, 2, 3), (2, 4, 0, 4), (2, 3, 0, 4), (2, 5, 1, 4), (2, 0, 2, 4),
    (2, 5, 0, 3), (2, 6, 2, 3), (2, 7, 2, 4), (2, 3, 0, 3), (2, 5, 1, 3), (1, 7, 1), (2, 2, 2, 4), (2, 7, 1, 4),
    (2, 5, 2, 4), (2, 1, 0, 4), (1, 7, 2), (2, 5, 2, 3), (2, 7, 0, 3), (1, 7, 0), (2, 3, 1, 4), (2, 1, 1, 3),
    (2, 2, 0, 4), (2, 7, 0, 4), (2, 0, 0, 4), (2, 1, 1, 4), (2, 7, 2, 3), (2, 6, 0, 4), (2, 3, 2, 4), (2, 5, 0, 4),
    (2, 2, 1, 4),
)


def forward_right(dh, p):
    return p < (PARTS + 1 - dh) // 2


def invert(a):
    n = a.shape[0]
    lane = lax.broadcasted_iota(jnp.int32, (n, n), 1)
    lane_one = lax.broadcasted_iota(jnp.int32, (1, n), 1)
    sub = lax.broadcasted_iota(jnp.int32, (8, n), 0)
    for k in range(n):
        row, col = a[k:k + 1, :], a[:, k:k + 1]
        scale = 1.0 / a[k:k + 1, k:k + 1]
        scaled = jnp.where(lane_one == k, scale, row * scale)
        a = jnp.where(lane == k, 0.0, a) - col * scaled
        g = k // 8 * 8
        middle = jnp.where(sub == k - g, jnp.broadcast_to(scaled, (8, n)), a[g:g + 8])
        a = jnp.concatenate([part for part in (a[:g], middle, a[g + 8:]) if part.shape[0]], axis=0)
        if k % PIVOTS == PIVOTS - 1:
            yield None
    yield a


def exact_dot(a, b):
    return jnp.dot(a, b, precision=lax.Precision.HIGHEST, preferred_element_type=jnp.float32)


def inverse_of_gram(fall, fall_t, gram, inverse):
    fall_t[...] = fall[...].T
    yield
    gram[...] = jnp.dot(fall_t[...], fall[...], preferred_element_type=jnp.float32)
    yield
    n = FACTORS // 2
    first = None
    for first in invert(gram[:n, :n]):
        yield
    upper, lower = gram[:n, n:], gram[n:, :n]
    right, left = exact_dot(first, upper), exact_dot(lower, first)
    schur = gram[n:, n:] - exact_dot(lower, right)
    yield
    second = None
    for second in invert(schur):
        yield
    off = -exact_dot(right, second)
    inverse[:n, :n] = first - exact_dot(off, left)
    inverse[:n, n:] = off
    inverse[n:, :n] = -exact_dot(second, left)
    inverse[n:, n:] = second
    yield


def gather_kernel(f_hbm, x_hbm, mine, cols, fall, fall_t, inverse, gram, load_sem, f_send, f_recv, f_pair,
                  m_send, m_recv, c_send, c_recv, c_pair, fp_send, cp_send):
    day, asset = lax.axis_index("days"), lax.axis_index("assets")
    x, h = day // 2, day % 2
    z, l, c = asset // 4, (asset // 2) % 2, asset % 2
    dl, dz = (l + h) % 2, (z - x + 4) % 4
    is_root = jnp.logical_and(dl == 0, dz == 0)

    def among(roles):
        return functools.reduce(jnp.logical_or, [jnp.logical_and(dl == i, dz == j) for i, j in roles])

    def day_of(dx, dh):
        return lax.rem(x + dx + 4, 4) * 2 + lax.rem(h + dh, 2)

    def asset_of(link):
        if link == "z+":
            return lax.rem(z + 1, 4) * 4 + l * 2 + c
        if link == "z-":
            return lax.rem(z + 3, 4) * 4 + l * 2 + c
        return z * 4 + (1 - l) * 2 + c

    sibling = z * 4 + l * 2 + 1 - c
    own_rows = pl.ds(pl.multiple_of(day * DAY_BLOCK, DAY_BLOCK), DAY_BLOCK)
    load_x = pltpu.make_async_copy(x_hbm, mine.at[own_rows], load_sem.at[0])
    load_f = pltpu.make_async_copy(f_hbm, fall.at[own_rows], load_sem.at[1])
    load_f.start()
    load_x.start()

    barrier = pltpu.get_barrier_semaphore()
    greeted = [(day_of(0, 1), asset), (day_of(1, 0), asset), (day_of(-1, 0), asset)]
    greeted += [(day, asset_of("z+")), (day, asset_of("z-")), (day, asset_of("y")), (day, sibling)]
    for d, a in greeted:
        pl.semaphore_signal(barrier, inc=1, device_id={"days": d, "assets": a}, device_id_type=MESH)
    pl.semaphore_wait(barrier, len(greeted))
    load_f.wait()
    load_x.wait()

    pending = []

    def send(src, dst, ssem, rsem, d, a, when=None):
        copy = pltpu.make_async_remote_copy(
            src_ref=src, dst_ref=dst, send_sem=ssem, recv_sem=rsem,
            device_id={"days": d, "assets": a}, device_id_type=MESH)
        if when is None:
            copy.start()
        else:
            pl.when(when)(copy.start)
        pending.append((when, copy))

    def arrived(ref, rsem):
        pltpu.make_async_remote_copy(
            src_ref=ref, dst_ref=ref, send_sem=load_sem.at[0], recv_sem=rsem,
            device_id={"days": day, "assets": sibling}, device_id_type=MESH).wait_recv()

    def f_rows(dx, dh, core):
        return fall.at[pl.ds(pl.multiple_of(day_of(dx, dh) * DAY_BLOCK + core * HALF, 32), HALF)]

    def part_rows(dx, dh, p):
        return pl.ds(pl.multiple_of(day_of(dx, dh) * DAY_BLOCK + p * PART, PART), PART)

    def m_part(dx, dh, p):
        return mine.at[part_rows(dx, dh, p)]

    def c_part(dx, dh, p, core):
        return cols.at[part_rows(dx, dh, p), pl.ds(pl.multiple_of(core * ASSET_BLOCK, ASSET_BLOCK), ASSET_BLOCK)]

    n_f, n_m, n_c = [0], [0], [0]

    def send_f(dx, dh, to):
        ref = f_rows(dx, dh, c)
        send(ref, ref, f_send.at[n_f[0]], f_recv.at[day_of(dx, dh)], day_of(*to), asset)
        n_f[0] += 1

    def send_m(dx, dh, p, to):
        ref = m_part(dx, dh, p)
        send(ref, ref, m_send.at[n_m[0]], m_recv.at[day_of(dx, dh), p], day_of(*to), asset)
        n_m[0] += 1

    def pair_f(dx, dh):
        ref = f_rows(dx, dh, c)
        arrived(ref, f_recv.at[day_of(dx, dh)])
        send(ref, ref, fp_send.at[day_of(dx, dh)], f_pair.at[day_of(dx, dh)], day, sibling)

    def root_sends(dx, dh, p):
        link = TREES[p * 3 // PARTS][0][0]
        src, dst = m_part(dx, dh, p), c_part(dx, dh, p, c)
        send(src, dst, c_send.at[n_c[0]], c_recv.at[day_of(dx, dh), p], day, asset_of(link), is_root)
        n_c[0] += 1
        send(src, dst, cp_send.at[day_of(dx, dh), p], c_pair.at[day_of(dx, dh), p], day, sibling, is_root)

    def relay_mine(dx, dh, p):
        arrived(m_part(dx, dh, p), m_recv.at[day_of(dx, dh), p])
        if (dx, dh) == (0, 1):
            send_m(dx, dh, p, (1, 0))
            send_m(dx, dh, p, (-1, 0))
        if dx == -1 and forward_right(dh, p):
            send_m(dx, dh, p, (1, 0))
        if dx == 1 and not forward_right(dh, p):
            send_m(dx, dh, p, (-1, 0))
        root_sends(dx, dh, p)

    def relay_cols(dx, dh, p, depth):
        ref = c_part(dx, dh, p, c)
        tree = p * 3 // PARTS
        here = DEPTHS[tree][depth - 1]
        pl.when(among(here))(lambda: arrived(ref, c_recv.at[day_of(dx, dh), p]))
        for link, roles in TREES[tree]:
            roles = [role for role in roles if role in here]
            if roles:
                send(ref, ref, c_send.at[n_c[0]], c_recv.at[day_of(dx, dh), p], day, asset_of(link), among(roles))
                n_c[0] += 1
        send(ref, ref, cp_send.at[day_of(dx, dh), p], c_pair.at[day_of(dx, dh), p], day, sibling, among(here))

    send_f(0, 0, (0, 1))
    send_f(0, 0, (1, 0))
    send_f(0, 0, (-1, 0))
    factor_steps = [
        lambda: (pair_f(0, 1), send_f(0, 1, (1, 0)), send_f(0, 1, (-1, 0))),
        lambda: (pair_f(1, 0), pair_f(-1, 0), send_f(-1, 0, (1, 0))),
        lambda: (pair_f(1, 1), send_f(1, 1, (-1, 0)), pair_f(-1, 1)),
        lambda: (pair_f(2, 0), pair_f(2, 1)),
        lambda: [arrived(f_rows(dx, dh, 1 - c), f_pair.at[day_of(dx, dh)]) for dx, dh in CHUNKS[1:]],
    ]
    solve = inverse_of_gram(fall, fall_t, gram, inverse)

    for i, (kind, a, p, *depth) in enumerate(ORDER):
        if kind == 0 and LINKS[a] == "root":
            root_sends(0, 0, p)
        elif kind == 0:
            send_m(0, 0, p, {"h": (0, 1), "x+": (1, 0), "x-": (-1, 0)}[LINKS[a]])
        elif kind == 1:
            relay_mine(*CHUNKS[a], p)
        else:
            relay_cols(*CHUNKS[a], p, *depth)
        if i in (10, 11, 12, 22, 23):
            factor_steps.pop(0)()
        if not factor_steps:
            for _ in range(1):
                next(solve, None)
    for step in factor_steps:
        step()
    for _ in solve:
        pass

    @pl.when(is_root)
    def _():
        @pl.loop(0, DAYS // 64)
        def _(i):
            rows = pl.ds(pl.multiple_of(i * 64, 64), 64)
            cols[rows, pl.ds(pl.multiple_of(c * ASSET_BLOCK, ASSET_BLOCK), ASSET_BLOCK)] = mine[rows, :]

    for dx, dh in CHUNKS:
        for p in range(PARTS):
            arrived(c_part(dx, dh, p, 1 - c), c_pair.at[day_of(dx, dh), p])
    for when, copy in pending:
        if when is None:
            copy.wait_send()
        else:
            pl.when(when)(copy.wait_send)


def gather(factors, returns):
    dma = pltpu.SemaphoreType.DMA
    return pl.pallas_call(
        gather_kernel,
        out_shape=(
            jax.ShapeDtypeStruct((DAYS, ASSET_BLOCK), jnp.bfloat16),
            jax.ShapeDtypeStruct((DAYS, 2 * ASSET_BLOCK), jnp.bfloat16),
            jax.ShapeDtypeStruct((DAYS, FACTORS), jnp.bfloat16),
            jax.ShapeDtypeStruct((FACTORS, DAYS), jnp.bfloat16),
            jax.ShapeDtypeStruct((FACTORS, FACTORS), jnp.float32),
        ),
        in_specs=[pl.BlockSpec(memory_space=pltpu.HBM)] * 2,
        out_specs=(pl.BlockSpec(memory_space=pltpu.VMEM),) * 5,
        scratch_shapes=[
            pltpu.VMEM((FACTORS, FACTORS), jnp.float32),
            dma((2,)), dma((7,)), dma((8,)), dma((8,)), dma((7 * PARTS,)), dma((8, PARTS)),
            dma((8 * PARTS * 7,)), dma((8, PARTS)), dma((8, PARTS)), dma((8,)), dma((8, PARTS)),
        ],
        compiler_params=pltpu.CompilerParams(
            collective_id=0, has_side_effects=True, vmem_limit_bytes=32 * 2**20),
        name="gather",
    )(factors, returns)


def covariance_kernel(mine, cols, fall, fall_t, inverse, loadings, covariance, mine_t):
    def residual_of(block):
        cross = jnp.dot(fall_t[...], block, preferred_element_type=jnp.float32)
        exposure = exact_dot(inverse[...], cross)
        fitted = jnp.dot(fall[...], exposure.astype(jnp.bfloat16), preferred_element_type=jnp.float32)
        return exposure, (block.astype(jnp.float32) - fitted).astype(jnp.bfloat16)

    @pl.when(pl.program_id(0) == 0)
    def _():
        @pl.loop(0, ASSET_BLOCK // TILE)
        def _(i):
            part = pl.ds(pl.multiple_of(i * TILE, TILE), TILE)
            exposure, residual = residual_of(mine[:, part])
            loadings[:, part] = exposure
            mine_t[part, :] = residual.T

    _, residual = residual_of(cols[...])
    covariance[...] = jnp.dot(mine_t[...], residual, preferred_element_type=jnp.float32) * (1.0 / DAYS)


def covariances(mine, cols, fall, fall_t, inverse):
    def whole(a):
        return pl.BlockSpec(a.shape, lambda i: (0, 0), pipeline_mode=pl.Buffered(1))

    return pl.pallas_call(
        covariance_kernel,
        out_shape=(
            jax.ShapeDtypeStruct((FACTORS, ASSET_BLOCK), jnp.float32),
            jax.ShapeDtypeStruct((ASSET_BLOCK, 2 * ASSET_BLOCK), jnp.float32),
        ),
        grid=(2 * ASSET_BLOCK // TILE,),
        in_specs=[whole(mine), pl.BlockSpec((DAYS, TILE), lambda i: (0, i)), whole(fall), whole(fall_t), whole(inverse)],
        out_specs=(
            pl.BlockSpec((FACTORS, ASSET_BLOCK), lambda i: (0, 0)),
            pl.BlockSpec((ASSET_BLOCK, TILE), lambda i: (0, i)),
        ),
        scratch_shapes=[pltpu.VMEM((ASSET_BLOCK, DAYS), jnp.bfloat16)],
        compiler_params=pltpu.CompilerParams(
            dimension_semantics=("arbitrary",), vmem_limit_bytes=32 * 2**20),
        name="covariances",
    )(mine, cols, fall, fall_t, inverse)


def per_device(factors, returns):
    factors = pltpu.with_memory_space_constraint(factors, pltpu.HBM)
    returns = pltpu.with_memory_space_constraint(returns, pltpu.HBM)
    return covariances(*gather(factors, returns))


def solution(mesh):
    in_specs = (P("days", None), P("days", "assets"))
    out_specs = (P(None, "assets"), P("assets", "days"))
    return jax.shard_map(
        per_device, mesh=mesh, in_specs=in_specs, out_specs=out_specs, check_vma=False
    )
```

```python
import functools
import itertools

import jax
import jax.numpy as jnp
from jax import lax
from jax.experimental import pallas as pl
from jax.experimental.pallas import tpu as pltpu
from jax.sharding import PartitionSpec as P

MESH = pl.DeviceIdType.MESH
DAY_BLOCK = 192
DAYS = 8 * DAY_BLOCK
ASSET_BLOCK = 1024
FACTORS = 256
HALF = 96
THIRDS, SIDES = 3, 2
PARTS = THIRDS * SIDES
PART = DAY_BLOCK // THIRDS
SIDE = ASSET_BLOCK // SIDES
PIVOTS = 8

TREES = (
    (("z+", ((0, 0), (0, 1), (0, 2), (1, 2))), ("y", ((0, 1), (0, 2))), ("z-", ((1, 1),))),
    (("z-", ((0, 0), (0, 3), (0, 2), (1, 3), (1, 2))), ("y", ((0, 3),)), ("z+", ((1, 3),))),
    (("y", ((0, 0), (1, 1), (1, 2), (1, 3))), ("z+", ((1, 0), (1, 1))), ("z-", ((1, 0),))),
)
DEPTHS = (
    (((0, 1),), ((0, 2), (1, 1)), ((0, 3), (1, 2), (1, 0)), ((1, 3),)),
    (((0, 3),), ((0, 2), (1, 3)), ((0, 1), (1, 2), (1, 0)), ((1, 1),)),
    (((1, 0),), ((1, 1), (1, 3)), ((0, 1), (1, 2), (0, 3)), ((0, 2),)),
)
CHUNKS = ((0, 0), (0, 1), (1, 0), (1, 1), (-1, 0), (-1, 1), (2, 0), (2, 1))

LINKS = ("h", "x+", "x-", "root")
ORDER = (
    (3, 0), (0, 1, 0), (0, 2, 0), (0, 3, 0), (0, 0, 0), (0, 1, 1), (0, 2, 1), (0, 3, 1),
    (0, 0, 1), (0, 1, 2), (0, 2, 2), (0, 3, 2), (0, 0, 2), (2, 0, 0, 1), (2, 0, 1, 1), (3, 1),
    (0, 1, 3), (0, 2, 3), (0, 3, 3), (0, 0, 3), (0, 1, 4), (0, 2, 4), (0, 3, 4), (0, 0, 4),
    (0, 1, 5), (0, 2, 5), (0, 3, 5), (0, 0, 5), (1, 2, 0), (1, 4, 0), (1, 2, 1), (1, 4, 1),
    (2, 0, 2, 1), (1, 2, 2), (1, 4, 2), (3, 2), (1, 1, 0), (2, 0, 0, 2), (2, 0, 1, 2), (2, 0, 3, 1),
    (2, 0, 4, 1), (1, 2, 3), (1, 4, 3), (1, 1, 1), (1, 1, 2), (2, 0, 2, 2), (2, 4, 0, 1), (2, 2, 0, 1),
    (2, 4, 1, 1), (1, 2, 4), (2, 2, 1, 1), (1, 4, 4), (2, 0, 5, 1), (1, 1, 3), (2, 0, 0, 3), (2, 1, 0, 1),
    (2, 0, 1, 3), (2, 0, 3, 2), (2, 1, 1, 1), (2, 0, 4, 2), (1, 2, 5), (1, 4, 5), (1, 1, 4), (2, 0, 2, 3),
    (1, 1, 5), (1, 6, 2), (1, 6, 0), (2, 4, 0, 2), (2, 4, 1, 2), (2, 0, 5, 2), (2, 4, 3, 1), (2, 2, 3, 1),
    (2, 4, 4, 1), (2, 2, 4, 1), (1, 3, 0), (1, 6, 1), (3, 3), (2, 0, 3, 3), (2, 0, 4, 3), (2, 0, 2, 4),
    (2, 2, 0, 2), (2, 2, 1, 2), (2, 1, 4, 1), (2, 0, 0, 4), (1, 3, 1), (2, 4, 2, 1), (2, 1, 0, 2), (2, 1, 1, 2),
    (1, 5, 0), (2, 6, 1, 1), (2, 0, 5, 3), (2, 0, 1, 4), (2, 4, 0, 3), (1, 3, 2), (2, 2, 2, 1), (2, 0, 3, 4),
    (2, 1, 3, 1), (2, 6, 0, 1), (2, 4, 1, 3), (2, 4, 3, 2), (2, 4, 4, 2), (1, 6, 3), (2, 3, 0, 1), (1, 3, 3),
    (2, 2, 0, 3), (2, 3, 1, 1), (2, 2, 1, 3), (2, 1, 2, 1), (2, 4, 2, 2), (2, 0, 4, 4), (2, 1, 0, 3), (1, 5, 1),
    (2, 1, 1, 3), (2, 2, 3, 2), (2, 4, 5, 1), (1, 6, 5), (2, 0, 5, 4), (2, 4, 0, 4), (2, 2, 4, 2), (2, 1, 3, 2),
    (2, 1, 4, 2), (1, 3, 4), (1, 5, 2), (2, 4, 3, 3), (2, 2, 5, 1), (2, 1, 5, 1), (2, 2, 2, 2), (2, 2, 0, 4),
    (1, 6, 4), (2, 6, 0, 2), (2, 6, 1, 2), (2, 4, 1, 4), (2, 1, 2, 2), (1, 3, 5), (2, 6, 2, 1), (2, 1, 0, 4),
    (2, 2, 3, 3), (1, 5, 3), (2, 3, 0, 2), (2, 3, 1, 2), (2, 2, 1, 4), (2, 1, 1, 4), (2, 4, 5, 2), (2, 4, 3, 4),
    (2, 2, 5, 2), (2, 1, 3, 3), (1, 7, 1), (3, 4), (4, 0), (2, 2, 3, 4), (4, 1), (2, 4, 4, 3),
    (2, 6, 0, 3), (4, 2), (2, 2, 4, 3), (2, 7, 1, 1), (2, 5, 1, 1), (2, 3, 4, 1), (4, 3), (2, 1, 4, 3),
    (4, 4), (2, 4, 2, 3), (4, 5), (2, 2, 2, 3), (4, 6), (2, 1, 2, 3), (4, 7), (4, 8),
    (4, 9), (2, 4, 2, 4), (4, 10), (4, 11), (4, 12), (4, 13), (4, 14), (4, 15),
    (2, 1, 3, 4), (4, 16), (2, 6, 0, 4), (1, 7, 2), (1, 5, 4), (4, 17), (4, 18), (4, 19),
    (2, 3, 0, 3), (1, 7, 0), (1, 5, 5), (4, 20), (2, 6, 4, 1), (2, 1, 5, 2), (2, 7, 2, 1), (2, 3, 2, 1),
    (1, 7, 4), (4, 21), (2, 4, 5, 3), (2, 2, 5, 3), (2, 6, 2, 2), (1, 7, 3), (2, 6, 1, 3), (1, 7, 5),
    (2, 7, 1, 2), (2, 3, 1, 3), (2, 5, 1, 2), (2, 7, 0, 1), (2, 3, 4, 2), (2, 5, 0, 1), (2, 6, 3, 1), (4, 22),
    (2, 3, 3, 1), (4, 23), (2, 3, 0, 4), (2, 5, 2, 1), (2, 4, 4, 4), (4, 24), (2, 7, 3, 1), (2, 5, 3, 1),
    (2, 7, 2, 2), (4, 25), (2, 7, 1, 3), (2, 7, 0, 2), (4, 26), (2, 3, 2, 2), (2, 6, 4, 2), (2, 1, 5, 3),
    (4, 27), (2, 5, 0, 2), (2, 2, 2, 4), (2, 2, 4, 4), (2, 1, 2, 4), (4, 28), (2, 6, 2, 3), (2, 6, 3, 2),
    (4, 29), (2, 7, 0, 3), (2, 6, 5, 1), (2, 5, 1, 3), (2, 7, 2, 3), (2, 1, 4, 4), (2, 4, 5, 4), (4, 30),
    (2, 3, 4, 3), (2, 3, 3, 2), (2, 5, 0, 3), (2, 7, 5, 1), (4, 31), (2, 6, 1, 4), (2, 2, 5, 4), (2, 5, 2, 2),
    (2, 5, 4, 1), (4, 32), (2, 6, 3, 3), (2, 3, 5, 1), (2, 7, 4, 1), (4, 33), (2, 7, 3, 2), (2, 7, 0, 4),
    (2, 3, 2, 3), (4, 34), (2, 3, 1, 4), (2, 1, 5, 4), (2, 7, 1, 4), (4, 35), (2, 5, 0, 4), (2, 6, 4, 3),
    (2, 3, 3, 3), (2, 5, 3, 2), (4, 36), (4, 37), (2, 6, 5, 2), (2, 5, 4, 2), (2, 5, 1, 4), (2, 7, 5, 2),
    (2, 6, 3, 4), (4, 38), (2, 3, 4, 4), (2, 5, 2, 3), (2, 6, 2, 4), (2, 5, 5, 1), (2, 7, 4, 2), (2, 7, 3, 3),
    (2, 3, 3, 4), (4, 39), (2, 6, 4, 4), (2, 7, 2, 4), (2, 5, 4, 3), (2, 3, 2, 4), (2, 6, 5, 3), (2, 5, 2, 4),
    (4, 40), (2, 7, 5, 3), (2, 7, 4, 3), (2, 5, 3, 3), (2, 3, 5, 2), (2, 5, 5, 2), (2, 7, 3, 4), (2, 5, 4, 4),
    (4, 41), (4, 42), (2, 6, 5, 4), (2, 3, 5, 3), (2, 5, 3, 4), (2, 7, 4, 4), (4, 43), (2, 7, 5, 4),
    (4, 44), (4, 45), (2, 3, 5, 4), (2, 5, 5, 3), (2, 5, 5, 4),
)


def forward_right(dh, p):
    return p % THIRDS < (THIRDS + 1 - dh) // 2


def invert(a):
    n = a.shape[0]
    lane = lax.broadcasted_iota(jnp.int32, (n, n), 1)
    lane_one = lax.broadcasted_iota(jnp.int32, (1, n), 1)
    sub = lax.broadcasted_iota(jnp.int32, (8, n), 0)
    for k in range(n):
        row, col = a[k:k + 1, :], a[:, k:k + 1]
        scale = 1.0 / a[k:k + 1, k:k + 1]
        scaled = jnp.where(lane_one == k, scale, row * scale)
        a = jnp.where(lane == k, 0.0, a) - col * scaled
        g = k // 8 * 8
        middle = jnp.where(sub == k - g, jnp.broadcast_to(scaled, (8, n)), a[g:g + 8])
        a = jnp.concatenate([part for part in (a[:g], middle, a[g + 8:]) if part.shape[0]], axis=0)
        if k % PIVOTS == PIVOTS - 1:
            yield None
    yield a


def exact_dot(a, b):
    return jnp.dot(a, b, precision=lax.Precision.HIGHEST, preferred_element_type=jnp.float32)


def inverse_of_gram(fall, fall_t, gram, inverse):
    fall_t[...] = fall[...].T
    yield
    gram[...] = jnp.dot(fall_t[...], fall[...], preferred_element_type=jnp.float32)
    yield
    n = FACTORS // 2
    first = None
    for first in invert(gram[:n, :n]):
        yield
    upper, lower = gram[:n, n:], gram[n:, :n]
    right, left = exact_dot(first, upper), exact_dot(lower, first)
    schur = gram[n:, n:] - exact_dot(lower, right)
    yield
    second = None
    for second in invert(schur):
        yield
    off = -exact_dot(right, second)
    inverse[:n, :n] = first - exact_dot(off, left)
    inverse[:n, n:] = off
    inverse[n:, :n] = -exact_dot(second, left)
    inverse[n:, n:] = second
    yield


def residual_of(block, fall, fall_t, inverse):
    cross = jnp.dot(fall_t[...], block, preferred_element_type=jnp.float32)
    exposure = exact_dot(inverse[...], cross)
    fitted = jnp.dot(fall[...], exposure.astype(jnp.bfloat16), preferred_element_type=jnp.float32)
    return exposure, (block.astype(jnp.float32) - fitted).astype(jnp.bfloat16)


def own_residuals(mine, fall, fall_t, inverse, loadings, mine_t):
    for side in range(SIDES):
        part = pl.ds(side * SIDE, SIDE)
        exposure, residual = residual_of(mine[:, part], fall, fall_t, inverse)
        loadings[:, part] = exposure
        mine_t[part, :] = residual.T
        yield


def early_columns(prepare, cols, fall, fall_t, inverse, mine_t, first_side, residuals):
    for core in range(2):
        if core == 0:
            prepare()
        part = pl.ds(core * ASSET_BLOCK, SIDE)
        residuals[core] = residual_of(cols[:, part], fall, fall_t, inverse)[1]
        yield
    for core in range(2):
        for block in range(2):
            rows = pl.ds(block * SIDE, SIDE)
            first_side[core, rows, :] = jnp.dot(
                mine_t[rows, :], residuals[core], preferred_element_type=jnp.float32) * (1.0 / DAYS)
            yield


def gather_kernel(f_hbm, x_hbm, cols, fall, fall_t, inverse, loadings, mine_t, first_side,
                  mine, residuals, gram, load_sem, f_send, f_recv, f_pair,
                  m_send, m_recv, c_send, c_recv, c_pair, fp_send, cp_send):
    day, asset = lax.axis_index("days"), lax.axis_index("assets")
    x, h = day // 2, day % 2
    z, l, c = asset // 4, (asset // 2) % 2, asset % 2
    dl, dz = (l + h) % 2, (z - x + 4) % 4
    is_root = jnp.logical_and(dl == 0, dz == 0)
    right_is_root = jnp.logical_and(dl == 0, dz == 1)
    left_is_root = jnp.logical_and(dl == 0, dz == 3)
    partner_is_root = jnp.logical_and(dl == 1, dz == 0)

    def among(roles):
        return functools.reduce(jnp.logical_or, [jnp.logical_and(dl == i, dz == j) for i, j in roles])

    def day_of(dx, dh):
        return lax.rem(x + dx + 4, 4) * 2 + lax.rem(h + dh, 2)

    def asset_of(link):
        if link == "z+":
            return lax.rem(z + 1, 4) * 4 + l * 2 + c
        if link == "z-":
            return lax.rem(z + 3, 4) * 4 + l * 2 + c
        return z * 4 + (1 - l) * 2 + c

    sibling = z * 4 + l * 2 + 1 - c
    own_rows = pl.ds(pl.multiple_of(day * DAY_BLOCK, DAY_BLOCK), DAY_BLOCK)
    load_x = pltpu.make_async_copy(x_hbm, mine.at[own_rows], load_sem.at[0])
    load_f = pltpu.make_async_copy(f_hbm, fall.at[own_rows], load_sem.at[1])
    load_f.start()
    load_x.start()

    barrier = pltpu.get_barrier_semaphore()
    greeted = [(day_of(0, 1), asset), (day_of(1, 0), asset), (day_of(-1, 0), asset)]
    greeted += [(day, asset_of("z+")), (day, asset_of("z-")), (day, asset_of("y")), (day, sibling)]
    for d, a in greeted:
        pl.semaphore_signal(barrier, inc=1, device_id={"days": d, "assets": a}, device_id_type=MESH)
    pl.semaphore_wait(barrier, len(greeted))
    load_f.wait()
    load_x.wait()

    pending = []

    def send(src, dst, ssem, rsem, d, a, when=None):
        copy = pltpu.make_async_remote_copy(
            src_ref=src, dst_ref=dst, send_sem=ssem, recv_sem=rsem,
            device_id={"days": d, "assets": a}, device_id_type=MESH)
        if when is None:
            copy.start()
        else:
            pl.when(when)(copy.start)
        pending.append((when, copy))

    def arrived(ref, rsem):
        pltpu.make_async_remote_copy(
            src_ref=ref, dst_ref=ref, send_sem=load_sem.at[0], recv_sem=rsem,
            device_id={"days": day, "assets": sibling}, device_id_type=MESH).wait_recv()

    def f_rows(dx, dh, core):
        return fall.at[pl.ds(pl.multiple_of(day_of(dx, dh) * DAY_BLOCK + core * HALF, 32), HALF)]

    def part_rows(dx, dh, p):
        return pl.ds(pl.multiple_of(day_of(dx, dh) * DAY_BLOCK + p % THIRDS * PART, PART), PART)

    def m_part(dx, dh, p):
        return mine.at[part_rows(dx, dh, p), pl.ds(p // THIRDS * SIDE, SIDE)]

    def c_part(dx, dh, p, core):
        lanes = pl.ds(pl.multiple_of(core * ASSET_BLOCK + p // THIRDS * SIDE, SIDE), SIDE)
        return cols.at[part_rows(dx, dh, p), lanes]

    n_f, n_m, n_c = [0], [0], [0]

    def send_f(dx, dh, to):
        ref = f_rows(dx, dh, c)
        send(ref, ref, f_send.at[n_f[0]], f_recv.at[day_of(dx, dh)], day_of(*to), asset)
        n_f[0] += 1

    def send_m(dx, dh, p, to, when=None):
        ref = m_part(dx, dh, p)
        send(ref, ref, m_send.at[n_m[0]], m_recv.at[day_of(dx, dh), p], day_of(*to), asset, when)
        n_m[0] += 1

    def pair_f(dx, dh):
        ref = f_rows(dx, dh, c)
        arrived(ref, f_recv.at[day_of(dx, dh)])
        send(ref, ref, fp_send.at[day_of(dx, dh)], f_pair.at[day_of(dx, dh)], day, sibling)

    def root_sends(dx, dh, p):
        link = TREES[p % THIRDS][0][0]
        src, dst = m_part(dx, dh, p), c_part(dx, dh, p, c)
        send(src, dst, c_send.at[n_c[0]], c_recv.at[day_of(dx, dh), p], day, asset_of(link), is_root)
        n_c[0] += 1
        send(src, dst, cp_send.at[day_of(dx, dh), p], c_pair.at[day_of(dx, dh), p], day, sibling, is_root)

    def relay_mine(dx, dh, p):
        arrived(m_part(dx, dh, p), m_recv.at[day_of(dx, dh), p])
        right, left = (None, None) if dh == 0 else (jnp.logical_not(right_is_root), jnp.logical_not(left_is_root))
        if (dx, dh) == (0, 1):
            send_m(dx, dh, p, (1, 0))
            send_m(dx, dh, p, (-1, 0))
        if dx == -1 and forward_right(dh, p):
            send_m(dx, dh, p, (1, 0), right)
        if dx == 1 and not forward_right(dh, p):
            send_m(dx, dh, p, (-1, 0), left)
        if (dx, dh) == (2, 0):
            send_m(dx, dh, p, (0, 1), partner_is_root)
        root_sends(dx, dh, p)

    def relay_cols(dx, dh, p, depth):
        ref = c_part(dx, dh, p, c)
        tree = p % THIRDS
        here = DEPTHS[tree][depth - 1]
        pl.when(among(here))(lambda: arrived(ref, c_recv.at[day_of(dx, dh), p]))
        for link, roles in TREES[tree]:
            roles = [role for role in roles if role in here]
            if roles:
                send(ref, ref, c_send.at[n_c[0]], c_recv.at[day_of(dx, dh), p], day, asset_of(link), among(roles))
                n_c[0] += 1
        send(ref, ref, cp_send.at[day_of(dx, dh), p], c_pair.at[day_of(dx, dh), p], day, sibling, among(here))

    def fill(side):
        @pl.when(is_root)
        def _():
            lanes = pl.ds(pl.multiple_of(c * ASSET_BLOCK + side * SIDE, SIDE), SIDE)

            @pl.loop(0, DAYS // 64)
            def _(i):
                rows = pl.ds(pl.multiple_of(i * 64, 64), 64)
                cols[rows, lanes] = mine[rows, pl.ds(side * SIDE, SIDE)]

        for dx, dh in CHUNKS:
            for p in range(side * THIRDS, (side + 1) * THIRDS):
                arrived(c_part(dx, dh, p, 1 - c), c_pair.at[day_of(dx, dh), p])

    factor_steps = iter((
        lambda: (send_f(0, 0, (0, 1)), send_f(0, 0, (1, 0)), send_f(0, 0, (-1, 0))),
        lambda: (pair_f(0, 1), send_f(0, 1, (1, 0)), send_f(0, 1, (-1, 0))),
        lambda: (pair_f(1, 0), pair_f(-1, 0), send_f(-1, 0, (1, 0))),
        lambda: (pair_f(1, 1), send_f(1, 1, (-1, 0)), pair_f(-1, 1)),
        lambda: (pair_f(2, 0), pair_f(2, 1),
                 [arrived(f_rows(dx, dh, 1 - c), f_pair.at[day_of(dx, dh)]) for dx, dh in CHUNKS[1:]]),
    ))
    compute = itertools.chain(
        inverse_of_gram(fall, fall_t, gram, inverse),
        own_residuals(mine, fall, fall_t, inverse, loadings, mine_t),
        early_columns(lambda: fill(0), cols, fall, fall_t, inverse, mine_t, first_side, residuals),
    )
    for kind, a, *rest in ORDER:
        if kind == 0 and LINKS[a] == "root":
            root_sends(0, 0, *rest)
        elif kind == 0:
            send_m(0, 0, *rest, {"h": (0, 1), "x+": (1, 0), "x-": (-1, 0)}[LINKS[a]])
        elif kind == 1:
            relay_mine(*CHUNKS[a], *rest)
        elif kind == 2:
            relay_cols(*CHUNKS[a], *rest)
        elif kind == 3:
            next(factor_steps)()
        else:
            next(compute)
    fill(1)
    for _ in compute:
        pass

    for when, copy in pending:
        if when is None:
            copy.wait_send()
        else:
            pl.when(when)(copy.wait_send)


def gather(factors, returns):
    dma = pltpu.SemaphoreType.DMA
    shape = jax.ShapeDtypeStruct
    return pl.pallas_call(
        gather_kernel,
        out_shape=(
            shape((DAYS, 2 * ASSET_BLOCK), jnp.bfloat16),
            shape((DAYS, FACTORS), jnp.bfloat16),
            shape((FACTORS, DAYS), jnp.bfloat16),
            shape((FACTORS, FACTORS), jnp.float32),
            shape((FACTORS, ASSET_BLOCK), jnp.float32),
            shape((ASSET_BLOCK, DAYS), jnp.bfloat16),
            shape((2, ASSET_BLOCK, SIDE), jnp.float32),
        ),
        in_specs=[pl.BlockSpec(memory_space=pl.ANY)] * 2,
        out_specs=(pl.BlockSpec(memory_space=pltpu.VMEM),) * 7,
        scratch_shapes=[
            pltpu.VMEM((DAYS, ASSET_BLOCK), jnp.bfloat16),
            pltpu.VMEM((2, DAYS, SIDE), jnp.bfloat16),
            pltpu.VMEM((FACTORS, FACTORS), jnp.float32),
            dma((2,)), dma((7,)), dma((8,)), dma((8,)), dma((10 * PARTS,)), dma((8, PARTS)),
            dma((8 * PARTS * 7,)), dma((8, PARTS)), dma((8, PARTS)), dma((8,)), dma((8, PARTS)),
        ],
        compiler_params=pltpu.CompilerParams(
            collective_id=0, has_side_effects=True, vmem_limit_bytes=36 * 2**20),
        name="gather",
    )(factors, returns)


def covariance_kernel(cols, fall, fall_t, inverse, loadings, mine_t, first_side, loadings_out, covariance, stage, sems):
    copies = [pltpu.make_async_copy(loadings, loadings_out, sems.at[0])]
    for core in range(2):
        lanes = pl.ds(core * ASSET_BLOCK, SIDE)
        copies.append(pltpu.make_async_copy(first_side.at[core], covariance.at[:, lanes], sems.at[1 + core]))
    for copy in copies:
        copy.start()
    for core in range(2):
        lanes = pl.ds(core * ASSET_BLOCK + SIDE, SIDE)
        _, residual = residual_of(cols[:, lanes], fall, fall_t, inverse)
        for block in range(2):
            rows = pl.ds(block * SIDE, SIDE)
            stage[core, rows, :] = jnp.dot(
                mine_t[rows, :], residual, preferred_element_type=jnp.float32) * (1.0 / DAYS)
            copy = pltpu.make_async_copy(
                stage.at[core, rows], covariance.at[rows, lanes], sems.at[3 + core * 2 + block])
            copy.start()
            copies.append(copy)
    for copy in copies:
        copy.wait()


def covariances(*args):
    return pl.pallas_call(
        covariance_kernel,
        out_shape=(
            jax.ShapeDtypeStruct((FACTORS, ASSET_BLOCK), jnp.float32),
            jax.ShapeDtypeStruct((ASSET_BLOCK, 2 * ASSET_BLOCK), jnp.float32),
        ),
        in_specs=[pl.BlockSpec(memory_space=pltpu.VMEM)] * len(args),
        out_specs=(pl.BlockSpec(memory_space=pltpu.HBM),) * 2,
        scratch_shapes=[pltpu.VMEM((2, ASSET_BLOCK, SIDE), jnp.float32), pltpu.SemaphoreType.DMA((7,))],
        compiler_params=pltpu.CompilerParams(vmem_limit_bytes=24 * 2**20),
        name="covariances",
    )(*args)


def per_device(factors, returns):
    factors = pltpu.with_memory_space_constraint(factors, pltpu.HBM)
    returns = pltpu.with_memory_space_constraint(returns, pltpu.HBM)
    return covariances(*gather(factors, returns))


def solution(mesh):
    in_specs = (P("days", None), P("days", "assets"))
    out_specs = (P(None, "assets"), P("assets", "days"))
    return jax.shard_map(
        per_device, mesh=mesh, in_specs=in_specs, out_specs=out_specs, check_vma=False
    )
```

```python
import functools
import itertools

import jax
import jax.numpy as jnp
from jax import lax
from jax.experimental import pallas as pl
from jax.experimental.pallas import tpu as pltpu
from jax.sharding import PartitionSpec as P

MESH = pl.DeviceIdType.MESH
DAY_BLOCK = 192
DAYS = 8 * DAY_BLOCK
ASSET_BLOCK = 1024
FACTORS = 256
HALF = 96
THIRDS, SIDES = 3, 2
PARTS = THIRDS * SIDES
PART = DAY_BLOCK // THIRDS
SIDE = ASSET_BLOCK // SIDES
PIVOTS = 8

TREES = (
    (("z+", ((0, 0), (0, 1), (0, 2), (1, 2))), ("y", ((0, 1), (0, 2))), ("z-", ((1, 1),))),
    (("z-", ((0, 0), (0, 3), (0, 2), (1, 3), (1, 2))), ("y", ((0, 3),)), ("z+", ((1, 3),))),
    (("y", ((0, 0), (1, 1), (1, 2), (1, 3))), ("z+", ((1, 0), (1, 1))), ("z-", ((1, 0),))),
)
DEPTHS = (
    (((0, 1),), ((0, 2), (1, 1)), ((0, 3), (1, 2), (1, 0)), ((1, 3),)),
    (((0, 3),), ((0, 2), (1, 3)), ((0, 1), (1, 2), (1, 0)), ((1, 1),)),
    (((1, 0),), ((1, 1), (1, 3)), ((0, 1), (1, 2), (0, 3)), ((0, 2),)),
)
CHUNKS = ((0, 0), (0, 1), (1, 0), (1, 1), (-1, 0), (-1, 1), (2, 0), (2, 1))

LINKS = ("h", "x+", "x-", "root")
ORDER = (
    (3, 0), (0, 2, 1), (0, 2, 2), (0, 1, 1), (0, 2, 0), (0, 0, 1), (0, 0, 0), (0, 1, 0),
    (0, 3, 3), (0, 2, 3), (0, 1, 3), (0, 1, 4), (0, 3, 5), (0, 3, 1), (0, 1, 2), (2, 0, 1, 1),
    (0, 3, 2), (0, 2, 4), (2, 0, 3, 1), (1, 4, 1), (0, 3, 0), (2, 0, 5, 1), (0, 0, 2), (3, 1),
    (0, 0, 4), (2, 0, 3, 2), (2, 4, 0, 1), (1, 2, 2), (1, 4, 0), (1, 1, 0), (1, 2, 1), (3, 2),
    (0, 1, 5), (2, 0, 1, 3), (2, 0, 1, 2), (0, 3, 4), (1, 4, 4), (2, 4, 1, 1), (1, 4, 3), (1, 4, 2),
    (0, 0, 3), (2, 4, 0, 2), (1, 1, 1), (0, 2, 5), (2, 2, 1, 2), (2, 0, 2, 1), (2, 4, 1, 2), (2, 4, 3, 1),
    (2, 2, 0, 1), (2, 2, 2, 1), (2, 0, 2, 2), (2, 2, 1, 1), (1, 2, 4), (2, 1, 0, 1), (2, 4, 2, 1), (1, 2, 0),
    (2, 0, 4, 1), (1, 2, 3), (3, 3), (2, 0, 0, 1), (2, 1, 1, 1), (1, 1, 2), (2, 4, 2, 2), (0, 0, 5),
    (1, 6, 1), (1, 5, 0), (1, 3, 1), (1, 1, 4), (2, 1, 2, 1), (2, 2, 1, 3), (1, 6, 0), (2, 6, 1, 1),
    (1, 2, 5), (1, 6, 2), (1, 1, 3), (1, 3, 0), (2, 2, 4, 1), (2, 1, 1, 2), (2, 2, 0, 2), (3, 4),
    (2, 2, 3, 1), (4, 0), (1, 3, 2), (2, 0, 0, 2), (2, 4, 3, 2), (2, 3, 1, 1), (2, 4, 4, 1), (2, 2, 2, 2),
    (2, 2, 5, 1), (2, 5, 0, 1), (2, 0, 4, 2), (2, 1, 2, 2), (1, 6, 4), (4, 1), (2, 4, 0, 3), (2, 1, 4, 1),
    (2, 4, 2, 3), (4, 2), (2, 6, 2, 1), (4, 3), (2, 4, 1, 3), (2, 0, 2, 3), (2, 6, 0, 1), (2, 4, 1, 4),
    (2, 0, 3, 3), (1, 1, 5), (2, 2, 4, 2), (2, 2, 3, 2), (2, 0, 5, 2), (2, 2, 5, 2), (4, 4), (2, 3, 1, 2),
    (1, 4, 5), (2, 5, 0, 2), (1, 6, 3), (4, 5), (4, 6), (2, 0, 4, 3), (2, 6, 4, 1), (2, 3, 2, 1),
    (2, 2, 1, 4), (1, 3, 4), (2, 6, 0, 2), (4, 7), (4, 8), (2, 4, 4, 2), (4, 9), (2, 1, 0, 2),
    (2, 3, 0, 1), (2, 6, 1, 2), (2, 3, 2, 2), (2, 3, 0, 2), (1, 7, 1), (1, 5, 2), (4, 10), (1, 3, 3),
    (1, 7, 0), (2, 6, 3, 1), (2, 6, 4, 2), (2, 2, 2, 3), (1, 5, 1), (4, 11), (2, 1, 3, 1), (2, 2, 4, 3),
    (2, 3, 4, 2), (2, 3, 4, 1), (2, 6, 2, 2), (4, 12), (2, 4, 5, 1), (2, 0, 0, 3), (2, 0, 0, 4), (2, 4, 3, 3),
    (2, 1, 2, 3), (1, 6, 5), (4, 13), (1, 7, 2), (2, 5, 2, 1), (2, 1, 5, 1), (4, 14), (4, 15),
    (2, 4, 2, 4), (4, 16), (2, 7, 1, 1), (2, 2, 0, 3), (1, 5, 3), (2, 5, 2, 2), (1, 5, 4), (4, 17),
    (4, 18), (4, 19), (4, 20), (2, 4, 5, 2), (2, 7, 0, 1), (4, 21), (2, 7, 0, 2), (4, 22),
    (2, 6, 0, 3), (2, 0, 3, 4), (2, 7, 2, 1), (2, 6, 5, 1), (2, 5, 1, 1), (2, 2, 2, 4), (2, 2, 5, 3), (2, 5, 1, 2),
    (2, 5, 3, 1), (2, 2, 3, 3), (2, 5, 0, 3), (1, 3, 5), (2, 7, 1, 2), (4, 23), (2, 1, 5, 2), (2, 7, 2, 2),
    (2, 1, 3, 2), (4, 24), (4, 25), (4, 26), (2, 0, 4, 4), (2, 3, 3, 2), (2, 5, 3, 2), (2, 3, 1, 3),
    (2, 5, 4, 1), (2, 6, 5, 2), (2, 3, 3, 1), (2, 4, 0, 4), (2, 3, 2, 3), (2, 3, 1, 4), (2, 3, 5, 1), (4, 27),
    (4, 28), (2, 1, 0, 3), (2, 0, 5, 3), (2, 6, 4, 3), (4, 29), (2, 1, 4, 2), (4, 30), (4, 31),
    (4, 32), (1, 7, 4), (4, 33), (1, 5, 5), (2, 3, 5, 2), (2, 1, 1, 3), (2, 2, 0, 4), (2, 2, 4, 4),
    (2, 5, 2, 3), (1, 7, 3), (4, 34), (2, 6, 1, 3), (2, 6, 3, 2), (2, 6, 2, 3), (2, 4, 4, 3), (4, 35),
    (2, 0, 2, 4), (2, 1, 1, 4), (2, 5, 5, 1), (2, 5, 4, 2), (2, 7, 4, 1), (4, 36), (2, 4, 5, 3), (4, 37),
    (2, 5, 5, 2), (2, 7, 0, 3), (2, 3, 0, 3), (1, 7, 5), (4, 38), (2, 1, 5, 3), (2, 3, 0, 4), (2, 4, 3, 4),
    (2, 7, 1, 3), (2, 7, 4, 2), (2, 7, 3, 1), (2, 0, 5, 4), (2, 7, 3, 2), (2, 6, 0, 4), (2, 1, 0, 4), (2, 7, 5, 1),
    (2, 5, 1, 3), (4, 39), (2, 5, 1, 4), (2, 6, 1, 4), (2, 1, 3, 3), (2, 5, 0, 4), (2, 5, 2, 4), (2, 2, 3, 4),
    (2, 4, 4, 4), (2, 0, 1, 4), (2, 7, 1, 4), (2, 7, 0, 4), (2, 2, 5, 4), (2, 3, 4, 3), (2, 7, 2, 3), (2, 6, 2, 4),
    (2, 3, 3, 3), (2, 1, 2, 4), (2, 7, 2, 4), (2, 7, 5, 2), (2, 5, 3, 3), (2, 3, 2, 4), (4, 40), (2, 6, 5, 3),
    (2, 3, 3, 4), (4, 41), (2, 1, 4, 3), (4, 42), (2, 1, 4, 4), (2, 3, 4, 4), (2, 6, 4, 4), (2, 5, 5, 3),
    (4, 43), (2, 3, 5, 3), (2, 1, 5, 4), (2, 5, 3, 4), (2, 4, 5, 4), (2, 5, 5, 4), (2, 5, 4, 3), (4, 44),
    (2, 6, 5, 4), (2, 7, 3, 3), (2, 7, 3, 4), (4, 45), (2, 7, 4, 3), (2, 1, 3, 4), (2, 7, 4, 4), (2, 6, 3, 3),
    (2, 7, 5, 4), (2, 6, 3, 4), (2, 5, 4, 4), (2, 3, 5, 4), (2, 7, 5, 3),
)


def forward_right(dh, p):
    return p % THIRDS < (THIRDS + 1 - dh) // 2


def with_row(a, k, row):
    n = a.shape[1]
    g = k // 8 * 8
    sub = lax.broadcasted_iota(jnp.int32, (8, n), 0)
    middle = jnp.where(sub == k - g, jnp.broadcast_to(row, (8, n)), a[g:g + 8])
    return jnp.concatenate([part for part in (a[:g], middle, a[g + 8:]) if part.shape[0]], axis=0)


def invert(a):
    n = a.shape[0]
    lane = lax.broadcasted_iota(jnp.int32, (n, n), 1)
    lane_one = lax.broadcasted_iota(jnp.int32, (1, n), 1)
    for start in range(0, n, PIVOTS):
        spread = [jnp.broadcast_to(a[:, k:k + 1], (n, n)) for k in range(start, start + PIVOTS)]
        for j in range(PIVOTS):
            k = start + j
            col = spread[j]
            scale = 1.0 / col[k:k + 1, :]
            row = jnp.where(lane_one == k, scale, a[k:k + 1, :] * scale)
            a = with_row(jnp.where(lane == k, 0.0, a) - col * row, k, row)
            for i in range(j + 1, PIVOTS):
                row = spread[i][k:k + 1, :] * scale
                spread[i] = with_row(spread[i] - col * row, k, row)
        yield None
    yield a


def exact_dot(a, b):
    return jnp.dot(a, b, precision=lax.Precision.HIGHEST, preferred_element_type=jnp.float32)


def inverse_of_gram(fall, fall_t, gram, inverse):
    fall_t[...] = fall[...].T
    yield
    gram[...] = jnp.dot(fall_t[...], fall[...], preferred_element_type=jnp.float32)
    yield
    n = FACTORS // 2
    first = None
    for first in invert(gram[:n, :n]):
        yield
    upper, lower = gram[:n, n:], gram[n:, :n]
    right, left = exact_dot(first, upper), exact_dot(lower, first)
    schur = gram[n:, n:] - exact_dot(lower, right)
    yield
    second = None
    for second in invert(schur):
        yield
    off = -exact_dot(right, second)
    inverse[:n, :n] = first - exact_dot(off, left)
    inverse[:n, n:] = off
    inverse[n:, :n] = -exact_dot(second, left)
    inverse[n:, n:] = second
    yield


def residual_of(block, fall, fall_t, inverse):
    cross = jnp.dot(fall_t[...], block, preferred_element_type=jnp.float32)
    exposure = exact_dot(inverse[...], cross)
    fitted = jnp.dot(fall[...], exposure.astype(jnp.bfloat16), preferred_element_type=jnp.float32)
    return exposure, (block.astype(jnp.float32) - fitted).astype(jnp.bfloat16)


def own_residuals(mine, fall, fall_t, inverse, loadings, mine_t):
    for side in range(SIDES):
        part = pl.ds(side * SIDE, SIDE)
        exposure, residual = residual_of(mine[:, part], fall, fall_t, inverse)
        loadings[:, part] = exposure
        mine_t[part, :] = residual.T
        yield


def early_columns(prepare, cols, fall, fall_t, inverse, mine_t, first_side, residuals):
    for core in range(2):
        if core == 0:
            prepare()
        part = pl.ds(core * ASSET_BLOCK, SIDE)
        residuals[core] = residual_of(cols[:, part], fall, fall_t, inverse)[1]
        yield
    for core in range(2):
        for block in range(2):
            rows = pl.ds(block * SIDE, SIDE)
            first_side[core, rows, :] = jnp.dot(
                mine_t[rows, :], residuals[core], preferred_element_type=jnp.float32) * (1.0 / DAYS)
            yield


def gather_kernel(f_hbm, x_hbm, cols, fall, fall_t, inverse, loadings, mine_t, first_side,
                  mine, residuals, gram, load_sem, f_send, f_recv, f_pair,
                  m_send, m_recv, c_send, c_recv, c_pair, fp_send, cp_send):
    day, asset = lax.axis_index("days"), lax.axis_index("assets")
    x, h = day // 2, day % 2
    z, l, c = asset // 4, (asset // 2) % 2, asset % 2
    dl, dz = (l + h) % 2, (z - x + 4) % 4
    is_root = jnp.logical_and(dl == 0, dz == 0)
    right_is_root = jnp.logical_and(dl == 0, dz == 1)
    left_is_root = jnp.logical_and(dl == 0, dz == 3)
    partner_is_root = jnp.logical_and(dl == 1, dz == 0)

    def among(roles):
        return functools.reduce(jnp.logical_or, [jnp.logical_and(dl == i, dz == j) for i, j in roles])

    def day_of(dx, dh):
        return lax.rem(x + dx + 4, 4) * 2 + lax.rem(h + dh, 2)

    def asset_of(link):
        if link == "z+":
            return lax.rem(z + 1, 4) * 4 + l * 2 + c
        if link == "z-":
            return lax.rem(z + 3, 4) * 4 + l * 2 + c
        return z * 4 + (1 - l) * 2 + c

    sibling = z * 4 + l * 2 + 1 - c
    own_rows = pl.ds(pl.multiple_of(day * DAY_BLOCK, DAY_BLOCK), DAY_BLOCK)
    load_x = pltpu.make_async_copy(x_hbm, mine.at[own_rows], load_sem.at[0])
    load_f = pltpu.make_async_copy(f_hbm, fall.at[own_rows], load_sem.at[1])
    load_f.start()
    load_x.start()

    barrier = pltpu.get_barrier_semaphore()
    greeted = [(day_of(0, 1), asset), (day_of(1, 0), asset), (day_of(-1, 0), asset)]
    greeted += [(day, asset_of("z+")), (day, asset_of("z-")), (day, asset_of("y")), (day, sibling)]
    for d, a in greeted:
        pl.semaphore_signal(barrier, inc=1, device_id={"days": d, "assets": a}, device_id_type=MESH)
    pl.semaphore_wait(barrier, len(greeted))
    load_f.wait()
    load_x.wait()

    pending = []

    def send(src, dst, ssem, rsem, d, a, when=None):
        copy = pltpu.make_async_remote_copy(
            src_ref=src, dst_ref=dst, send_sem=ssem, recv_sem=rsem,
            device_id={"days": d, "assets": a}, device_id_type=MESH)
        if when is None:
            copy.start()
        else:
            pl.when(when)(copy.start)
        pending.append((when, copy))

    def arrived(ref, rsem):
        pltpu.make_async_remote_copy(
            src_ref=ref, dst_ref=ref, send_sem=load_sem.at[0], recv_sem=rsem,
            device_id={"days": day, "assets": sibling}, device_id_type=MESH).wait_recv()

    def f_rows(dx, dh, core):
        return fall.at[pl.ds(pl.multiple_of(day_of(dx, dh) * DAY_BLOCK + core * HALF, 32), HALF)]

    def part_rows(dx, dh, p):
        return pl.ds(pl.multiple_of(day_of(dx, dh) * DAY_BLOCK + p % THIRDS * PART, PART), PART)

    def m_part(dx, dh, p):
        return mine.at[part_rows(dx, dh, p), pl.ds(p // THIRDS * SIDE, SIDE)]

    def c_part(dx, dh, p, core):
        lanes = pl.ds(pl.multiple_of(core * ASSET_BLOCK + p // THIRDS * SIDE, SIDE), SIDE)
        return cols.at[part_rows(dx, dh, p), lanes]

    n_f, n_m, n_c = [0], [0], [0]

    def send_f(dx, dh, to):
        ref = f_rows(dx, dh, c)
        send(ref, ref, f_send.at[n_f[0]], f_recv.at[day_of(dx, dh)], day_of(*to), asset)
        n_f[0] += 1

    def send_m(dx, dh, p, to, when=None):
        ref = m_part(dx, dh, p)
        send(ref, ref, m_send.at[n_m[0]], m_recv.at[day_of(dx, dh), p], day_of(*to), asset, when)
        n_m[0] += 1

    def pair_f(dx, dh):
        ref = f_rows(dx, dh, c)
        arrived(ref, f_recv.at[day_of(dx, dh)])
        send(ref, ref, fp_send.at[day_of(dx, dh)], f_pair.at[day_of(dx, dh)], day, sibling)

    def root_sends(dx, dh, p):
        link = TREES[p % THIRDS][0][0]
        src, dst = m_part(dx, dh, p), c_part(dx, dh, p, c)
        send(src, dst, c_send.at[n_c[0]], c_recv.at[day_of(dx, dh), p], day, asset_of(link), is_root)
        n_c[0] += 1
        send(src, dst, cp_send.at[day_of(dx, dh), p], c_pair.at[day_of(dx, dh), p], day, sibling, is_root)

    def relay_mine(dx, dh, p):
        arrived(m_part(dx, dh, p), m_recv.at[day_of(dx, dh), p])
        right, left = (None, None) if dh == 0 else (jnp.logical_not(right_is_root), jnp.logical_not(left_is_root))
        if (dx, dh) == (0, 1):
            send_m(dx, dh, p, (1, 0))
            send_m(dx, dh, p, (-1, 0))
        if dx == -1 and forward_right(dh, p):
            send_m(dx, dh, p, (1, 0), right)
        if dx == 1 and not forward_right(dh, p):
            send_m(dx, dh, p, (-1, 0), left)
        if (dx, dh) == (2, 0):
            send_m(dx, dh, p, (0, 1), partner_is_root)
        root_sends(dx, dh, p)

    def relay_cols(dx, dh, p, depth):
        ref = c_part(dx, dh, p, c)
        tree = p % THIRDS
        here = DEPTHS[tree][depth - 1]
        pl.when(among(here))(lambda: arrived(ref, c_recv.at[day_of(dx, dh), p]))
        for link, roles in TREES[tree]:
            roles = [role for role in roles if role in here]
            if roles:
                send(ref, ref, c_send.at[n_c[0]], c_recv.at[day_of(dx, dh), p], day, asset_of(link), among(roles))
                n_c[0] += 1
        send(ref, ref, cp_send.at[day_of(dx, dh), p], c_pair.at[day_of(dx, dh), p], day, sibling, among(here))

    def fill(side):
        @pl.when(is_root)
        def _():
            lanes = pl.ds(pl.multiple_of(c * ASSET_BLOCK + side * SIDE, SIDE), SIDE)

            @pl.loop(0, DAYS // 64)
            def _(i):
                rows = pl.ds(pl.multiple_of(i * 64, 64), 64)
                cols[rows, lanes] = mine[rows, pl.ds(side * SIDE, SIDE)]

        for dx, dh in CHUNKS:
            for p in range(side * THIRDS, (side + 1) * THIRDS):
                arrived(c_part(dx, dh, p, 1 - c), c_pair.at[day_of(dx, dh), p])

    factor_steps = iter((
        lambda: (send_f(0, 0, (0, 1)), send_f(0, 0, (1, 0)), send_f(0, 0, (-1, 0))),
        lambda: (pair_f(0, 1), send_f(0, 1, (1, 0)), send_f(0, 1, (-1, 0))),
        lambda: (pair_f(1, 0), pair_f(-1, 0), send_f(-1, 0, (1, 0))),
        lambda: (pair_f(1, 1), send_f(1, 1, (-1, 0)), pair_f(-1, 1)),
        lambda: (pair_f(2, 0), pair_f(2, 1),
                 [arrived(f_rows(dx, dh, 1 - c), f_pair.at[day_of(dx, dh)]) for dx, dh in CHUNKS[1:]]),
    ))
    compute = itertools.chain(
        inverse_of_gram(fall, fall_t, gram, inverse),
        own_residuals(mine, fall, fall_t, inverse, loadings, mine_t),
        early_columns(lambda: fill(0), cols, fall, fall_t, inverse, mine_t, first_side, residuals),
    )
    for kind, a, *rest in ORDER:
        if kind == 0 and LINKS[a] == "root":
            root_sends(0, 0, *rest)
        elif kind == 0:
            send_m(0, 0, *rest, {"h": (0, 1), "x+": (1, 0), "x-": (-1, 0)}[LINKS[a]])
        elif kind == 1:
            relay_mine(*CHUNKS[a], *rest)
        elif kind == 2:
            relay_cols(*CHUNKS[a], *rest)
        elif kind == 3:
            next(factor_steps)()
        else:
            next(compute)
    fill(1)
    for _ in compute:
        pass

    for when, copy in pending:
        if when is None:
            copy.wait_send()
        else:
            pl.when(when)(copy.wait_send)


def gather(factors, returns):
    dma = pltpu.SemaphoreType.DMA
    shape = jax.ShapeDtypeStruct
    return pl.pallas_call(
        gather_kernel,
        out_shape=(
            shape((DAYS, 2 * ASSET_BLOCK), jnp.bfloat16),
            shape((DAYS, FACTORS), jnp.bfloat16),
            shape((FACTORS, DAYS), jnp.bfloat16),
            shape((FACTORS, FACTORS), jnp.float32),
            shape((FACTORS, ASSET_BLOCK), jnp.float32),
            shape((ASSET_BLOCK, DAYS), jnp.bfloat16),
            shape((2, ASSET_BLOCK, SIDE), jnp.float32),
        ),
        in_specs=[pl.BlockSpec(memory_space=pl.ANY)] * 2,
        out_specs=(pl.BlockSpec(memory_space=pltpu.VMEM),) * 7,
        scratch_shapes=[
            pltpu.VMEM((DAYS, ASSET_BLOCK), jnp.bfloat16),
            pltpu.VMEM((2, DAYS, SIDE), jnp.bfloat16),
            pltpu.VMEM((FACTORS, FACTORS), jnp.float32),
            dma((2,)), dma((7,)), dma((8,)), dma((8,)), dma((10 * PARTS,)), dma((8, PARTS)),
            dma((8 * PARTS * 7,)), dma((8, PARTS)), dma((8, PARTS)), dma((8,)), dma((8, PARTS)),
        ],
        compiler_params=pltpu.CompilerParams(
            collective_id=0, has_side_effects=True, vmem_limit_bytes=36 * 2**20),
        name="gather",
    )(factors, returns)


def covariance_kernel(cols, fall, fall_t, inverse, loadings, mine_t, first_side, loadings_out, covariance, stage, sems):
    copies = [pltpu.make_async_copy(loadings, loadings_out, sems.at[0])]
    for core in range(2):
        lanes = pl.ds(core * ASSET_BLOCK, SIDE)
        copies.append(pltpu.make_async_copy(first_side.at[core], covariance.at[:, lanes], sems.at[1 + core]))
    for copy in copies:
        copy.start()
    for core in range(2):
        lanes = pl.ds(core * ASSET_BLOCK + SIDE, SIDE)
        _, residual = residual_of(cols[:, lanes], fall, fall_t, inverse)
        for block in range(2):
            rows = pl.ds(block * SIDE, SIDE)
            stage[core, rows, :] = jnp.dot(
                mine_t[rows, :], residual, preferred_element_type=jnp.float32) * (1.0 / DAYS)
            copy = pltpu.make_async_copy(
                stage.at[core, rows], covariance.at[rows, lanes], sems.at[3 + core * 2 + block])
            copy.start()
            copies.append(copy)
    for copy in copies:
        copy.wait()


def covariances(*args):
    return pl.pallas_call(
        covariance_kernel,
        out_shape=(
            jax.ShapeDtypeStruct((FACTORS, ASSET_BLOCK), jnp.float32),
            jax.ShapeDtypeStruct((ASSET_BLOCK, 2 * ASSET_BLOCK), jnp.float32),
        ),
        in_specs=[pl.BlockSpec(memory_space=pltpu.VMEM)] * len(args),
        out_specs=(pl.BlockSpec(memory_space=pltpu.HBM),) * 2,
        scratch_shapes=[pltpu.VMEM((2, ASSET_BLOCK, SIDE), jnp.float32), pltpu.SemaphoreType.DMA((7,))],
        compiler_params=pltpu.CompilerParams(vmem_limit_bytes=24 * 2**20),
        name="covariances",
    )(*args)


def per_device(factors, returns):
    factors = pltpu.with_memory_space_constraint(factors, pltpu.HBM)
    returns = pltpu.with_memory_space_constraint(returns, pltpu.HBM)
    return covariances(*gather(factors, returns))


def solution(mesh):
    in_specs = (P("days", None), P("days", "assets"))
    out_specs = (P(None, "assets"), P("assets", "days"))
    return jax.shard_map(
        per_device, mesh=mesh, in_specs=in_specs, out_specs=out_specs, check_vma=False
    )
```

```python
import functools
import itertools

import jax
import jax.numpy as jnp
from jax import lax
from jax.experimental import pallas as pl
from jax.experimental.pallas import tpu as pltpu
from jax.sharding import PartitionSpec as P

MESH = pl.DeviceIdType.MESH
DAY_BLOCK = 192
DAYS = 8 * DAY_BLOCK
ASSET_BLOCK = 1024
FACTORS = 256
HALF = 96
THIRDS, SIDES = 3, 2
PARTS = THIRDS * SIDES
PART = DAY_BLOCK // THIRDS
SIDE_WIDTH = (512, 512)
SIDE_AT = (0, SIDE_WIDTH[0])
ROWS = 512
PIVOTS = 8

TREES = (
    (("z+", ((0, 0), (0, 1), (0, 2), (1, 2))), ("y", ((0, 1), (0, 2))), ("z-", ((1, 1),))),
    (("z-", ((0, 0), (0, 3), (0, 2), (1, 3), (1, 2))), ("y", ((0, 3),)), ("z+", ((1, 3),))),
    (("y", ((0, 0), (1, 1), (1, 2), (1, 3))), ("z+", ((1, 0), (1, 1))), ("z-", ((1, 0),))),
)
DEPTHS = (
    (((0, 1),), ((0, 2), (1, 1)), ((0, 3), (1, 2), (1, 0)), ((1, 3),)),
    (((0, 3),), ((0, 2), (1, 3)), ((0, 1), (1, 2), (1, 0)), ((1, 1),)),
    (((1, 0),), ((1, 1), (1, 3)), ((0, 1), (1, 2), (0, 3)), ((0, 2),)),
)
CHUNKS = ((0, 0), (0, 1), (1, 0), (1, 1), (-1, 0), (-1, 1), (2, 0), (2, 1))

LINKS = ("h", "x+", "x-", "root")
ORDER = (
    (3, 0), (0, 3, 1), (0, 2, 0), (0, 2, 2), (0, 3, 4), (0, 1, 0), (0, 3, 2), (0, 0, 1),
    (0, 1, 2), (0, 1, 1), (0, 0, 2), (0, 0, 0), (0, 1, 4), (0, 1, 3), (0, 3, 3), (0, 2, 3),
    (1, 4, 0), (2, 0, 3, 1), (0, 2, 1), (0, 2, 4), (0, 0, 4), (1, 2, 2), (3, 1), (2, 0, 1, 1),
    (1, 4, 2), (0, 0, 5), (2, 0, 2, 1), (2, 0, 4, 1), (1, 1, 0), (2, 0, 2, 2), (0, 3, 0), (2, 0, 1, 2),
    (2, 2, 2, 1), (2, 4, 0, 1), (2, 4, 2, 1), (1, 4, 1), (2, 4, 1, 1), (3, 2), (0, 2, 5), (0, 0, 3),
    (2, 1, 0, 1), (2, 0, 0, 1), (1, 4, 4), (1, 2, 4), (2, 0, 3, 2), (1, 2, 0), (2, 2, 0, 1), (1, 4, 3),
    (1, 2, 1), (0, 1, 5), (1, 2, 3), (1, 6, 0), (3, 3), (1, 1, 1), (1, 1, 2), (2, 2, 4, 1),
    (0, 3, 5), (2, 4, 2, 2), (2, 4, 1, 2), (2, 4, 3, 1), (1, 3, 0), (2, 1, 2, 1), (2, 4, 0, 2), (2, 2, 3, 1),
    (1, 5, 0), (1, 2, 5), (1, 6, 2), (1, 6, 1), (2, 6, 0, 1), (2, 0, 4, 2), (1, 1, 4), (2, 2, 1, 1),
    (2, 0, 5, 1), (2, 0, 0, 2), (3, 4), (2, 3, 0, 1), (2, 2, 5, 1), (2, 4, 4, 1), (1, 1, 3), (4, 0),
    (1, 6, 4), (2, 1, 0, 2), (2, 2, 2, 2), (4, 1), (2, 5, 0, 1), (2, 2, 4, 2), (1, 3, 2), (4, 2),
    (2, 4, 1, 3), (1, 1, 5), (2, 1, 2, 2), (2, 0, 5, 2), (2, 0, 0, 3), (2, 6, 2, 1), (2, 2, 0, 2), (2, 1, 1, 1),
    (2, 6, 1, 1), (4, 3), (2, 2, 3, 2), (2, 6, 0, 2), (1, 3, 1), (2, 2, 5, 2), (2, 0, 4, 3), (4, 4),
    (2, 3, 2, 1), (1, 4, 5), (1, 6, 3), (4, 5), (4, 6), (2, 2, 2, 3), (2, 2, 1, 2), (2, 3, 0, 2),
    (1, 5, 1), (2, 4, 1, 4), (4, 7), (2, 4, 2, 3), (2, 0, 1, 3), (4, 8), (4, 9), (2, 6, 1, 2),
    (2, 1, 5, 1), (2, 4, 3, 2), (2, 3, 1, 1), (2, 1, 4, 1), (2, 0, 2, 3), (4, 10), (2, 6, 2, 2), (2, 1, 3, 1),
    (1, 3, 4), (2, 1, 1, 2), (2, 5, 2, 1), (2, 2, 4, 3), (1, 7, 0), (2, 4, 4, 2), (1, 5, 2), (2, 1, 2, 3),
    (2, 5, 0, 2), (4, 11), (1, 6, 5), (2, 1, 5, 2), (1, 7, 2), (4, 12), (2, 4, 5, 1), (2, 6, 5, 1),
    (4, 13), (2, 0, 3, 3), (1, 5, 4), (1, 3, 3), (4, 14), (2, 3, 2, 2), (2, 0, 5, 3), (4, 15),
    (2, 5, 1, 1), (2, 4, 0, 3), (2, 1, 3, 2), (2, 7, 0, 1), (2, 1, 4, 2), (2, 3, 1, 2), (1, 3, 5), (1, 7, 1),
    (4, 16), (4, 17), (4, 18), (2, 5, 2, 2), (2, 0, 0, 4), (1, 5, 3), (2, 7, 2, 1), (4, 19),
    (2, 7, 1, 1), (2, 6, 3, 1), (4, 20), (2, 3, 5, 1), (1, 5, 5), (2, 4, 5, 2), (2, 1, 0, 3), (2, 5, 1, 2),
    (4, 21), (2, 5, 3, 1), (4, 22), (2, 6, 3, 2), (2, 5, 4, 1), (2, 6, 5, 2), (2, 7, 0, 2), (4, 23),
    (2, 3, 3, 1), (2, 5, 5, 1), (4, 24), (2, 1, 0, 4), (4, 25), (2, 6, 0, 3), (2, 6, 1, 3), (2, 7, 1, 2),
    (2, 5, 3, 2), (2, 4, 3, 3), (2, 7, 2, 2), (4, 26), (4, 27), (1, 7, 4), (2, 2, 4, 4), (2, 5, 4, 2),
    (4, 28), (4, 29), (4, 30), (2, 7, 4, 1), (2, 1, 5, 3), (2, 2, 1, 3), (2, 3, 0, 3), (2, 6, 4, 1),
    (2, 1, 2, 4), (2, 3, 5, 2), (2, 6, 2, 3), (2, 7, 5, 1), (2, 3, 4, 1), (2, 0, 2, 4), (2, 4, 4, 3), (2, 2, 2, 4),
    (4, 31), (4, 32), (4, 33), (2, 5, 5, 2), (2, 7, 4, 2), (2, 3, 0, 4), (1, 7, 5), (4, 34),
    (2, 2, 0, 3), (2, 6, 1, 4), (4, 35), (4, 36), (4, 37), (2, 3, 1, 3), (2, 6, 4, 2), (2, 5, 2, 3),
    (2, 3, 2, 3), (2, 2, 0, 4), (2, 2, 5, 3), (2, 5, 0, 3), (2, 0, 5, 4), (2, 7, 5, 2), (2, 7, 3, 1), (2, 1, 1, 3),
    (1, 7, 3), (4, 38), (4, 39), (4, 40), (2, 5, 1, 3), (2, 4, 2, 4), (2, 3, 3, 2), (4, 41),
    (2, 7, 0, 3), (4, 42), (2, 4, 0, 4), (2, 5, 1, 4), (4, 43), (2, 6, 2, 4), (2, 5, 2, 4), (2, 7, 0, 4),
    (2, 0, 4, 4), (4, 44), (2, 0, 1, 4), (2, 3, 4, 2), (2, 7, 2, 3), (2, 2, 3, 3), (2, 7, 3, 2), (2, 6, 0, 4),
    (2, 6, 3, 3), (4, 45), (2, 1, 1, 4), (2, 3, 1, 4), (2, 7, 1, 3), (2, 2, 3, 4), (2, 5, 3, 3), (2, 5, 0, 4),
    (2, 7, 2, 4), (2, 4, 4, 4), (2, 4, 3, 4), (2, 2, 1, 4), (2, 1, 4, 3), (2, 6, 5, 3), (2, 7, 1, 4), (2, 2, 5, 4),
    (2, 3, 2, 4), (4, 46), (2, 5, 4, 3), (4, 47), (2, 3, 5, 3), (4, 48), (4, 49), (4, 50),
    (2, 4, 5, 3), (4, 51), (4, 52), (2, 6, 4, 3), (2, 7, 5, 3), (2, 1, 3, 3), (4, 53), (2, 5, 5, 3),
    (2, 7, 4, 3), (2, 4, 5, 4), (2, 1, 4, 4), (2, 3, 3, 3), (4, 54), (2, 7, 4, 4), (2, 5, 3, 4), (4, 55),
    (2, 5, 4, 4), (2, 6, 4, 4), (2, 1, 3, 4), (2, 3, 5, 4), (2, 6, 3, 4), (2, 3, 4, 4), (2, 7, 5, 4), (2, 1, 5, 4),
    (2, 3, 3, 4), (2, 7, 3, 3), (2, 3, 4, 3), (2, 0, 3, 4), (2, 6, 5, 4), (2, 7, 3, 4), (2, 5, 5, 4),
)


def forward_right(dh, p):
    return p % THIRDS < (THIRDS + 1 - dh) // 2


def with_row(a, k, row):
    n = a.shape[1]
    g = k // 8 * 8
    sub = lax.broadcasted_iota(jnp.int32, (8, n), 0)
    middle = jnp.where(sub == k - g, jnp.broadcast_to(row, (8, n)), a[g:g + 8])
    return jnp.concatenate([part for part in (a[:g], middle, a[g + 8:]) if part.shape[0]], axis=0)


def invert(a):
    n = a.shape[0]
    lane = lax.broadcasted_iota(jnp.int32, (n, n), 1)
    lane_one = lax.broadcasted_iota(jnp.int32, (1, n), 1)
    for start in range(0, n, PIVOTS):
        spread = [jnp.broadcast_to(a[:, k:k + 1], (n, n)) for k in range(start, start + PIVOTS)]
        for j in range(PIVOTS):
            k = start + j
            col = spread[j]
            scale = 1.0 / col[k:k + 1, :]
            row = jnp.where(lane_one == k, scale, a[k:k + 1, :] * scale)
            a = with_row(jnp.where(lane == k, 0.0, a) - col * row, k, row)
            for i in range(j + 1, PIVOTS):
                row = spread[i][k:k + 1, :] * scale
                spread[i] = with_row(spread[i] - col * row, k, row)
        yield None
    yield a


def exact_dot(a, b):
    return jnp.dot(a, b, precision=lax.Precision.HIGHEST, preferred_element_type=jnp.float32)


def inverse_of_gram(fall, fall_t, gram, inverse):
    fall_t[...] = fall[...].T
    yield
    gram[...] = jnp.dot(fall_t[...], fall[...], preferred_element_type=jnp.float32)
    yield
    n = FACTORS // 2
    first = None
    for first in invert(gram[:n, :n]):
        yield
    upper, lower = gram[:n, n:], gram[n:, :n]
    right, left = exact_dot(first, upper), exact_dot(lower, first)
    schur = gram[n:, n:] - exact_dot(lower, right)
    yield
    second = None
    for second in invert(schur):
        yield
    off = -exact_dot(right, second)
    inverse[:n, :n] = first - exact_dot(off, left)
    inverse[:n, n:] = off
    inverse[n:, :n] = -exact_dot(second, left)
    inverse[n:, n:] = second
    yield


def residual_steps(block, fall, fall_t, inverse):
    cross = jnp.dot(fall_t[...], block, preferred_element_type=jnp.float32)
    yield
    exposure = exact_dot(inverse[...], cross)
    yield
    fitted = jnp.dot(fall[...], exposure.astype(jnp.bfloat16), preferred_element_type=jnp.float32)
    return exposure, (block.astype(jnp.float32) - fitted).astype(jnp.bfloat16)


def residual_of(*args):
    steps = residual_steps(*args)
    while True:
        try:
            next(steps)
        except StopIteration as done:
            return done.value


def own_residuals(mine, fall, fall_t, inverse, loadings, mine_t):
    for side in range(SIDES):
        part = pl.ds(SIDE_AT[side], SIDE_WIDTH[side])
        exposure, residual = yield from residual_steps(mine[:, part], fall, fall_t, inverse)
        loadings[:, part] = exposure
        yield
        mine_t[part, :] = residual.T
        yield


def early_columns(prepare, cols, fall, fall_t, inverse, mine_t, first_side, residuals):
    for core in range(2):
        if core == 0:
            prepare()
        part = pl.ds(core * ASSET_BLOCK, SIDE_WIDTH[0])
        _, residuals[core] = yield from residual_steps(cols[:, part], fall, fall_t, inverse)
        yield
    for core in range(2):
        for block in range(2):
            rows = pl.ds(block * ROWS, ROWS)
            first_side[core, rows, :] = jnp.dot(
                mine_t[rows, :], residuals[core], preferred_element_type=jnp.float32) * (1.0 / DAYS)
            yield


def gather_kernel(f_hbm, x_hbm, cols, fall, fall_t, inverse, loadings, mine_t, first_side,
                  mine, residuals, gram, load_sem, f_send, f_recv, f_pair,
                  m_send, m_recv, c_send, c_recv, c_pair, fp_send, cp_send):
    day, asset = lax.axis_index("days"), lax.axis_index("assets")
    x, h = day // 2, day % 2
    z, l, c = asset // 4, (asset // 2) % 2, asset % 2
    dl, dz = (l + h) % 2, (z - x + 4) % 4
    is_root = jnp.logical_and(dl == 0, dz == 0)
    right_is_root = jnp.logical_and(dl == 0, dz == 1)
    left_is_root = jnp.logical_and(dl == 0, dz == 3)
    partner_is_root = jnp.logical_and(dl == 1, dz == 0)

    def among(roles):
        return functools.reduce(jnp.logical_or, [jnp.logical_and(dl == i, dz == j) for i, j in roles])

    def day_of(dx, dh):
        return lax.rem(x + dx + 4, 4) * 2 + lax.rem(h + dh, 2)

    def asset_of(link):
        if link == "z+":
            return lax.rem(z + 1, 4) * 4 + l * 2 + c
        if link == "z-":
            return lax.rem(z + 3, 4) * 4 + l * 2 + c
        return z * 4 + (1 - l) * 2 + c

    sibling = z * 4 + l * 2 + 1 - c
    own_rows = pl.ds(pl.multiple_of(day * DAY_BLOCK, DAY_BLOCK), DAY_BLOCK)
    load_x = pltpu.make_async_copy(x_hbm, mine.at[own_rows], load_sem.at[0])
    load_f = pltpu.make_async_copy(f_hbm, fall.at[own_rows], load_sem.at[1])
    load_f.start()
    load_x.start()

    barrier = pltpu.get_barrier_semaphore()
    greeted = [(day_of(0, 1), asset), (day_of(1, 0), asset), (day_of(-1, 0), asset)]
    greeted += [(day, asset_of("z+")), (day, asset_of("z-")), (day, asset_of("y")), (day, sibling)]
    for d, a in greeted:
        pl.semaphore_signal(barrier, inc=1, device_id={"days": d, "assets": a}, device_id_type=MESH)
    pl.semaphore_wait(barrier, len(greeted))
    load_f.wait()
    load_x.wait()

    pending = []

    def send(src, dst, ssem, rsem, d, a, when=None):
        copy = pltpu.make_async_remote_copy(
            src_ref=src, dst_ref=dst, send_sem=ssem, recv_sem=rsem,
            device_id={"days": d, "assets": a}, device_id_type=MESH)
        if when is None:
            copy.start()
        else:
            pl.when(when)(copy.start)
        pending.append((when, copy))

    def arrived(ref, rsem):
        pltpu.make_async_remote_copy(
            src_ref=ref, dst_ref=ref, send_sem=load_sem.at[0], recv_sem=rsem,
            device_id={"days": day, "assets": sibling}, device_id_type=MESH).wait_recv()

    def f_rows(dx, dh, core):
        return fall.at[pl.ds(pl.multiple_of(day_of(dx, dh) * DAY_BLOCK + core * HALF, 32), HALF)]

    def part_rows(dx, dh, p):
        return pl.ds(pl.multiple_of(day_of(dx, dh) * DAY_BLOCK + p % THIRDS * PART, PART), PART)

    def m_part(dx, dh, p):
        return mine.at[part_rows(dx, dh, p), pl.ds(SIDE_AT[p // THIRDS], SIDE_WIDTH[p // THIRDS])]

    def c_part(dx, dh, p, core):
        side = p // THIRDS
        lanes = pl.ds(pl.multiple_of(core * ASSET_BLOCK + SIDE_AT[side], 128), SIDE_WIDTH[side])
        return cols.at[part_rows(dx, dh, p), lanes]

    n_f, n_m, n_c = [0], [0], [0]

    def send_f(dx, dh, to):
        ref = f_rows(dx, dh, c)
        send(ref, ref, f_send.at[n_f[0]], f_recv.at[day_of(dx, dh)], day_of(*to), asset)
        n_f[0] += 1

    def send_m(dx, dh, p, to, when=None):
        ref = m_part(dx, dh, p)
        send(ref, ref, m_send.at[n_m[0]], m_recv.at[day_of(dx, dh), p], day_of(*to), asset, when)
        n_m[0] += 1

    def pair_f(dx, dh):
        ref = f_rows(dx, dh, c)
        arrived(ref, f_recv.at[day_of(dx, dh)])
        send(ref, ref, fp_send.at[day_of(dx, dh)], f_pair.at[day_of(dx, dh)], day, sibling)

    def root_sends(dx, dh, p):
        link = TREES[p % THIRDS][0][0]
        src, dst = m_part(dx, dh, p), c_part(dx, dh, p, c)
        send(src, dst, c_send.at[n_c[0]], c_recv.at[day_of(dx, dh), p], day, asset_of(link), is_root)
        n_c[0] += 1
        send(src, dst, cp_send.at[day_of(dx, dh), p], c_pair.at[day_of(dx, dh), p], day, sibling, is_root)

    def relay_mine(dx, dh, p):
        arrived(m_part(dx, dh, p), m_recv.at[day_of(dx, dh), p])
        right, left = (None, None) if dh == 0 else (jnp.logical_not(right_is_root), jnp.logical_not(left_is_root))
        if (dx, dh) == (0, 1):
            send_m(dx, dh, p, (1, 0))
            send_m(dx, dh, p, (-1, 0))
        if dx == -1 and forward_right(dh, p):
            send_m(dx, dh, p, (1, 0), right)
        if dx == 1 and not forward_right(dh, p):
            send_m(dx, dh, p, (-1, 0), left)
        if (dx, dh) == (2, 0):
            send_m(dx, dh, p, (0, 1), partner_is_root)
        root_sends(dx, dh, p)

    def relay_cols(dx, dh, p, depth):
        ref = c_part(dx, dh, p, c)
        tree = p % THIRDS
        here = DEPTHS[tree][depth - 1]
        pl.when(among(here))(lambda: arrived(ref, c_recv.at[day_of(dx, dh), p]))
        for link, roles in TREES[tree]:
            roles = [role for role in roles if role in here]
            if roles:
                send(ref, ref, c_send.at[n_c[0]], c_recv.at[day_of(dx, dh), p], day, asset_of(link), among(roles))
                n_c[0] += 1
        send(ref, ref, cp_send.at[day_of(dx, dh), p], c_pair.at[day_of(dx, dh), p], day, sibling, among(here))

    def fill(side):
        @pl.when(is_root)
        def _():
            at, width = SIDE_AT[side], SIDE_WIDTH[side]
            lanes = pl.ds(pl.multiple_of(c * ASSET_BLOCK + at, 128), width)

            @pl.loop(0, DAYS // 64)
            def _(i):
                rows = pl.ds(pl.multiple_of(i * 64, 64), 64)
                cols[rows, lanes] = mine[rows, pl.ds(at, width)]

        for dx, dh in CHUNKS:
            for p in range(side * THIRDS, (side + 1) * THIRDS):
                arrived(c_part(dx, dh, p, 1 - c), c_pair.at[day_of(dx, dh), p])

    factor_steps = iter((
        lambda: (send_f(0, 0, (0, 1)), send_f(0, 0, (1, 0)), send_f(0, 0, (-1, 0))),
        lambda: (pair_f(0, 1), send_f(0, 1, (1, 0)), send_f(0, 1, (-1, 0))),
        lambda: (pair_f(1, 0), pair_f(-1, 0), send_f(-1, 0, (1, 0))),
        lambda: (pair_f(1, 1), send_f(1, 1, (-1, 0)), pair_f(-1, 1)),
        lambda: (pair_f(2, 0), pair_f(2, 1),
                 [arrived(f_rows(dx, dh, 1 - c), f_pair.at[day_of(dx, dh)]) for dx, dh in CHUNKS[1:]]),
    ))
    compute = itertools.chain(
        inverse_of_gram(fall, fall_t, gram, inverse),
        own_residuals(mine, fall, fall_t, inverse, loadings, mine_t),
        early_columns(lambda: fill(0), cols, fall, fall_t, inverse, mine_t, first_side, residuals),
    )
    for kind, a, *rest in ORDER:
        if kind == 0 and LINKS[a] == "root":
            root_sends(0, 0, *rest)
        elif kind == 0:
            send_m(0, 0, *rest, {"h": (0, 1), "x+": (1, 0), "x-": (-1, 0)}[LINKS[a]])
        elif kind == 1:
            relay_mine(*CHUNKS[a], *rest)
        elif kind == 2:
            relay_cols(*CHUNKS[a], *rest)
        elif kind == 3:
            next(factor_steps)()
        else:
            next(compute)
    fill(1)
    for _ in compute:
        pass

    for when, copy in pending:
        if when is None:
            copy.wait_send()
        else:
            pl.when(when)(copy.wait_send)


def gather(factors, returns):
    dma = pltpu.SemaphoreType.DMA
    shape = jax.ShapeDtypeStruct
    return pl.pallas_call(
        gather_kernel,
        out_shape=(
            shape((DAYS, 2 * ASSET_BLOCK), jnp.bfloat16),
            shape((DAYS, FACTORS), jnp.bfloat16),
            shape((FACTORS, DAYS), jnp.bfloat16),
            shape((FACTORS, FACTORS), jnp.float32),
            shape((FACTORS, ASSET_BLOCK), jnp.float32),
            shape((ASSET_BLOCK, DAYS), jnp.bfloat16),
            shape((2, ASSET_BLOCK, SIDE_WIDTH[0]), jnp.float32),
        ),
        in_specs=[pl.BlockSpec(memory_space=pl.ANY)] * 2,
        out_specs=(pl.BlockSpec(memory_space=pltpu.VMEM),) * 7,
        scratch_shapes=[
            pltpu.VMEM((DAYS, ASSET_BLOCK), jnp.bfloat16),
            pltpu.VMEM((2, DAYS, SIDE_WIDTH[0]), jnp.bfloat16),
            pltpu.VMEM((FACTORS, FACTORS), jnp.float32),
            dma((2,)), dma((7,)), dma((8,)), dma((8,)), dma((10 * PARTS,)), dma((8, PARTS)),
            dma((8 * PARTS * 7,)), dma((8, PARTS)), dma((8, PARTS)), dma((8,)), dma((8, PARTS)),
        ],
        compiler_params=pltpu.CompilerParams(
            collective_id=0, has_side_effects=True, vmem_limit_bytes=36 * 2**20),
        name="gather",
    )(factors, returns)


def covariance_kernel(cols, fall, fall_t, inverse, loadings, mine_t, first_side, loadings_out, covariance, stage, sems):
    width = SIDE_WIDTH[1]
    copies = [pltpu.make_async_copy(loadings, loadings_out, sems.at[0])]
    for core in range(2):
        lanes = pl.ds(core * ASSET_BLOCK, SIDE_WIDTH[0])
        copies.append(pltpu.make_async_copy(first_side.at[core], covariance.at[:, lanes], sems.at[1 + core]))
    for copy in copies:
        copy.start()
    lanes = [pl.ds(core * ASSET_BLOCK + SIDE_AT[1], width) for core in range(2)]
    blocks = [cols[:, part] for part in lanes]
    groups = [(0,), (1,)] if width >= 512 else [(0, 1)]
    for group in groups:
        block = jnp.concatenate([blocks[core] for core in group], axis=1)
        _, residual = residual_of(block, fall, fall_t, inverse)
        for half in range(2):
            rows = pl.ds(half * ROWS, ROWS)
            product = jnp.dot(mine_t[rows, :], residual, preferred_element_type=jnp.float32) * (1.0 / DAYS)
            for i, core in enumerate(group):
                stage[core, rows, :] = product[:, i * width:(i + 1) * width]
                copy = pltpu.make_async_copy(
                    stage.at[core, rows], covariance.at[rows, lanes[core]], sems.at[3 + core * 2 + half])
                copy.start()
                copies.append(copy)
    for copy in copies:
        copy.wait()


def covariances(*args):
    return pl.pallas_call(
        covariance_kernel,
        out_shape=(
            jax.ShapeDtypeStruct((FACTORS, ASSET_BLOCK), jnp.float32),
            jax.ShapeDtypeStruct((ASSET_BLOCK, 2 * ASSET_BLOCK), jnp.float32),
        ),
        in_specs=[pl.BlockSpec(memory_space=pltpu.VMEM)] * len(args),
        out_specs=(pl.BlockSpec(memory_space=pltpu.HBM),) * 2,
        scratch_shapes=[pltpu.VMEM((2, ASSET_BLOCK, SIDE_WIDTH[1]), jnp.float32), pltpu.SemaphoreType.DMA((7,))],
        compiler_params=pltpu.CompilerParams(vmem_limit_bytes=24 * 2**20),
        name="covariances",
    )(*args)


def per_device(factors, returns):
    factors = pltpu.with_memory_space_constraint(factors, pltpu.HBM)
    returns = pltpu.with_memory_space_constraint(returns, pltpu.HBM)
    return covariances(*gather(factors, returns))


def solution(mesh):
    in_specs = (P("days", None), P("days", "assets"))
    out_specs = (P(None, "assets"), P("assets", "days"))
    return jax.shard_map(
        per_device, mesh=mesh, in_specs=in_specs, out_specs=out_specs, check_vma=False
    )
```

```python
import functools
import itertools

import jax
import jax.numpy as jnp
from jax import lax
from jax.experimental import pallas as pl
from jax.experimental.pallas import tpu as pltpu
from jax.sharding import PartitionSpec as P

MESH = pl.DeviceIdType.MESH
DAY_BLOCK = 192
DAYS = 8 * DAY_BLOCK
ASSET_BLOCK = 1024
FACTORS = 256
HALF = 96
THIRDS, SIDES = 3, 2
PARTS = THIRDS * SIDES
PART = DAY_BLOCK // THIRDS
SIDE_WIDTH = (512, 512)
SIDE_AT = (0, SIDE_WIDTH[0])
ROWS = 512
PIVOTS = 8

TREES = (
    (("z+", ((0, 0), (0, 1), (0, 2), (1, 2))), ("y", ((0, 1), (0, 2))), ("z-", ((1, 1),))),
    (("z-", ((0, 0), (0, 3), (0, 2), (1, 3), (1, 2))), ("y", ((0, 3),)), ("z+", ((1, 3),))),
    (("y", ((0, 0), (1, 1), (1, 2), (1, 3))), ("z+", ((1, 0), (1, 1))), ("z-", ((1, 0),))),
)
ROLES = ((0, 1), (0, 2), (0, 3), (1, 0), (1, 1), (1, 2), (1, 3))
CHUNKS = ((0, 0), (0, 1), (1, 0), (1, 1), (-1, 0), (-1, 1), (2, 0), (2, 1))

LINKS = ("h", "x+", "x-", "root")
ORDER = (
    (3, 0), (0, 1, 2), (0, 3, 2), (0, 1, 0), (0, 1, 1), (0, 0, 1), (0, 2, 4), (0, 2, 1),
    (0, 0, 0), (0, 2, 0), (0, 1, 3), (0, 3, 1), (0, 3, 3), (0, 0, 2), (0, 3, 0), (2, 0, 1, 2),
    (2, 0, 2, 3), (0, 2, 2), (2, 0, 3, 0), (0, 3, 4), (0, 1, 4), (1, 4, 2), (1, 4, 0), (1, 2, 4),
    (3, 1), (2, 0, 0, 0), (0, 2, 3), (1, 4, 1), (0, 0, 3), (2, 0, 4, 2), (1, 1, 0), (0, 0, 4),
    (3, 2), (1, 2, 1), (2, 4, 0, 0), (2, 2, 4, 2), (1, 4, 3), (0, 2, 5), (1, 4, 4), (2, 4, 2, 3),
    (2, 4, 1, 2), (1, 2, 0), (1, 2, 2), (1, 2, 3), (0, 1, 5), (2, 2, 2, 3), (2, 0, 4, 6), (2, 0, 1, 6),
    (0, 0, 5), (2, 0, 2, 6), (2, 0, 2, 4), (2, 4, 2, 4), (2, 0, 4, 1), (3, 3), (1, 1, 1), (2, 1, 0, 0),
    (2, 4, 1, 6), (1, 1, 2), (1, 3, 0), (2, 2, 1, 2), (1, 6, 0), (2, 1, 2, 3), (2, 4, 4, 2), (2, 0, 0, 1),
    (2, 0, 3, 4), (1, 6, 1), (2, 0, 3, 1), (2, 2, 0, 0), (0, 3, 5), (2, 4, 3, 0), (2, 1, 0, 4), (1, 5, 0),
    (2, 4, 0, 1), (1, 1, 4), (2, 2, 2, 4), (2, 2, 4, 6), (1, 2, 5), (3, 4), (2, 0, 5, 3), (2, 6, 1, 2),
    (1, 6, 2), (2, 3, 0, 0), (4, 0), (2, 0, 4, 3), (2, 6, 0, 0), (2, 2, 4, 1), (4, 1), (2, 1, 2, 6),
    (1, 1, 3), (2, 2, 5, 3), (2, 4, 2, 5), (2, 0, 0, 4), (1, 6, 3), (2, 4, 2, 6), (1, 1, 5), (1, 3, 1),
    (2, 1, 2, 4), (2, 0, 0, 5), (4, 2), (2, 2, 0, 1), (2, 5, 0, 0), (2, 0, 1, 1), (2, 4, 0, 5), (2, 4, 1, 5),
    (2, 6, 2, 3), (2, 2, 0, 4), (2, 4, 0, 4), (4, 3), (2, 3, 0, 1), (2, 6, 0, 1), (2, 0, 5, 4), (1, 3, 2),
    (2, 0, 2, 0), (4, 4), (4, 5), (2, 0, 1, 3), (1, 4, 5), (2, 0, 4, 5), (1, 3, 4), (2, 1, 5, 3),
    (2, 1, 0, 3), (4, 6), (2, 1, 0, 1), (2, 0, 0, 2), (2, 0, 3, 3), (1, 6, 4), (2, 2, 3, 0), (2, 2, 1, 6),
    (2, 0, 3, 5), (2, 5, 0, 1), (2, 4, 1, 3), (4, 7), (2, 1, 4, 2), (2, 2, 2, 6), (2, 4, 1, 4), (2, 1, 3, 0),
    (2, 2, 5, 4), (2, 4, 3, 4), (2, 4, 1, 1), (2, 6, 0, 4), (2, 3, 2, 3), (2, 3, 0, 4), (2, 0, 1, 0), (4, 8),
    (4, 9), (2, 4, 4, 6), (2, 3, 1, 2), (4, 10), (2, 6, 2, 4), (2, 4, 4, 1), (2, 0, 5, 6), (2, 4, 0, 6),
    (2, 4, 5, 3), (2, 6, 1, 6), (1, 7, 0), (2, 2, 4, 3), (2, 3, 2, 4), (1, 5, 2), (2, 1, 1, 2), (2, 2, 2, 0),
    (1, 3, 3), (2, 5, 2, 3), (2, 1, 2, 2), (2, 0, 1, 5), (1, 6, 5), (1, 5, 1), (2, 1, 2, 5), (2, 5, 0, 4),
    (2, 2, 5, 6), (2, 6, 3, 0), (4, 11), (4, 12), (2, 1, 5, 6), (2, 0, 2, 2), (4, 13), (2, 1, 5, 4),
    (4, 14), (2, 3, 0, 2), (2, 2, 4, 0), (2, 0, 4, 0), (2, 6, 1, 1), (2, 1, 3, 4), (1, 3, 5), (2, 3, 1, 6),
    (2, 7, 0, 0), (2, 2, 1, 3), (2, 2, 3, 4), (2, 2, 3, 1), (1, 5, 4), (2, 6, 4, 2), (2, 4, 2, 0), (4, 15),
    (2, 6, 5, 3), (2, 3, 3, 0), (4, 16), (2, 4, 3, 1), (2, 1, 2, 0), (2, 2, 1, 1), (2, 2, 0, 5), (2, 5, 2, 4),
    (4, 17), (2, 0, 2, 5), (4, 18), (1, 5, 3), (2, 0, 1, 4), (1, 7, 1), (2, 5, 1, 2), (2, 1, 1, 6),
    (2, 3, 0, 5), (2, 4, 2, 2), (4, 19), (2, 0, 5, 0), (2, 2, 4, 5), (2, 7, 2, 3), (2, 0, 0, 3), (2, 1, 0, 2),
    (2, 2, 5, 5), (2, 6, 2, 6), (2, 4, 1, 0), (2, 1, 1, 1), (2, 6, 0, 3), (2, 0, 0, 6), (2, 4, 5, 4), (2, 2, 4, 4),
    (2, 3, 3, 4), (2, 2, 2, 2), (2, 3, 1, 1), (4, 20), (2, 5, 2, 6), (2, 1, 4, 6), (1, 7, 2), (4, 21),
    (4, 22), (2, 5, 3, 0), (2, 4, 3, 3), (2, 2, 0, 3), (2, 3, 5, 3), (2, 7, 0, 4), (2, 7, 1, 2), (2, 4, 2, 1),
    (2, 2, 2, 5), (2, 6, 2, 0), (2, 5, 4, 2), (2, 5, 1, 6), (2, 4, 5, 6), (2, 1, 0, 5), (4, 23), (2, 7, 0, 1),
    (2, 1, 4, 1), (4, 24), (2, 0, 2, 1), (2, 6, 5, 6), (2, 4, 0, 3), (1, 7, 4), (2, 6, 3, 1), (4, 25),
    (4, 26), (2, 5, 5, 3), (2, 2, 1, 5), (2, 0, 3, 2), (2, 4, 0, 2), (2, 1, 0, 6), (2, 2, 3, 5), (2, 6, 3, 4),
    (2, 7, 1, 6), (2, 1, 3, 1), (2, 7, 2, 4), (2, 5, 0, 5), (1, 5, 5), (4, 27), (2, 7, 1, 1), (2, 7, 4, 2),
    (2, 3, 2, 6), (2, 3, 1, 3), (2, 2, 3, 6), (2, 3, 3, 1), (2, 6, 1, 5), (2, 2, 2, 1), (2, 0, 5, 2), (2, 5, 4, 6),
    (2, 6, 5, 4), (2, 5, 1, 1), (2, 5, 3, 1), (2, 3, 4, 2), (2, 5, 3, 4), (4, 28), (2, 6, 2, 5), (4, 29),
    (2, 3, 2, 5), (2, 6, 0, 5), (2, 7, 2, 6), (4, 30), (4, 31), (2, 3, 5, 4), (1, 7, 3), (2, 7, 5, 3),
    (2, 4, 4, 5), (4, 32), (2, 6, 4, 6), (2, 7, 4, 6), (1, 7, 5), (2, 3, 0, 3), (2, 1, 5, 5), (2, 5, 0, 2),
    (2, 1, 1, 3), (2, 5, 0, 6), (4, 33), (2, 7, 3, 0), (2, 5, 4, 1), (4, 34), (2, 5, 2, 0), (2, 3, 1, 5),
    (4, 35), (2, 1, 1, 5), (2, 7, 4, 1), (4, 36), (4, 37), (4, 38), (2, 0, 5, 5), (2, 3, 4, 6),
    (2, 7, 0, 5), (2, 4, 3, 5), (2, 2, 3, 3), (2, 5, 5, 4), (2, 3, 1, 0), (4, 39), (2, 6, 1, 3), (2, 7, 3, 1),
    (2, 6, 0, 2), (2, 1, 5, 0), (2, 5, 1, 5), (2, 7, 5, 6), (2, 2, 0, 6), (4, 40), (2, 5, 2, 5), (2, 2, 3, 2),
    (4, 41), (4, 42), (2, 5, 5, 6), (2, 6, 4, 1), (2, 7, 1, 5), (4, 43), (2, 7, 0, 3), (2, 2, 5, 0),
    (2, 6, 3, 2), (2, 7, 1, 3), (2, 3, 5, 6), (2, 1, 5, 2), (2, 2, 1, 4), (2, 7, 5, 4), (2, 1, 5, 1), (2, 5, 4, 5),
    (2, 3, 4, 1), (2, 5, 1, 3), (2, 3, 2, 2), (2, 6, 2, 1), (2, 6, 2, 2), (2, 4, 4, 3), (2, 1, 4, 5), (2, 1, 2, 1),
    (2, 7, 2, 5), (4, 44), (2, 1, 3, 5), (2, 1, 3, 3), (2, 4, 5, 5), (2, 3, 3, 5), (2, 5, 2, 1), (2, 7, 0, 2),
    (4, 45), (2, 7, 1, 0), (2, 7, 0, 6), (2, 6, 1, 4), (2, 1, 4, 0), (2, 7, 2, 1), (2, 2, 5, 2), (2, 4, 5, 2),
    (2, 6, 5, 5), (2, 6, 4, 3), (2, 0, 4, 4), (2, 6, 3, 3), (2, 5, 0, 3), (2, 2, 0, 2), (2, 7, 2, 0), (2, 1, 4, 3),
    (2, 5, 1, 0), (2, 3, 0, 6), (2, 3, 2, 0), (2, 1, 1, 0), (2, 5, 3, 2), (2, 5, 3, 3), (2, 4, 4, 4), (2, 7, 4, 3),
    (2, 5, 2, 2), (2, 1, 1, 4), (2, 3, 1, 4), (2, 6, 0, 6), (2, 7, 1, 4), (2, 3, 2, 1), (2, 5, 1, 4), (2, 4, 5, 0),
    (2, 6, 3, 5), (2, 7, 2, 2), (2, 4, 3, 2), (2, 6, 1, 0), (2, 3, 3, 3), (2, 2, 1, 0), (4, 46), (4, 47),
    (4, 48), (2, 6, 5, 2), (2, 1, 3, 2), (2, 7, 3, 4), (2, 6, 4, 5), (4, 49), (4, 50), (4, 51),
    (2, 3, 5, 5), (2, 0, 3, 6), (2, 3, 3, 2), (2, 4, 5, 1), (2, 4, 4, 0), (4, 52), (2, 6, 3, 6), (2, 5, 5, 0),
    (2, 7, 4, 5), (2, 7, 5, 2), (2, 5, 3, 5), (2, 5, 4, 0), (2, 5, 5, 5), (2, 3, 3, 6), (2, 3, 4, 5), (2, 4, 3, 6),
    (4, 53), (2, 5, 4, 4), (2, 1, 4, 4), (2, 7, 3, 2), (4, 54), (2, 6, 4, 4), (2, 6, 4, 0), (2, 6, 5, 0),
    (2, 7, 4, 4), (2, 7, 3, 5), (2, 3, 5, 1), (2, 5, 5, 2), (2, 7, 5, 5), (2, 1, 3, 6), (2, 0, 5, 1), (2, 5, 3, 6),
    (2, 5, 5, 1), (2, 5, 4, 3), (4, 55), (2, 3, 4, 4), (2, 2, 5, 1), (2, 3, 5, 2), (2, 6, 5, 1), (2, 3, 4, 0),
    (2, 3, 4, 3), (2, 7, 4, 0), (2, 7, 5, 1), (2, 3, 5, 0), (2, 7, 3, 3), (2, 7, 5, 0), (2, 7, 3, 6),
)


def forward_right(dh, p):
    return p % THIRDS < (THIRDS + 1 - dh) // 2


def with_row(a, k, row):
    n = a.shape[1]
    g = k // 8 * 8
    sub = lax.broadcasted_iota(jnp.int32, (8, n), 0)
    middle = jnp.where(sub == k - g, jnp.broadcast_to(row, (8, n)), a[g:g + 8])
    return jnp.concatenate([part for part in (a[:g], middle, a[g + 8:]) if part.shape[0]], axis=0)


def invert(a):
    n = a.shape[0]
    lane = lax.broadcasted_iota(jnp.int32, (n, n), 1)
    lane_one = lax.broadcasted_iota(jnp.int32, (1, n), 1)
    for start in range(0, n, PIVOTS):
        spread = [jnp.broadcast_to(a[:, k:k + 1], (n, n)) for k in range(start, start + PIVOTS)]
        for j in range(PIVOTS):
            k = start + j
            col = spread[j]
            scale = 1.0 / col[k:k + 1, :]
            row = jnp.where(lane_one == k, scale, a[k:k + 1, :] * scale)
            a = with_row(jnp.where(lane == k, 0.0, a) - col * row, k, row)
            for i in range(j + 1, PIVOTS):
                row = spread[i][k:k + 1, :] * scale
                spread[i] = with_row(spread[i] - col * row, k, row)
        yield None
    yield a


def exact_dot(a, b):
    return jnp.dot(a, b, precision=lax.Precision.HIGHEST, preferred_element_type=jnp.float32)


def inverse_of_gram(fall, fall_t, gram, inverse):
    fall_t[...] = fall[...].T
    yield
    gram[...] = jnp.dot(fall_t[...], fall[...], preferred_element_type=jnp.float32)
    yield
    n = FACTORS // 2
    first = None
    for first in invert(gram[:n, :n]):
        yield
    upper, lower = gram[:n, n:], gram[n:, :n]
    right, left = exact_dot(first, upper), exact_dot(lower, first)
    schur = gram[n:, n:] - exact_dot(lower, right)
    yield
    second = None
    for second in invert(schur):
        yield
    off = -exact_dot(right, second)
    inverse[:n, :n] = first - exact_dot(off, left)
    inverse[:n, n:] = off
    inverse[n:, :n] = -exact_dot(second, left)
    inverse[n:, n:] = second
    yield


def residual_steps(block, fall, fall_t, inverse):
    cross = jnp.dot(fall_t[...], block, preferred_element_type=jnp.float32)
    yield
    exposure = exact_dot(inverse[...], cross)
    yield
    fitted = jnp.dot(fall[...], exposure.astype(jnp.bfloat16), preferred_element_type=jnp.float32)
    return exposure, (block.astype(jnp.float32) - fitted).astype(jnp.bfloat16)


def residual_of(*args):
    steps = residual_steps(*args)
    while True:
        try:
            next(steps)
        except StopIteration as done:
            return done.value


def own_residuals(mine, fall, fall_t, inverse, loadings, mine_t):
    for side in range(SIDES):
        part = pl.ds(SIDE_AT[side], SIDE_WIDTH[side])
        exposure, residual = yield from residual_steps(mine[:, part], fall, fall_t, inverse)
        loadings[:, part] = exposure
        yield
        mine_t[part, :] = residual.T
        yield


def early_columns(prepare, cols, fall, fall_t, inverse, mine_t, first_side, residuals):
    for core in range(2):
        if core == 0:
            prepare()
        part = pl.ds(core * ASSET_BLOCK, SIDE_WIDTH[0])
        _, residuals[core] = yield from residual_steps(cols[:, part], fall, fall_t, inverse)
        yield
    for core in range(2):
        for block in range(2):
            rows = pl.ds(block * ROWS, ROWS)
            first_side[core, rows, :] = jnp.dot(
                mine_t[rows, :], residuals[core], preferred_element_type=jnp.float32) * (1.0 / DAYS)
            yield


def gather_kernel(f_hbm, x_hbm, cols, fall, fall_t, inverse, loadings, mine_t, first_side,
                  mine, residuals, gram, load_sem, f_send, f_recv, f_pair,
                  m_send, m_recv, c_send, c_recv, c_pair, fp_send, cp_send):
    day, asset = lax.axis_index("days"), lax.axis_index("assets")
    x, h = day // 2, day % 2
    z, l, c = asset // 4, (asset // 2) % 2, asset % 2
    dl, dz = (l + h) % 2, (z - x + 4) % 4
    is_root = jnp.logical_and(dl == 0, dz == 0)
    right_is_root = jnp.logical_and(dl == 0, dz == 1)
    left_is_root = jnp.logical_and(dl == 0, dz == 3)
    partner_is_root = jnp.logical_and(dl == 1, dz == 0)

    def among(roles):
        return functools.reduce(jnp.logical_or, [jnp.logical_and(dl == i, dz == j) for i, j in roles])

    def day_of(dx, dh):
        return lax.rem(x + dx + 4, 4) * 2 + lax.rem(h + dh, 2)

    def asset_of(link):
        if link == "z+":
            return lax.rem(z + 1, 4) * 4 + l * 2 + c
        if link == "z-":
            return lax.rem(z + 3, 4) * 4 + l * 2 + c
        return z * 4 + (1 - l) * 2 + c

    sibling = z * 4 + l * 2 + 1 - c
    own_rows = pl.ds(pl.multiple_of(day * DAY_BLOCK, DAY_BLOCK), DAY_BLOCK)
    load_x = pltpu.make_async_copy(x_hbm, mine.at[own_rows], load_sem.at[0])
    load_f = pltpu.make_async_copy(f_hbm, fall.at[own_rows], load_sem.at[1])
    load_f.start()
    load_x.start()

    barrier = pltpu.get_barrier_semaphore()
    greeted = [(day_of(0, 1), asset), (day_of(1, 0), asset), (day_of(-1, 0), asset)]
    greeted += [(day, asset_of("z+")), (day, asset_of("z-")), (day, asset_of("y")), (day, sibling)]
    for d, a in greeted:
        pl.semaphore_signal(barrier, inc=1, device_id={"days": d, "assets": a}, device_id_type=MESH)
    pl.semaphore_wait(barrier, len(greeted))
    load_f.wait()
    load_x.wait()

    pending = []

    def send(src, dst, ssem, rsem, d, a, when=None):
        copy = pltpu.make_async_remote_copy(
            src_ref=src, dst_ref=dst, send_sem=ssem, recv_sem=rsem,
            device_id={"days": d, "assets": a}, device_id_type=MESH)
        if when is None:
            copy.start()
        else:
            pl.when(when)(copy.start)
        pending.append((when, copy))

    def arrived(ref, rsem):
        pltpu.make_async_remote_copy(
            src_ref=ref, dst_ref=ref, send_sem=load_sem.at[0], recv_sem=rsem,
            device_id={"days": day, "assets": sibling}, device_id_type=MESH).wait_recv()

    def f_rows(dx, dh, core):
        return fall.at[pl.ds(pl.multiple_of(day_of(dx, dh) * DAY_BLOCK + core * HALF, 32), HALF)]

    def part_rows(dx, dh, p):
        return pl.ds(pl.multiple_of(day_of(dx, dh) * DAY_BLOCK + p % THIRDS * PART, PART), PART)

    def m_part(dx, dh, p):
        return mine.at[part_rows(dx, dh, p), pl.ds(SIDE_AT[p // THIRDS], SIDE_WIDTH[p // THIRDS])]

    def c_part(dx, dh, p, core):
        side = p // THIRDS
        lanes = pl.ds(pl.multiple_of(core * ASSET_BLOCK + SIDE_AT[side], 128), SIDE_WIDTH[side])
        return cols.at[part_rows(dx, dh, p), lanes]

    n_f, n_m = [0], [0]

    def send_f(dx, dh, to):
        ref = f_rows(dx, dh, c)
        send(ref, ref, f_send.at[n_f[0]], f_recv.at[day_of(dx, dh)], day_of(*to), asset)
        n_f[0] += 1

    def send_m(dx, dh, p, to, when=None):
        ref = m_part(dx, dh, p)
        send(ref, ref, m_send.at[n_m[0]], m_recv.at[day_of(dx, dh), p], day_of(*to), asset, when)
        n_m[0] += 1

    def pair_f(dx, dh):
        ref = f_rows(dx, dh, c)
        arrived(ref, f_recv.at[day_of(dx, dh)])
        send(ref, ref, fp_send.at[day_of(dx, dh)], f_pair.at[day_of(dx, dh)], day, sibling)

    def relayed(src, dst, ssem, rsem, a):
        return pltpu.make_async_remote_copy(
            src_ref=src, dst_ref=dst, send_sem=ssem, recv_sem=rsem,
            device_id={"days": day, "assets": a}, device_id_type=MESH)

    def to_chip(src, dx, dh, p, i):
        k = day_of(dx, dh)
        link = TREES[p % THIRDS][i][0]
        return relayed(src, c_part(dx, dh, p, c), c_send.at[k, p, i], c_recv.at[k, p], asset_of(link))

    def to_sibling(src, dx, dh, p):
        k = day_of(dx, dh)
        return relayed(src, c_part(dx, dh, p, c), cp_send.at[k, p], c_pair.at[k, p], sibling)

    def root_sends(dx, dh, p):
        @pl.when(is_root)
        def _():
            to_chip(m_part(dx, dh, p), dx, dh, p, 0).start()
            to_sibling(m_part(dx, dh, p), dx, dh, p).start()

    def relay_mine(dx, dh, p):
        arrived(m_part(dx, dh, p), m_recv.at[day_of(dx, dh), p])
        right, left = (None, None) if dh == 0 else (jnp.logical_not(right_is_root), jnp.logical_not(left_is_root))
        if (dx, dh) == (0, 1):
            send_m(dx, dh, p, (1, 0))
            send_m(dx, dh, p, (-1, 0))
        if dx == -1 and forward_right(dh, p):
            send_m(dx, dh, p, (1, 0), right)
        if dx == 1 and not forward_right(dh, p):
            send_m(dx, dh, p, (-1, 0), left)
        if (dx, dh) == (2, 0):
            send_m(dx, dh, p, (0, 1), partner_is_root)
        root_sends(dx, dh, p)

    def relay_cols(dx, dh, p, role):
        @pl.when(among((ROLES[role],)))
        def _():
            ref = c_part(dx, dh, p, c)
            arrived(ref, c_recv.at[day_of(dx, dh), p])
            for i, (_, roles) in enumerate(TREES[p % THIRDS]):
                if ROLES[role] in roles:
                    to_chip(ref, dx, dh, p, i).start()
            to_sibling(ref, dx, dh, p).start()

    def fill(side):
        @pl.when(is_root)
        def _():
            at, width = SIDE_AT[side], SIDE_WIDTH[side]
            lanes = pl.ds(pl.multiple_of(c * ASSET_BLOCK + at, 128), width)

            @pl.loop(0, DAYS // 64)
            def _(i):
                rows = pl.ds(pl.multiple_of(i * 64, 64), 64)
                cols[rows, lanes] = mine[rows, pl.ds(at, width)]

        for dx, dh in CHUNKS:
            for p in range(side * THIRDS, (side + 1) * THIRDS):
                arrived(c_part(dx, dh, p, 1 - c), c_pair.at[day_of(dx, dh), p])

    factor_steps = iter((
        lambda: (send_f(0, 0, (0, 1)), send_f(0, 0, (1, 0)), send_f(0, 0, (-1, 0))),
        lambda: (pair_f(0, 1), send_f(0, 1, (1, 0)), send_f(0, 1, (-1, 0))),
        lambda: (pair_f(1, 0), pair_f(-1, 0), send_f(-1, 0, (1, 0))),
        lambda: (pair_f(1, 1), send_f(1, 1, (-1, 0)), pair_f(-1, 1)),
        lambda: (pair_f(2, 0), pair_f(2, 1),
                 [arrived(f_rows(dx, dh, 1 - c), f_pair.at[day_of(dx, dh)]) for dx, dh in CHUNKS[1:]]),
    ))
    compute = itertools.chain(
        inverse_of_gram(fall, fall_t, gram, inverse),
        own_residuals(mine, fall, fall_t, inverse, loadings, mine_t),
        early_columns(lambda: fill(0), cols, fall, fall_t, inverse, mine_t, first_side, residuals),
    )
    for kind, a, *rest in ORDER:
        if kind == 0 and LINKS[a] == "root":
            root_sends(0, 0, *rest)
        elif kind == 0:
            send_m(0, 0, *rest, {"h": (0, 1), "x+": (1, 0), "x-": (-1, 0)}[LINKS[a]])
        elif kind == 1:
            relay_mine(*CHUNKS[a], *rest)
        elif kind == 2:
            relay_cols(*CHUNKS[a], *rest)
        elif kind == 3:
            next(factor_steps)()
        else:
            next(compute)
    fill(1)
    for _ in compute:
        pass

    for when, copy in pending:
        if when is None:
            copy.wait_send()
        else:
            pl.when(when)(copy.wait_send)
    for i in range(THIRDS):
        for third in range(THIRDS):
            @pl.when(among(TREES[third][i][1]))
            def _():
                for dx, dh in CHUNKS:
                    for p in range(third, PARTS, THIRDS):
                        to_chip(c_part(dx, dh, p, c), dx, dh, p, i).wait_send()
    for dx, dh in CHUNKS:
        for p in range(PARTS):
            to_sibling(c_part(dx, dh, p, c), dx, dh, p).wait_send()


def gather(factors, returns):
    dma = pltpu.SemaphoreType.DMA
    shape = jax.ShapeDtypeStruct
    return pl.pallas_call(
        gather_kernel,
        out_shape=(
            shape((DAYS, 2 * ASSET_BLOCK), jnp.bfloat16),
            shape((DAYS, FACTORS), jnp.bfloat16),
            shape((FACTORS, DAYS), jnp.bfloat16),
            shape((FACTORS, FACTORS), jnp.float32),
            shape((FACTORS, ASSET_BLOCK), jnp.float32),
            shape((ASSET_BLOCK, DAYS), jnp.bfloat16),
            shape((2, ASSET_BLOCK, SIDE_WIDTH[0]), jnp.float32),
        ),
        in_specs=[pl.BlockSpec(memory_space=pl.ANY)] * 2,
        out_specs=(pl.BlockSpec(memory_space=pltpu.VMEM),) * 7,
        scratch_shapes=[
            pltpu.VMEM((DAYS, ASSET_BLOCK), jnp.bfloat16),
            pltpu.VMEM((2, DAYS, SIDE_WIDTH[0]), jnp.bfloat16),
            pltpu.VMEM((FACTORS, FACTORS), jnp.float32),
            dma((2,)), dma((7,)), dma((8,)), dma((8,)), dma((10 * PARTS,)), dma((8, PARTS)),
            dma((8, PARTS, 3)), dma((8, PARTS)), dma((8, PARTS)), dma((8,)), dma((8, PARTS)),
        ],
        compiler_params=pltpu.CompilerParams(
            collective_id=0, has_side_effects=True, vmem_limit_bytes=36 * 2**20),
        name="gather",
    )(factors, returns)


def covariance_kernel(cols, fall, fall_t, inverse, loadings, mine_t, first_side, loadings_out, covariance, stage, sems):
    width = SIDE_WIDTH[1]
    copies = [pltpu.make_async_copy(loadings, loadings_out, sems.at[0])]
    for core in range(2):
        lanes = pl.ds(core * ASSET_BLOCK, SIDE_WIDTH[0])
        copies.append(pltpu.make_async_copy(first_side.at[core], covariance.at[:, lanes], sems.at[1 + core]))
    for copy in copies:
        copy.start()
    lanes = [pl.ds(core * ASSET_BLOCK + SIDE_AT[1], width) for core in range(2)]
    blocks = [cols[:, part] for part in lanes]
    groups = [(0,), (1,)] if width >= 512 else [(0, 1)]
    for group in groups:
        block = jnp.concatenate([blocks[core] for core in group], axis=1)
        _, residual = residual_of(block, fall, fall_t, inverse)
        for half in range(2):
            rows = pl.ds(half * ROWS, ROWS)
            product = jnp.dot(mine_t[rows, :], residual, preferred_element_type=jnp.float32) * (1.0 / DAYS)
            for i, core in enumerate(group):
                stage[core, rows, :] = product[:, i * width:(i + 1) * width]
                copy = pltpu.make_async_copy(
                    stage.at[core, rows], covariance.at[rows, lanes[core]], sems.at[3 + core * 2 + half])
                copy.start()
                copies.append(copy)
    for copy in copies:
        copy.wait()


def covariances(*args):
    return pl.pallas_call(
        covariance_kernel,
        out_shape=(
            jax.ShapeDtypeStruct((FACTORS, ASSET_BLOCK), jnp.float32),
            jax.ShapeDtypeStruct((ASSET_BLOCK, 2 * ASSET_BLOCK), jnp.float32),
        ),
        in_specs=[pl.BlockSpec(memory_space=pltpu.VMEM)] * len(args),
        out_specs=(pl.BlockSpec(memory_space=pltpu.HBM),) * 2,
        scratch_shapes=[pltpu.VMEM((2, ASSET_BLOCK, SIDE_WIDTH[1]), jnp.float32), pltpu.SemaphoreType.DMA((7,))],
        compiler_params=pltpu.CompilerParams(vmem_limit_bytes=24 * 2**20),
        name="covariances",
    )(*args)


def per_device(factors, returns):
    factors = pltpu.with_memory_space_constraint(factors, pltpu.HBM)
    returns = pltpu.with_memory_space_constraint(returns, pltpu.HBM)
    return covariances(*gather(factors, returns))


def solution(mesh):
    in_specs = (P("days", None), P("days", "assets"))
    out_specs = (P(None, "assets"), P("assets", "days"))
    return jax.shard_map(
        per_device, mesh=mesh, in_specs=in_specs, out_specs=out_specs, check_vma=False
    )
```

```python
import functools
import itertools

import jax
import jax.numpy as jnp
from jax import lax
from jax.experimental import pallas as pl
from jax.experimental.pallas import tpu as pltpu
from jax.sharding import PartitionSpec as P

MESH = pl.DeviceIdType.MESH
DAY_BLOCK = 192
DAYS = 8 * DAY_BLOCK
ASSET_BLOCK = 1024
FACTORS = 256
HALF = 96
THIRDS, SIDES = 3, 2
PARTS = THIRDS * SIDES
PART = DAY_BLOCK // THIRDS
SIDE_WIDTH = (512, 512)
SIDE_AT = (0, SIDE_WIDTH[0])
ROWS = 512
PIVOTS = 8

TREES = (
    (("z+", ((0, 0), (0, 1), (0, 2), (1, 2))), ("y", ((0, 1), (0, 2))), ("z-", ((1, 1),))),
    (("z-", ((0, 0), (0, 3), (0, 2), (1, 3), (1, 2))), ("y", ((0, 3),)), ("z+", ((1, 3),))),
    (("y", ((0, 0), (1, 1), (1, 2), (1, 3))), ("z+", ((1, 0), (1, 1))), ("z-", ((1, 0),))),
)
ROLES = ((0, 1), (0, 2), (0, 3), (1, 0), (1, 1), (1, 2), (1, 3))
CHUNKS = ((0, 0), (0, 1), (1, 0), (1, 1), (-1, 0), (-1, 1), (2, 0), (2, 1))

LINKS = ("h", "x+", "x-", "root")
ORDER = (
    (0, 3, 2), (0, 2, 4), (0, 3, 3), (0, 1, 2), (0, 2, 2), (0, 2, 1), (0, 1, 0), (0, 1, 1),
    (0, 3, 1), (0, 2, 0), (0, 0, 0), (3, 0), (0, 3, 0), (0, 0, 2), (0, 3, 4), (2, 0, 2, 3),
    (1, 4, 2), (0, 1, 3), (2, 0, 1, 2), (2, 0, 4, 2), (0, 1, 4), (1, 1, 0), (2, 0, 1, 6), (0, 2, 5),
    (2, 0, 0, 0), (0, 0, 4), (2, 0, 2, 4), (3, 1), (1, 2, 4), (1, 4, 1), (2, 2, 4, 2), (1, 2, 2),
    (1, 4, 0), (0, 0, 1), (3, 2), (1, 2, 0), (2, 0, 0, 1), (2, 1, 0, 0), (0, 1, 5), (1, 1, 2),
    (0, 0, 3), (0, 3, 5), (2, 4, 2, 3), (2, 0, 4, 6), (1, 2, 1), (2, 4, 1, 2), (1, 4, 4), (1, 3, 0),
    (1, 4, 3), (2, 0, 3, 0), (1, 5, 0), (2, 0, 4, 1), (2, 2, 2, 3), (0, 0, 5), (3, 3), (0, 2, 3),
    (2, 2, 0, 0), (2, 3, 0, 0), (2, 1, 2, 3), (1, 1, 1), (1, 2, 5), (1, 6, 1), (2, 1, 0, 1), (2, 4, 2, 4),
    (1, 1, 4), (1, 6, 2), (2, 4, 0, 0), (2, 2, 2, 4), (2, 0, 2, 6), (1, 1, 3), (2, 0, 5, 3), (2, 2, 1, 2),
    (2, 0, 0, 2), (2, 0, 4, 5), (2, 4, 3, 0), (2, 2, 0, 1), (1, 6, 0), (2, 1, 1, 2), (2, 0, 1, 1), (3, 4),
    (4, 0), (2, 6, 0, 0), (2, 1, 2, 4), (2, 4, 4, 2), (2, 0, 4, 4), (2, 6, 1, 2), (2, 1, 0, 4), (1, 2, 3),
    (2, 2, 5, 3), (2, 0, 3, 1), (2, 3, 0, 1), (2, 0, 2, 0), (1, 1, 5), (4, 1), (2, 2, 4, 6), (4, 2),
    (2, 0, 3, 4), (2, 5, 0, 0), (2, 6, 2, 3), (1, 3, 1), (1, 3, 2), (2, 1, 3, 0), (2, 0, 2, 5), (1, 4, 5),
    (4, 3), (4, 4), (2, 4, 0, 1), (2, 2, 2, 5), (2, 0, 1, 5), (2, 4, 0, 4), (2, 2, 1, 6), (1, 5, 2),
    (2, 2, 4, 1), (2, 0, 5, 6), (2, 0, 0, 5), (4, 5), (2, 0, 0, 4), (2, 0, 5, 4), (2, 1, 5, 3), (4, 6),
    (2, 2, 5, 4), (2, 1, 1, 1), (2, 4, 1, 6), (2, 1, 0, 5), (2, 2, 0, 5), (2, 4, 2, 6), (2, 2, 3, 0), (1, 6, 4),
    (4, 7), (2, 0, 1, 0), (4, 8), (1, 3, 4), (2, 2, 2, 6), (2, 1, 0, 2), (2, 2, 4, 3), (1, 6, 3),
    (2, 6, 0, 1), (2, 3, 2, 3), (2, 3, 0, 4), (4, 9), (2, 6, 2, 4), (4, 10), (2, 0, 1, 3), (2, 1, 0, 3),
    (2, 4, 4, 6), (4, 11), (2, 3, 1, 2), (1, 6, 5), (2, 4, 5, 3), (1, 7, 0), (4, 12), (4, 13),
    (2, 6, 2, 6), (2, 4, 3, 4), (2, 1, 5, 4), (2, 5, 0, 1), (1, 5, 1), (2, 1, 0, 6), (2, 4, 1, 3), (2, 0, 4, 3),
    (1, 3, 3), (2, 5, 2, 3), (2, 2, 5, 6), (2, 0, 1, 4), (2, 4, 2, 5), (2, 4, 3, 1), (2, 6, 1, 6), (2, 0, 4, 0),
    (2, 6, 1, 1), (4, 14), (2, 1, 4, 2), (4, 15), (4, 16), (2, 2, 4, 5), (2, 4, 0, 5), (4, 17),
    (2, 6, 5, 3), (2, 3, 1, 6), (2, 3, 1, 1), (2, 7, 0, 0), (2, 0, 3, 5), (2, 1, 2, 6), (2, 2, 4, 0), (2, 3, 0, 5),
    (2, 6, 0, 4), (2, 6, 4, 2), (1, 7, 1), (2, 2, 1, 1), (2, 3, 2, 4), (4, 18), (2, 2, 3, 1), (4, 19),
    (1, 5, 3), (2, 1, 1, 6), (4, 20), (1, 5, 4), (2, 0, 5, 0), (2, 1, 3, 1), (2, 2, 0, 4), (2, 5, 1, 2),
    (2, 4, 4, 1), (1, 7, 2), (2, 3, 3, 0), (2, 4, 5, 4), (4, 21), (2, 0, 5, 5), (1, 3, 5), (2, 5, 3, 0),
    (2, 0, 3, 2), (2, 4, 4, 5), (2, 6, 3, 0), (2, 7, 0, 4), (4, 22), (2, 1, 4, 6), (2, 2, 1, 5), (4, 23),
    (2, 6, 0, 5), (2, 5, 2, 6), (2, 7, 1, 2), (2, 5, 2, 4), (2, 7, 2, 3), (4, 24), (2, 4, 0, 3), (2, 3, 1, 0),
    (2, 2, 5, 5), (4, 25), (2, 7, 0, 1), (2, 6, 5, 4), (2, 5, 4, 2), (2, 3, 3, 4), (4, 26), (2, 6, 1, 3),
    (2, 5, 0, 5), (2, 1, 2, 5), (2, 3, 2, 6), (2, 5, 1, 6), (2, 2, 0, 2), (2, 5, 0, 4), (1, 5, 5), (2, 3, 5, 3),
    (2, 3, 4, 2), (4, 27), (2, 1, 5, 6), (2, 4, 1, 5), (2, 2, 2, 1), (4, 28), (2, 3, 0, 6), (1, 7, 4),
    (4, 29), (2, 5, 1, 1), (2, 7, 1, 6), (2, 7, 2, 4), (2, 2, 5, 2), (2, 2, 3, 5), (2, 3, 3, 1), (4, 30),
    (2, 6, 4, 6), (2, 3, 1, 5), (2, 1, 2, 2), (2, 2, 3, 2), (2, 3, 2, 5), (2, 1, 1, 5), (2, 6, 2, 5), (1, 7, 3),
    (2, 1, 2, 0), (2, 3, 0, 2), (2, 6, 1, 5), (2, 4, 3, 3), (2, 4, 5, 0), (2, 3, 1, 3), (4, 31), (4, 32),
    (2, 4, 1, 4), (2, 1, 1, 0), (2, 4, 5, 6), (2, 5, 3, 1), (2, 5, 5, 3), (2, 0, 0, 6), (2, 7, 2, 6), (2, 6, 3, 4),
    (2, 7, 3, 0), (2, 7, 4, 2), (2, 4, 3, 5), (2, 5, 4, 6), (2, 7, 1, 1), (2, 3, 5, 4), (4, 33), (4, 34),
    (1, 7, 5), (4, 35), (2, 0, 0, 3), (2, 1, 3, 5), (4, 36), (2, 1, 2, 1), (2, 1, 5, 5), (2, 3, 2, 0),
    (4, 37), (2, 5, 1, 5), (2, 0, 3, 3), (2, 4, 1, 1), (2, 4, 2, 0), (2, 6, 3, 1), (2, 1, 3, 4), (2, 7, 5, 3),
    (2, 5, 2, 5), (2, 4, 3, 2), (4, 38), (2, 3, 4, 6), (2, 5, 4, 1), (2, 2, 3, 4), (2, 4, 4, 3), (2, 7, 0, 5),
    (2, 2, 1, 4), (2, 2, 0, 6), (2, 2, 5, 0), (4, 39), (2, 0, 3, 6), (2, 5, 0, 2), (2, 5, 5, 4), (2, 7, 3, 1),
    (2, 1, 4, 1), (4, 40), (2, 2, 2, 2), (2, 5, 0, 6), (2, 2, 1, 0), (2, 5, 5, 6), (2, 6, 1, 0), (2, 7, 0, 3),
    (2, 2, 4, 4), (4, 41), (2, 4, 4, 0), (2, 6, 0, 3), (2, 1, 5, 1), (2, 1, 1, 3), (2, 7, 1, 3), (2, 1, 4, 3),
    (2, 3, 3, 2), (4, 42), (2, 6, 0, 2), (2, 6, 2, 1), (2, 2, 0, 3), (2, 6, 5, 6), (2, 5, 2, 1), (2, 4, 2, 1),
    (2, 5, 3, 5), (2, 3, 5, 6), (2, 3, 4, 1), (2, 7, 1, 5), (2, 3, 2, 1), (2, 3, 0, 3), (2, 0, 5, 1), (2, 0, 2, 1),
    (2, 1, 1, 4), (2, 3, 1, 4), (2, 5, 2, 0), (2, 6, 2, 2), (2, 2, 2, 0), (2, 5, 1, 4), (2, 6, 0, 6), (2, 3, 3, 5),
    (2, 7, 2, 5), (2, 5, 2, 2), (2, 1, 4, 5), (2, 1, 3, 2), (2, 5, 0, 3), (2, 6, 5, 5), (2, 4, 2, 2), (2, 2, 1, 3),
    (2, 7, 5, 4), (4, 43), (2, 1, 5, 2), (4, 44), (2, 0, 2, 2), (2, 6, 1, 4), (2, 1, 3, 6), (2, 7, 5, 6),
    (4, 45), (2, 3, 2, 2), (2, 7, 2, 0), (2, 4, 5, 2), (2, 7, 4, 6), (2, 6, 4, 5), (2, 1, 5, 0), (2, 4, 1, 0),
    (2, 6, 2, 0), (2, 6, 4, 1), (2, 4, 0, 6), (2, 7, 2, 1), (2, 4, 5, 5), (2, 7, 1, 4), (2, 7, 0, 6), (2, 4, 0, 2),
    (2, 3, 5, 0), (2, 5, 1, 3), (2, 7, 0, 2), (2, 6, 3, 5), (2, 7, 2, 2), (2, 5, 1, 0), (2, 5, 3, 4), (2, 7, 1, 0),
    (2, 7, 3, 4), (4, 46), (2, 7, 4, 1), (2, 4, 3, 6), (2, 6, 3, 2), (4, 47), (4, 48), (2, 3, 4, 5),
    (2, 3, 3, 3), (2, 3, 5, 5), (4, 49), (2, 5, 4, 5), (2, 3, 4, 3), (4, 50), (4, 51), (4, 52),
    (2, 5, 5, 5), (2, 7, 3, 5), (4, 53), (2, 7, 5, 5), (2, 6, 3, 3), (2, 4, 5, 1), (2, 5, 5, 2), (2, 7, 4, 5),
    (4, 54), (2, 1, 4, 4), (4, 55), (2, 7, 4, 0), (2, 3, 5, 1), (2, 2, 5, 1), (2, 7, 4, 3), (2, 3, 3, 6),
    (2, 6, 5, 1), (2, 4, 4, 4), (2, 5, 4, 0), (2, 6, 4, 4), (2, 5, 4, 4), (2, 5, 3, 2), (2, 5, 5, 0), (2, 5, 5, 1),
    (2, 3, 5, 2), (2, 1, 4, 0), (2, 7, 4, 4), (2, 7, 3, 6), (2, 7, 5, 2), (2, 7, 5, 1), (2, 7, 5, 0), (2, 6, 3, 6),
    (2, 1, 3, 3), (2, 2, 3, 3), (2, 6, 4, 3), (2, 5, 3, 3), (2, 5, 4, 3), (2, 6, 4, 0), (2, 3, 4, 4), (2, 6, 5, 2),
    (2, 3, 4, 0), (2, 5, 3, 6), (2, 7, 3, 3), (2, 7, 3, 2), (2, 0, 5, 2), (2, 6, 5, 0), (2, 2, 3, 6),
)


def forward_right(dh, p):
    return p % THIRDS < (THIRDS + 1 - dh) // 2


def with_row(a, k, row):
    n = a.shape[1]
    g = k // 8 * 8
    sub = lax.broadcasted_iota(jnp.int32, (8, n), 0)
    middle = jnp.where(sub == k - g, jnp.broadcast_to(row, (8, n)), a[g:g + 8])
    return jnp.concatenate([part for part in (a[:g], middle, a[g + 8:]) if part.shape[0]], axis=0)


def invert(a):
    n = a.shape[0]
    lane = lax.broadcasted_iota(jnp.int32, (n, n), 1)
    lane_one = lax.broadcasted_iota(jnp.int32, (1, n), 1)
    for start in range(0, n, PIVOTS):
        spread = [jnp.broadcast_to(a[:, k:k + 1], (n, n)) for k in range(start, start + PIVOTS)]
        for j in range(PIVOTS):
            k = start + j
            col = spread[j]
            scale = 1.0 / col[k:k + 1, :]
            row = jnp.where(lane_one == k, scale, a[k:k + 1, :] * scale)
            a = with_row(jnp.where(lane == k, 0.0, a) - col * row, k, row)
            for i in range(j + 1, PIVOTS):
                row = spread[i][k:k + 1, :] * scale
                spread[i] = with_row(spread[i] - col * row, k, row)
        yield None
    yield a


def exact_dot(a, b):
    return jnp.dot(a, b, precision=lax.Precision.HIGHEST, preferred_element_type=jnp.float32)


def inverse_of_gram(fall, fall_t, gram, inverse):
    fall_t[...] = fall[...].T
    yield
    gram[...] = jnp.dot(fall_t[...], fall[...], preferred_element_type=jnp.float32)
    yield
    n = FACTORS // 2
    first = None
    for first in invert(gram[:n, :n]):
        yield
    upper, lower = gram[:n, n:], gram[n:, :n]
    right, left = exact_dot(first, upper), exact_dot(lower, first)
    schur = gram[n:, n:] - exact_dot(lower, right)
    yield
    second = None
    for second in invert(schur):
        yield
    off = -exact_dot(right, second)
    inverse[:n, :n] = first - exact_dot(off, left)
    inverse[:n, n:] = off
    inverse[n:, :n] = -exact_dot(second, left)
    inverse[n:, n:] = second
    yield


def residual_steps(block, fall, fall_t, inverse):
    cross = jnp.dot(fall_t[...], block, preferred_element_type=jnp.float32)
    yield
    exposure = exact_dot(inverse[...], cross)
    yield
    fitted = jnp.dot(fall[...], exposure.astype(jnp.bfloat16), preferred_element_type=jnp.float32)
    return exposure, (block.astype(jnp.float32) - fitted).astype(jnp.bfloat16)


def residual_of(*args):
    steps = residual_steps(*args)
    while True:
        try:
            next(steps)
        except StopIteration as done:
            return done.value


def own_residuals(mine, fall, fall_t, inverse, loadings, mine_t):
    for side in range(SIDES):
        part = pl.ds(SIDE_AT[side], SIDE_WIDTH[side])
        exposure, residual = yield from residual_steps(mine[:, part], fall, fall_t, inverse)
        loadings[:, part] = exposure
        yield
        mine_t[part, :] = residual.T
        yield


def early_columns(prepare, cols, fall, fall_t, inverse, mine_t, first_side, residuals):
    for core in range(2):
        if core == 0:
            prepare()
        part = pl.ds(core * ASSET_BLOCK, SIDE_WIDTH[0])
        _, residuals[core] = yield from residual_steps(cols[:, part], fall, fall_t, inverse)
        yield
    for core in range(2):
        for block in range(2):
            rows = pl.ds(block * ROWS, ROWS)
            first_side[core, rows, :] = jnp.dot(
                mine_t[rows, :], residuals[core], preferred_element_type=jnp.float32) * (1.0 / DAYS)
            yield


def gather_kernel(f_hbm, x_hbm, cols, fall, fall_t, inverse, loadings, mine_t, first_side,
                  mine, residuals, gram, load_sem, f_send, f_recv, f_pair,
                  m_send, m_recv, c_send, c_recv, c_pair, fp_send, cp_send):
    day, asset = lax.axis_index("days"), lax.axis_index("assets")
    x, h = day // 2, day % 2
    z, l, c = asset // 4, (asset // 2) % 2, asset % 2
    dl, dz = (l + h) % 2, (z - x + 4) % 4
    is_root = jnp.logical_and(dl == 0, dz == 0)
    right_is_root = jnp.logical_and(dl == 0, dz == 1)
    left_is_root = jnp.logical_and(dl == 0, dz == 3)
    partner_is_root = jnp.logical_and(dl == 1, dz == 0)

    def among(roles):
        return functools.reduce(jnp.logical_or, [jnp.logical_and(dl == i, dz == j) for i, j in roles])

    def day_of(dx, dh):
        return lax.rem(x + dx + 4, 4) * 2 + lax.rem(h + dh, 2)

    def asset_of(link):
        if link == "z+":
            return lax.rem(z + 1, 4) * 4 + l * 2 + c
        if link == "z-":
            return lax.rem(z + 3, 4) * 4 + l * 2 + c
        return z * 4 + (1 - l) * 2 + c

    sibling = z * 4 + l * 2 + 1 - c
    own_rows = pl.ds(pl.multiple_of(day * DAY_BLOCK, DAY_BLOCK), DAY_BLOCK)
    load_x = pltpu.make_async_copy(x_hbm, mine.at[own_rows], load_sem.at[0])
    load_f = pltpu.make_async_copy(f_hbm, fall.at[own_rows], load_sem.at[1])
    load_f.start()
    load_x.start()

    barrier = pltpu.get_barrier_semaphore()
    greeted = [(day_of(0, 1), asset), (day_of(1, 0), asset), (day_of(-1, 0), asset)]
    greeted += [(day, asset_of("z+")), (day, asset_of("z-")), (day, asset_of("y")), (day, sibling)]
    for d, a in greeted:
        pl.semaphore_signal(barrier, inc=1, device_id={"days": d, "assets": a}, device_id_type=MESH)
    pl.semaphore_wait(barrier, len(greeted))
    load_f.wait()
    load_x.wait()

    pending = []

    def send(src, dst, ssem, rsem, d, a, when=None):
        copy = pltpu.make_async_remote_copy(
            src_ref=src, dst_ref=dst, send_sem=ssem, recv_sem=rsem,
            device_id={"days": d, "assets": a}, device_id_type=MESH)
        if when is None:
            copy.start()
        else:
            pl.when(when)(copy.start)
        pending.append((when, copy))

    def arrived(ref, rsem):
        pltpu.make_async_remote_copy(
            src_ref=ref, dst_ref=ref, send_sem=load_sem.at[0], recv_sem=rsem,
            device_id={"days": day, "assets": sibling}, device_id_type=MESH).wait_recv()

    def f_rows(dx, dh, core):
        return fall.at[pl.ds(pl.multiple_of(day_of(dx, dh) * DAY_BLOCK + core * HALF, 32), HALF)]

    def part_rows(dx, dh, p):
        return pl.ds(pl.multiple_of(day_of(dx, dh) * DAY_BLOCK + p % THIRDS * PART, PART), PART)

    def m_part(dx, dh, p):
        return mine.at[part_rows(dx, dh, p), pl.ds(SIDE_AT[p // THIRDS], SIDE_WIDTH[p // THIRDS])]

    def c_part(dx, dh, p, core):
        side = p // THIRDS
        lanes = pl.ds(pl.multiple_of(core * ASSET_BLOCK + SIDE_AT[side], 128), SIDE_WIDTH[side])
        return cols.at[part_rows(dx, dh, p), lanes]

    n_f, n_m = [0], [0]

    def send_f(dx, dh, to):
        ref = f_rows(dx, dh, c)
        send(ref, ref, f_send.at[n_f[0]], f_recv.at[day_of(dx, dh)], day_of(*to), asset)
        n_f[0] += 1

    def send_m(dx, dh, p, to, when=None):
        ref = m_part(dx, dh, p)
        send(ref, ref, m_send.at[n_m[0]], m_recv.at[day_of(dx, dh), p], day_of(*to), asset, when)
        n_m[0] += 1

    def pair_f(dx, dh):
        ref = f_rows(dx, dh, c)
        arrived(ref, f_recv.at[day_of(dx, dh)])
        send(ref, ref, fp_send.at[day_of(dx, dh)], f_pair.at[day_of(dx, dh)], day, sibling)

    def relayed(src, dst, ssem, rsem, a):
        return pltpu.make_async_remote_copy(
            src_ref=src, dst_ref=dst, send_sem=ssem, recv_sem=rsem,
            device_id={"days": day, "assets": a}, device_id_type=MESH)

    def to_chip(src, dx, dh, p, i):
        k = day_of(dx, dh)
        link = TREES[p % THIRDS][i][0]
        return relayed(src, c_part(dx, dh, p, c), c_send.at[k, p, i], c_recv.at[k, p], asset_of(link))

    def to_sibling(src, dx, dh, p):
        k = day_of(dx, dh)
        return relayed(src, c_part(dx, dh, p, c), cp_send.at[k, p], c_pair.at[k, p], sibling)

    def root_sends(dx, dh, p):
        @pl.when(is_root)
        def _():
            to_chip(m_part(dx, dh, p), dx, dh, p, 0).start()
            to_sibling(m_part(dx, dh, p), dx, dh, p).start()

    def relay_mine(dx, dh, p):
        arrived(m_part(dx, dh, p), m_recv.at[day_of(dx, dh), p])
        right, left = (None, None) if dh == 0 else (jnp.logical_not(right_is_root), jnp.logical_not(left_is_root))
        if (dx, dh) == (0, 1):
            send_m(dx, dh, p, (1, 0))
            send_m(dx, dh, p, (-1, 0))
        if dx == -1 and forward_right(dh, p):
            send_m(dx, dh, p, (1, 0), right)
        if dx == 1 and not forward_right(dh, p):
            send_m(dx, dh, p, (-1, 0), left)
        if (dx, dh) == (2, 0):
            send_m(dx, dh, p, (0, 1), partner_is_root)
        root_sends(dx, dh, p)

    def relay_cols(dx, dh, p, role):
        @pl.when(among((ROLES[role],)))
        def _():
            ref = c_part(dx, dh, p, c)
            arrived(ref, c_recv.at[day_of(dx, dh), p])
            for i, (_, roles) in enumerate(TREES[p % THIRDS]):
                if ROLES[role] in roles:
                    to_chip(ref, dx, dh, p, i).start()
            to_sibling(ref, dx, dh, p).start()

    def fill(side):
        @pl.when(is_root)
        def _():
            at, width = SIDE_AT[side], SIDE_WIDTH[side]
            lanes = pl.ds(pl.multiple_of(c * ASSET_BLOCK + at, 128), width)

            @pl.loop(0, DAYS // 64)
            def _(i):
                rows = pl.ds(pl.multiple_of(i * 64, 64), 64)
                cols[rows, lanes] = mine[rows, pl.ds(at, width)]

        for dx, dh in CHUNKS:
            for p in range(side * THIRDS, (side + 1) * THIRDS):
                arrived(c_part(dx, dh, p, 1 - c), c_pair.at[day_of(dx, dh), p])

    factor_steps = iter((
        lambda: (send_f(0, 0, (0, 1)), send_f(0, 0, (1, 0)), send_f(0, 0, (-1, 0))),
        lambda: (pair_f(0, 1), send_f(0, 1, (1, 0)), send_f(0, 1, (-1, 0))),
        lambda: (pair_f(1, 0), pair_f(-1, 0), send_f(-1, 0, (1, 0))),
        lambda: (pair_f(1, 1), send_f(1, 1, (-1, 0)), pair_f(-1, 1)),
        lambda: (pair_f(2, 0), pair_f(2, 1),
                 [arrived(f_rows(dx, dh, 1 - c), f_pair.at[day_of(dx, dh)]) for dx, dh in CHUNKS[1:]]),
    ))
    compute = itertools.chain(
        inverse_of_gram(fall, fall_t, gram, inverse),
        own_residuals(mine, fall, fall_t, inverse, loadings, mine_t),
        early_columns(lambda: fill(0), cols, fall, fall_t, inverse, mine_t, first_side, residuals),
    )
    for kind, a, *rest in ORDER:
        if kind == 0 and LINKS[a] == "root":
            root_sends(0, 0, *rest)
        elif kind == 0:
            send_m(0, 0, *rest, {"h": (0, 1), "x+": (1, 0), "x-": (-1, 0)}[LINKS[a]])
        elif kind == 1:
            relay_mine(*CHUNKS[a], *rest)
        elif kind == 2:
            relay_cols(*CHUNKS[a], *rest)
        elif kind == 3:
            next(factor_steps)()
        else:
            next(compute)
    fill(1)
    for _ in compute:
        pass

    for when, copy in pending:
        if when is None:
            copy.wait_send()
        else:
            pl.when(when)(copy.wait_send)
    for i in range(THIRDS):
        for third in range(THIRDS):
            @pl.when(among(TREES[third][i][1]))
            def _():
                for dx, dh in CHUNKS:
                    for p in range(third, PARTS, THIRDS):
                        to_chip(c_part(dx, dh, p, c), dx, dh, p, i).wait_send()
    for dx, dh in CHUNKS:
        for p in range(PARTS):
            to_sibling(c_part(dx, dh, p, c), dx, dh, p).wait_send()


def gather(factors, returns):
    dma = pltpu.SemaphoreType.DMA
    shape = jax.ShapeDtypeStruct
    return pl.pallas_call(
        gather_kernel,
        out_shape=(
            shape((DAYS, 2 * ASSET_BLOCK), jnp.bfloat16),
            shape((DAYS, FACTORS), jnp.bfloat16),
            shape((FACTORS, DAYS), jnp.bfloat16),
            shape((FACTORS, FACTORS), jnp.float32),
            shape((FACTORS, ASSET_BLOCK), jnp.float32),
            shape((ASSET_BLOCK, DAYS), jnp.bfloat16),
            shape((2, ASSET_BLOCK, SIDE_WIDTH[0]), jnp.float32),
        ),
        in_specs=[pl.BlockSpec(memory_space=pl.ANY)] * 2,
        out_specs=(pl.BlockSpec(memory_space=pltpu.VMEM),) * 7,
        scratch_shapes=[
            pltpu.VMEM((DAYS, ASSET_BLOCK), jnp.bfloat16),
            pltpu.VMEM((2, DAYS, SIDE_WIDTH[0]), jnp.bfloat16),
            pltpu.VMEM((FACTORS, FACTORS), jnp.float32),
            dma((2,)), dma((7,)), dma((8,)), dma((8,)), dma((10 * PARTS,)), dma((8, PARTS)),
            dma((8, PARTS, 3)), dma((8, PARTS)), dma((8, PARTS)), dma((8,)), dma((8, PARTS)),
        ],
        compiler_params=pltpu.CompilerParams(
            collective_id=0, has_side_effects=True, vmem_limit_bytes=36 * 2**20),
        name="gather",
    )(factors, returns)


def covariance_kernel(cols, fall, fall_t, inverse, loadings, mine_t, first_side, loadings_out, covariance, stage, sems):
    width = SIDE_WIDTH[1]
    copies = [pltpu.make_async_copy(loadings, loadings_out, sems.at[0])]
    for core in range(2):
        lanes = pl.ds(core * ASSET_BLOCK, SIDE_WIDTH[0])
        copies.append(pltpu.make_async_copy(first_side.at[core], covariance.at[:, lanes], sems.at[1 + core]))
    for copy in copies:
        copy.start()
    lanes = [pl.ds(core * ASSET_BLOCK + SIDE_AT[1], width) for core in range(2)]
    blocks = [cols[:, part] for part in lanes]
    groups = [(0,), (1,)] if width >= 512 else [(0, 1)]
    for group in groups:
        block = jnp.concatenate([blocks[core] for core in group], axis=1)
        _, residual = residual_of(block, fall, fall_t, inverse)
        for half in range(2):
            rows = pl.ds(half * ROWS, ROWS)
            product = jnp.dot(mine_t[rows, :], residual, preferred_element_type=jnp.float32) * (1.0 / DAYS)
            for i, core in enumerate(group):
                stage[core, rows, :] = product[:, i * width:(i + 1) * width]
                copy = pltpu.make_async_copy(
                    stage.at[core, rows], covariance.at[rows, lanes[core]], sems.at[3 + core * 2 + half])
                copy.start()
                copies.append(copy)
    for copy in copies:
        copy.wait()


def covariances(*args):
    return pl.pallas_call(
        covariance_kernel,
        out_shape=(
            jax.ShapeDtypeStruct((FACTORS, ASSET_BLOCK), jnp.float32),
            jax.ShapeDtypeStruct((ASSET_BLOCK, 2 * ASSET_BLOCK), jnp.float32),
        ),
        in_specs=[pl.BlockSpec(memory_space=pltpu.VMEM)] * len(args),
        out_specs=(pl.BlockSpec(memory_space=pltpu.HBM),) * 2,
        scratch_shapes=[pltpu.VMEM((2, ASSET_BLOCK, SIDE_WIDTH[1]), jnp.float32), pltpu.SemaphoreType.DMA((7,))],
        compiler_params=pltpu.CompilerParams(vmem_limit_bytes=24 * 2**20),
        name="covariances",
    )(*args)


def per_device(factors, returns):
    factors = pltpu.with_memory_space_constraint(factors, pltpu.HBM)
    returns = pltpu.with_memory_space_constraint(returns, pltpu.HBM)
    return covariances(*gather(factors, returns))


def solution(mesh):
    in_specs = (P("days", None), P("days", "assets"))
    out_specs = (P(None, "assets"), P("assets", "days"))
    return jax.shard_map(
        per_device, mesh=mesh, in_specs=in_specs, out_specs=out_specs, check_vma=False
    )
```

```python
import functools
import itertools

import jax
import jax.numpy as jnp
from jax import lax
from jax.experimental import pallas as pl
from jax.experimental.pallas import tpu as pltpu
from jax.sharding import PartitionSpec as P

MESH = pl.DeviceIdType.MESH
DAY_BLOCK = 192
DAYS = 8 * DAY_BLOCK
ASSET_BLOCK = 1024
FACTORS = 256
HALF = 96
THIRDS, SIDES = 3, 2
PARTS = THIRDS * SIDES
PART = DAY_BLOCK // THIRDS
SIDE_WIDTH = (512, 512)
SIDE_AT = (0, SIDE_WIDTH[0])
ROWS = 512
PIVOTS = 8

TREES = (
    (("z+", ((0, 0), (0, 1), (0, 2), (1, 2))), ("y", ((0, 1), (0, 2))), ("z-", ((1, 1),))),
    (("z-", ((0, 0), (0, 3), (0, 2), (1, 3), (1, 2))), ("y", ((0, 3),)), ("z+", ((1, 3),))),
    (("y", ((0, 0), (1, 1), (1, 2), (1, 3))), ("z+", ((1, 0), (1, 1))), ("z-", ((1, 0),))),
)
ROLES = ((0, 1), (0, 2), (0, 3), (1, 0), (1, 1), (1, 2), (1, 3))
CHUNKS = ((0, 0), (0, 1), (1, 0), (1, 1), (-1, 0), (-1, 1), (2, 0), (2, 1))

LINKS = ("h", "x+", "x-", "root")
ORDER = (
    (3, 0), (0, 0, 2), (0, 3, 4), (0, 3, 3), (0, 1, 2), (0, 3, 2), (0, 1, 3), (0, 2, 2),
    (0, 3, 1), (0, 2, 0), (0, 0, 0), (0, 1, 0), (2, 0, 3, 0), (0, 2, 4), (0, 1, 1), (2, 0, 2, 3),
    (0, 3, 0), (1, 4, 2), (0, 0, 3), (3, 1), (0, 2, 1), (0, 0, 4), (2, 0, 0, 0), (1, 1, 0),
    (0, 1, 4), (2, 0, 1, 2), (0, 0, 1), (2, 4, 2, 3), (0, 2, 5), (2, 0, 0, 1), (1, 2, 4), (3, 2),
    (0, 2, 3), (1, 4, 0), (1, 4, 1), (2, 0, 3, 1), (1, 2, 0), (3, 3), (2, 1, 0, 0), (2, 0, 2, 4),
    (1, 2, 1), (2, 0, 2, 6), (2, 0, 4, 2), (1, 2, 2), (2, 2, 4, 2), (0, 3, 5), (2, 1, 0, 1), (1, 4, 3),
    (2, 4, 0, 0), (0, 1, 5), (1, 3, 0), (1, 4, 4), (0, 0, 5), (1, 1, 2), (2, 2, 0, 0), (2, 4, 3, 0),
    (2, 2, 2, 3), (2, 2, 4, 1), (1, 5, 0), (2, 3, 0, 0), (2, 4, 2, 4), (2, 4, 0, 1), (2, 0, 0, 5), (2, 2, 1, 2),
    (1, 1, 1), (2, 4, 1, 2), (2, 0, 4, 6), (1, 1, 3), (1, 6, 0), (2, 0, 5, 3), (1, 2, 5), (3, 4),
    (1, 6, 1), (2, 0, 1, 6), (1, 6, 2), (2, 5, 0, 0), (2, 4, 0, 4), (4, 0), (2, 2, 1, 6), (2, 1, 1, 2),
    (2, 4, 2, 5), (2, 0, 5, 4), (2, 1, 2, 3), (2, 2, 1, 1), (2, 4, 4, 2), (1, 1, 4), (2, 0, 0, 4), (4, 1),
    (2, 6, 0, 0), (4, 2), (2, 4, 3, 1), (2, 0, 4, 5), (2, 2, 0, 4), (2, 2, 2, 4), (4, 3), (1, 1, 5),
    (4, 4), (1, 6, 3), (1, 3, 1), (2, 4, 3, 4), (2, 6, 1, 2), (2, 4, 0, 5), (2, 1, 3, 0), (2, 1, 2, 4),
    (2, 2, 5, 3), (2, 1, 0, 4), (2, 0, 4, 1), (2, 2, 0, 1), (1, 2, 3), (4, 5), (2, 0, 3, 5), (2, 6, 2, 3),
    (2, 1, 0, 5), (2, 1, 5, 3), (2, 2, 4, 6), (4, 6), (2, 1, 2, 6), (1, 3, 2), (1, 4, 5), (4, 7),
    (2, 0, 1, 1), (2, 1, 1, 6), (2, 3, 1, 2), (4, 8), (2, 0, 1, 5), (1, 6, 4), (2, 3, 0, 1), (2, 3, 2, 3),
    (2, 4, 2, 6), (2, 2, 4, 0), (4, 9), (2, 2, 5, 4), (2, 2, 1, 3), (2, 4, 3, 5), (4, 10), (2, 0, 1, 3),
    (2, 5, 0, 4), (2, 2, 1, 5), (2, 0, 2, 5), (2, 6, 0, 4), (2, 4, 1, 6), (4, 11), (2, 4, 5, 3), (2, 1, 4, 2),
    (1, 7, 0), (4, 12), (2, 2, 0, 5), (1, 5, 2), (2, 2, 3, 0), (2, 0, 4, 0), (2, 1, 2, 2), (2, 6, 0, 1),
    (2, 1, 1, 1), (2, 6, 2, 4), (4, 13), (1, 6, 5), (2, 0, 5, 5), (2, 6, 1, 6), (2, 4, 4, 6), (2, 2, 0, 2),
    (2, 4, 2, 0), (2, 6, 4, 2), (2, 2, 2, 5), (2, 1, 3, 1), (4, 14), (1, 5, 1), (2, 5, 2, 3), (4, 15),
    (2, 1, 5, 4), (1, 3, 3), (2, 7, 0, 0), (2, 2, 2, 6), (4, 16), (2, 3, 1, 6), (2, 2, 4, 5), (2, 5, 1, 2),
    (4, 17), (2, 3, 0, 4), (2, 3, 2, 4), (2, 5, 0, 1), (2, 6, 3, 0), (2, 0, 0, 6), (1, 7, 1), (1, 3, 4),
    (1, 5, 3), (2, 6, 5, 3), (2, 0, 5, 6), (4, 18), (4, 19), (2, 1, 4, 6), (2, 0, 2, 1), (2, 3, 1, 1),
    (4, 20), (2, 4, 2, 2), (1, 7, 2), (2, 4, 1, 3), (2, 4, 5, 4), (2, 3, 2, 6), (4, 21), (2, 3, 3, 0),
    (2, 6, 2, 6), (2, 7, 1, 2), (2, 7, 2, 3), (2, 7, 0, 4), (2, 6, 0, 5), (2, 2, 3, 1), (2, 0, 0, 3), (1, 5, 4),
    (2, 4, 4, 3), (2, 1, 1, 5), (2, 6, 0, 3), (1, 3, 5), (2, 5, 2, 4), (2, 2, 4, 4), (2, 2, 5, 5), (4, 22),
    (2, 2, 5, 6), (4, 23), (4, 24), (2, 1, 2, 5), (2, 2, 4, 3), (2, 5, 4, 2), (2, 0, 5, 0), (2, 3, 4, 2),
    (2, 7, 0, 1), (2, 4, 2, 1), (2, 4, 0, 3), (2, 6, 1, 1), (2, 3, 0, 5), (2, 1, 0, 3), (2, 5, 3, 0), (2, 5, 1, 1),
    (2, 0, 1, 0), (2, 4, 1, 5), (2, 6, 2, 5), (2, 3, 5, 3), (2, 6, 4, 6), (2, 2, 0, 6), (2, 6, 5, 4), (2, 5, 1, 6),
    (2, 1, 3, 2), (2, 2, 1, 4), (4, 25), (2, 4, 3, 3), (4, 26), (4, 27), (2, 0, 4, 3), (2, 1, 1, 0),
    (2, 4, 4, 1), (2, 6, 0, 6), (2, 3, 2, 0), (4, 28), (1, 5, 5), (2, 3, 0, 3), (2, 1, 5, 5), (2, 3, 1, 5),
    (2, 3, 3, 1), (2, 7, 2, 4), (2, 2, 3, 2), (2, 6, 1, 5), (4, 29), (2, 6, 3, 4), (2, 3, 0, 2), (2, 5, 3, 1),
    (2, 3, 3, 4), (2, 1, 3, 5), (2, 1, 1, 4), (2, 7, 1, 1), (2, 5, 5, 3), (2, 5, 0, 5), (2, 4, 1, 1), (2, 1, 4, 3),
    (1, 7, 4), (2, 0, 4, 4), (2, 7, 4, 2), (2, 7, 1, 6), (1, 7, 3), (4, 30), (2, 6, 3, 1), (2, 2, 3, 5),
    (2, 7, 3, 0), (2, 1, 5, 6), (2, 5, 0, 3), (2, 1, 4, 1), (4, 31), (2, 5, 0, 2), (2, 1, 1, 3), (2, 6, 1, 0),
    (2, 4, 4, 5), (2, 0, 5, 1), (4, 32), (4, 33), (4, 34), (2, 6, 2, 1), (2, 6, 1, 3), (2, 2, 2, 1),
    (2, 5, 1, 3), (2, 3, 5, 4), (2, 7, 2, 6), (4, 35), (2, 5, 4, 1), (2, 7, 5, 3), (2, 0, 3, 4), (2, 5, 2, 6),
    (4, 36), (2, 1, 5, 1), (2, 3, 2, 5), (2, 5, 2, 5), (2, 0, 2, 0), (2, 4, 1, 4), (2, 5, 4, 6), (4, 37),
    (1, 7, 5), (4, 38), (2, 5, 5, 4), (2, 5, 1, 5), (2, 7, 0, 5), (2, 4, 5, 0), (2, 5, 3, 4), (2, 0, 3, 6),
    (2, 7, 3, 1), (2, 6, 4, 3), (2, 3, 4, 6), (2, 4, 0, 2), (4, 39), (4, 40), (2, 1, 5, 2), (2, 7, 2, 0),
    (2, 0, 1, 4), (2, 5, 5, 6), (2, 1, 3, 4), (2, 2, 2, 0), (2, 7, 0, 2), (2, 7, 3, 4), (2, 3, 4, 1), (2, 4, 4, 0),
    (4, 41), (2, 7, 2, 5), (2, 1, 5, 0), (2, 7, 1, 0), (2, 2, 2, 2), (2, 4, 5, 6), (2, 5, 0, 6), (2, 7, 1, 5),
    (4, 42), (2, 3, 1, 0), (2, 3, 3, 3), (2, 6, 5, 5), (2, 0, 2, 2), (4, 43), (2, 6, 4, 5), (2, 7, 5, 4),
    (4, 44), (4, 45), (2, 5, 1, 0), (2, 3, 2, 2), (2, 0, 3, 3), (2, 3, 5, 6), (2, 5, 2, 0), (2, 7, 4, 1),
    (2, 6, 4, 1), (2, 0, 0, 2), (2, 7, 4, 6), (2, 1, 2, 1), (2, 7, 2, 2), (2, 6, 2, 2), (2, 7, 1, 4), (2, 4, 3, 6),
    (2, 2, 0, 3), (2, 5, 1, 4), (2, 3, 1, 4), (2, 6, 3, 2), (2, 5, 4, 3), (2, 5, 3, 5), (2, 7, 5, 6), (2, 0, 3, 2),
    (2, 6, 3, 3), (2, 6, 5, 6), (2, 5, 2, 1), (2, 1, 2, 0), (2, 2, 3, 4), (2, 7, 2, 1), (2, 2, 1, 0), (2, 4, 1, 0),
    (2, 7, 0, 3), (2, 1, 4, 5), (2, 7, 0, 6), (2, 6, 1, 4), (2, 3, 1, 3), (2, 3, 2, 1), (2, 3, 3, 5), (2, 6, 0, 2),
    (2, 1, 0, 2), (2, 5, 2, 2), (2, 1, 0, 6), (2, 6, 2, 0), (2, 3, 3, 2), (2, 3, 0, 6), (2, 4, 4, 4), (2, 7, 1, 3),
    (2, 6, 3, 5), (2, 2, 5, 0), (2, 3, 4, 3), (2, 4, 0, 6), (4, 46), (2, 4, 5, 5), (4, 47), (4, 48),
    (4, 49), (4, 50), (2, 2, 5, 2), (2, 6, 4, 4), (2, 3, 5, 5), (2, 3, 4, 5), (2, 6, 5, 1), (4, 51),
    (2, 5, 5, 5), (2, 5, 4, 5), (2, 5, 3, 3), (4, 52), (2, 7, 3, 5), (4, 53), (2, 7, 5, 5), (2, 7, 4, 5),
    (2, 2, 5, 1), (2, 7, 3, 2), (2, 6, 5, 0), (4, 54), (4, 55), (2, 7, 3, 3), (2, 3, 4, 0), (2, 5, 3, 6),
    (2, 4, 3, 2), (2, 5, 5, 2), (2, 6, 3, 6), (2, 3, 4, 4), (2, 4, 5, 2), (2, 0, 5, 2), (2, 1, 4, 4), (2, 5, 4, 4),
    (2, 2, 3, 3), (2, 7, 5, 2), (2, 5, 5, 1), (2, 3, 5, 0), (2, 2, 3, 6), (2, 6, 4, 0), (2, 7, 4, 4), (2, 3, 3, 6),
    (2, 1, 3, 3), (2, 1, 3, 6), (2, 7, 4, 0), (2, 7, 4, 3), (2, 5, 3, 2), (2, 7, 3, 6), (2, 4, 5, 1), (2, 3, 5, 1),
    (2, 5, 4, 0), (2, 3, 5, 2), (2, 6, 5, 2), (2, 7, 5, 1), (2, 5, 5, 0), (2, 7, 5, 0), (2, 1, 4, 0),
)


def forward_right(dh, p):
    return p % THIRDS < (THIRDS + 1 - dh) // 2


def with_row(a, k, row):
    n = a.shape[1]
    g = k // 8 * 8
    sub = lax.broadcasted_iota(jnp.int32, (8, n), 0)
    middle = jnp.where(sub == k - g, jnp.broadcast_to(row, (8, n)), a[g:g + 8])
    return jnp.concatenate([part for part in (a[:g], middle, a[g + 8:]) if part.shape[0]], axis=0)


def invert(a):
    n = a.shape[0]
    lane = lax.broadcasted_iota(jnp.int32, (n, n), 1)
    lane_one = lax.broadcasted_iota(jnp.int32, (1, n), 1)
    for start in range(0, n, PIVOTS):
        spread = [jnp.broadcast_to(a[:, k:k + 1], (n, n)) for k in range(start, start + PIVOTS)]
        for j in range(PIVOTS):
            k = start + j
            col = spread[j]
            scale = 1.0 / col[k:k + 1, :]
            row = jnp.where(lane_one == k, scale, a[k:k + 1, :] * scale)
            a = with_row(jnp.where(lane == k, 0.0, a) - col * row, k, row)
            for i in range(j + 1, PIVOTS):
                row = spread[i][k:k + 1, :] * scale
                spread[i] = with_row(spread[i] - col * row, k, row)
        yield None
    yield a


def exact_dot(a, b):
    return jnp.dot(a, b, precision=lax.Precision.HIGHEST, preferred_element_type=jnp.float32)


def inverse_of_gram(fall, fall_t, gram, inverse):
    fall_t[...] = fall[...].T
    yield
    gram[...] = jnp.dot(fall_t[...], fall[...], preferred_element_type=jnp.float32)
    yield
    n = FACTORS // 2
    first = None
    for first in invert(gram[:n, :n]):
        yield
    upper, lower = gram[:n, n:], gram[n:, :n]
    right, left = exact_dot(first, upper), exact_dot(lower, first)
    schur = gram[n:, n:] - exact_dot(lower, right)
    yield
    second = None
    for second in invert(schur):
        yield
    off = -exact_dot(right, second)
    inverse[:n, :n] = first - exact_dot(off, left)
    inverse[:n, n:] = off
    inverse[n:, :n] = -exact_dot(second, left)
    inverse[n:, n:] = second
    yield


def residual_steps(block, fall, fall_t, inverse):
    cross = jnp.dot(fall_t[...], block, preferred_element_type=jnp.float32)
    yield
    exposure = exact_dot(inverse[...], cross)
    yield
    fitted = jnp.dot(fall[...], exposure.astype(jnp.bfloat16), preferred_element_type=jnp.float32)
    return exposure, (block.astype(jnp.float32) - fitted).astype(jnp.bfloat16)


def residual_of(*args):
    steps = residual_steps(*args)
    while True:
        try:
            next(steps)
        except StopIteration as done:
            return done.value


def own_residuals(mine, fall, fall_t, inverse, loadings, mine_t):
    for side in range(SIDES):
        part = pl.ds(SIDE_AT[side], SIDE_WIDTH[side])
        exposure, residual = yield from residual_steps(mine[:, part], fall, fall_t, inverse)
        loadings[:, part] = exposure
        yield
        mine_t[part, :] = residual.T
        yield


def early_columns(prepare, cols, fall, fall_t, inverse, mine_t, first_side, residuals):
    for core in range(2):
        if core == 0:
            prepare()
        part = pl.ds(core * ASSET_BLOCK, SIDE_WIDTH[0])
        _, residuals[core] = yield from residual_steps(cols[:, part], fall, fall_t, inverse)
        yield
    for core in range(2):
        for block in range(2):
            rows = pl.ds(block * ROWS, ROWS)
            first_side[core, rows, :] = jnp.dot(
                mine_t[rows, :], residuals[core], preferred_element_type=jnp.float32) * (1.0 / DAYS)
            yield


def gather_kernel(f_hbm, x_hbm, cols, fall, fall_t, inverse, loadings, mine_t, first_side,
                  mine, residuals, gram, load_sem, f_send, f_recv, f_pair,
                  m_send, m_recv, c_send, c_recv, c_pair, fp_send, cp_send):
    day, asset = lax.axis_index("days"), lax.axis_index("assets")
    x, h = day // 2, day % 2
    z, l, c = asset // 4, (asset // 2) % 2, asset % 2
    dl, dz = (l + h) % 2, (z - x + 4) % 4
    is_root = jnp.logical_and(dl == 0, dz == 0)
    right_is_root = jnp.logical_and(dl == 0, dz == 1)
    left_is_root = jnp.logical_and(dl == 0, dz == 3)
    partner_is_root = jnp.logical_and(dl == 1, dz == 0)

    def among(roles):
        return functools.reduce(jnp.logical_or, [jnp.logical_and(dl == i, dz == j) for i, j in roles])

    def day_of(dx, dh):
        return lax.rem(x + dx + 4, 4) * 2 + lax.rem(h + dh, 2)

    def asset_of(link):
        if link == "z+":
            return lax.rem(z + 1, 4) * 4 + l * 2 + c
        if link == "z-":
            return lax.rem(z + 3, 4) * 4 + l * 2 + c
        return z * 4 + (1 - l) * 2 + c

    sibling = z * 4 + l * 2 + 1 - c
    own_rows = pl.ds(pl.multiple_of(day * DAY_BLOCK, DAY_BLOCK), DAY_BLOCK)
    load_x = pltpu.make_async_copy(x_hbm, mine.at[own_rows], load_sem.at[0])
    load_f = pltpu.make_async_copy(f_hbm, fall.at[own_rows], load_sem.at[1])
    load_f.start()
    load_x.start()

    barrier = pltpu.get_barrier_semaphore()
    greeted = [(day_of(0, 1), asset), (day_of(1, 0), asset), (day_of(-1, 0), asset)]
    greeted += [(day, asset_of("z+")), (day, asset_of("z-")), (day, asset_of("y")), (day, sibling)]
    for d, a in greeted:
        pl.semaphore_signal(barrier, inc=1, device_id={"days": d, "assets": a}, device_id_type=MESH)
    pl.semaphore_wait(barrier, len(greeted))
    load_f.wait()
    load_x.wait()

    pending = []

    def send(src, dst, ssem, rsem, d, a, when=None):
        copy = pltpu.make_async_remote_copy(
            src_ref=src, dst_ref=dst, send_sem=ssem, recv_sem=rsem,
            device_id={"days": d, "assets": a}, device_id_type=MESH)
        if when is None:
            copy.start()
        else:
            pl.when(when)(copy.start)
        pending.append((when, copy))

    def arrived(ref, rsem):
        pltpu.make_async_remote_copy(
            src_ref=ref, dst_ref=ref, send_sem=load_sem.at[0], recv_sem=rsem,
            device_id={"days": day, "assets": sibling}, device_id_type=MESH).wait_recv()

    def f_rows(dx, dh, core):
        return fall.at[pl.ds(pl.multiple_of(day_of(dx, dh) * DAY_BLOCK + core * HALF, 32), HALF)]

    def part_rows(dx, dh, p):
        return pl.ds(pl.multiple_of(day_of(dx, dh) * DAY_BLOCK + p % THIRDS * PART, PART), PART)

    def m_part(dx, dh, p):
        return mine.at[part_rows(dx, dh, p), pl.ds(SIDE_AT[p // THIRDS], SIDE_WIDTH[p // THIRDS])]

    def c_part(dx, dh, p, core):
        side = p // THIRDS
        lanes = pl.ds(pl.multiple_of(core * ASSET_BLOCK + SIDE_AT[side], 128), SIDE_WIDTH[side])
        return cols.at[part_rows(dx, dh, p), lanes]

    n_f, n_m = [0], [0]

    def send_f(dx, dh, to):
        ref = f_rows(dx, dh, c)
        send(ref, ref, f_send.at[n_f[0]], f_recv.at[day_of(dx, dh)], day_of(*to), asset)
        n_f[0] += 1

    def send_m(dx, dh, p, to, when=None):
        ref = m_part(dx, dh, p)
        send(ref, ref, m_send.at[n_m[0]], m_recv.at[day_of(dx, dh), p], day_of(*to), asset, when)
        n_m[0] += 1

    def pair_f(dx, dh):
        ref = f_rows(dx, dh, c)
        arrived(ref, f_recv.at[day_of(dx, dh)])
        send(ref, ref, fp_send.at[day_of(dx, dh)], f_pair.at[day_of(dx, dh)], day, sibling)

    def relayed(src, dst, ssem, rsem, a):
        return pltpu.make_async_remote_copy(
            src_ref=src, dst_ref=dst, send_sem=ssem, recv_sem=rsem,
            device_id={"days": day, "assets": a}, device_id_type=MESH)

    def to_chip(src, dx, dh, p, i):
        k = day_of(dx, dh)
        link = TREES[p % THIRDS][i][0]
        return relayed(src, c_part(dx, dh, p, c), c_send.at[k, p, i], c_recv.at[k, p], asset_of(link))

    def to_sibling(src, dx, dh, p):
        k = day_of(dx, dh)
        return relayed(src, c_part(dx, dh, p, c), cp_send.at[k, p], c_pair.at[k, p], sibling)

    def root_sends(dx, dh, p):
        @pl.when(is_root)
        def _():
            to_chip(m_part(dx, dh, p), dx, dh, p, 0).start()
            to_sibling(m_part(dx, dh, p), dx, dh, p).start()

    def relay_mine(dx, dh, p):
        arrived(m_part(dx, dh, p), m_recv.at[day_of(dx, dh), p])
        right, left = (None, None) if dh == 0 else (jnp.logical_not(right_is_root), jnp.logical_not(left_is_root))
        if (dx, dh) == (0, 1):
            send_m(dx, dh, p, (1, 0))
            send_m(dx, dh, p, (-1, 0))
        if dx == -1 and forward_right(dh, p):
            send_m(dx, dh, p, (1, 0), right)
        if dx == 1 and not forward_right(dh, p):
            send_m(dx, dh, p, (-1, 0), left)
        if (dx, dh) == (2, 0):
            send_m(dx, dh, p, (0, 1), partner_is_root)
        root_sends(dx, dh, p)

    def relay_cols(dx, dh, p, role):
        @pl.when(among((ROLES[role],)))
        def _():
            ref = c_part(dx, dh, p, c)
            arrived(ref, c_recv.at[day_of(dx, dh), p])
            for i, (_, roles) in enumerate(TREES[p % THIRDS]):
                if ROLES[role] in roles:
                    to_chip(ref, dx, dh, p, i).start()
            to_sibling(ref, dx, dh, p).start()

    def fill(side):
        @pl.when(is_root)
        def _():
            at, width = SIDE_AT[side], SIDE_WIDTH[side]
            lanes = pl.ds(pl.multiple_of(c * ASSET_BLOCK + at, 128), width)

            @pl.loop(0, DAYS // 64)
            def _(i):
                rows = pl.ds(pl.multiple_of(i * 64, 64), 64)
                cols[rows, lanes] = mine[rows, pl.ds(at, width)]

        for dx, dh in CHUNKS:
            for p in range(side * THIRDS, (side + 1) * THIRDS):
                arrived(c_part(dx, dh, p, 1 - c), c_pair.at[day_of(dx, dh), p])

    factor_steps = iter((
        lambda: (send_f(0, 0, (0, 1)), send_f(0, 0, (1, 0)), send_f(0, 0, (-1, 0))),
        lambda: (pair_f(0, 1), send_f(0, 1, (1, 0)), send_f(0, 1, (-1, 0))),
        lambda: (pair_f(1, 0), pair_f(-1, 0), send_f(-1, 0, (1, 0))),
        lambda: (pair_f(1, 1), send_f(1, 1, (-1, 0)), pair_f(-1, 1)),
        lambda: (pair_f(2, 0), pair_f(2, 1),
                 [arrived(f_rows(dx, dh, 1 - c), f_pair.at[day_of(dx, dh)]) for dx, dh in CHUNKS[1:]]),
    ))
    compute = itertools.chain(
        inverse_of_gram(fall, fall_t, gram, inverse),
        own_residuals(mine, fall, fall_t, inverse, loadings, mine_t),
        early_columns(lambda: fill(0), cols, fall, fall_t, inverse, mine_t, first_side, residuals),
    )
    for kind, a, *rest in ORDER:
        if kind == 0 and LINKS[a] == "root":
            root_sends(0, 0, *rest)
        elif kind == 0:
            send_m(0, 0, *rest, {"h": (0, 1), "x+": (1, 0), "x-": (-1, 0)}[LINKS[a]])
        elif kind == 1:
            relay_mine(*CHUNKS[a], *rest)
        elif kind == 2:
            relay_cols(*CHUNKS[a], *rest)
        elif kind == 3:
            next(factor_steps)()
        else:
            next(compute)
    fill(1)
    for _ in compute:
        pass

    for when, copy in pending:
        if when is None:
            copy.wait_send()
        else:
            pl.when(when)(copy.wait_send)
    for i in range(THIRDS):
        for third in range(THIRDS):
            @pl.when(among(TREES[third][i][1]))
            def _():
                for dx, dh in CHUNKS:
                    for p in range(third, PARTS, THIRDS):
                        to_chip(c_part(dx, dh, p, c), dx, dh, p, i).wait_send()
    for dx, dh in CHUNKS:
        for p in range(PARTS):
            to_sibling(c_part(dx, dh, p, c), dx, dh, p).wait_send()


def gather(factors, returns):
    dma = pltpu.SemaphoreType.DMA
    shape = jax.ShapeDtypeStruct
    return pl.pallas_call(
        gather_kernel,
        out_shape=(
            shape((DAYS, 2 * ASSET_BLOCK), jnp.bfloat16),
            shape((DAYS, FACTORS), jnp.bfloat16),
            shape((FACTORS, DAYS), jnp.bfloat16),
            shape((FACTORS, FACTORS), jnp.float32),
            shape((FACTORS, ASSET_BLOCK), jnp.float32),
            shape((ASSET_BLOCK, DAYS), jnp.bfloat16),
            shape((2, ASSET_BLOCK, SIDE_WIDTH[0]), jnp.float32),
        ),
        in_specs=[pl.BlockSpec(memory_space=pl.ANY)] * 2,
        out_specs=(pl.BlockSpec(memory_space=pltpu.VMEM),) * 7,
        scratch_shapes=[
            pltpu.VMEM((DAYS, ASSET_BLOCK), jnp.bfloat16),
            pltpu.VMEM((2, DAYS, SIDE_WIDTH[0]), jnp.bfloat16),
            pltpu.VMEM((FACTORS, FACTORS), jnp.float32),
            dma((2,)), dma((7,)), dma((8,)), dma((8,)), dma((10 * PARTS,)), dma((8, PARTS)),
            dma((8, PARTS, 3)), dma((8, PARTS)), dma((8, PARTS)), dma((8,)), dma((8, PARTS)),
        ],
        compiler_params=pltpu.CompilerParams(
            collective_id=0, has_side_effects=True, vmem_limit_bytes=36 * 2**20),
        name="gather",
    )(factors, returns)


def covariance_kernel(cols, fall, fall_t, inverse, loadings, mine_t, first_side, loadings_out, covariance, stage, sems):
    width = SIDE_WIDTH[1]
    copies = [pltpu.make_async_copy(loadings, loadings_out, sems.at[0])]
    for core in range(2):
        lanes = pl.ds(core * ASSET_BLOCK, SIDE_WIDTH[0])
        copies.append(pltpu.make_async_copy(first_side.at[core], covariance.at[:, lanes], sems.at[1 + core]))
    for copy in copies:
        copy.start()
    lanes = [pl.ds(core * ASSET_BLOCK + SIDE_AT[1], width) for core in range(2)]
    blocks = [cols[:, part] for part in lanes]
    groups = [(0,), (1,)] if width >= 512 else [(0, 1)]
    for group in groups:
        block = jnp.concatenate([blocks[core] for core in group], axis=1)
        _, residual = residual_of(block, fall, fall_t, inverse)
        for half in range(2):
            rows = pl.ds(half * ROWS, ROWS)
            product = jnp.dot(mine_t[rows, :], residual, preferred_element_type=jnp.float32) * (1.0 / DAYS)
            for i, core in enumerate(group):
                stage[core, rows, :] = product[:, i * width:(i + 1) * width]
                copy = pltpu.make_async_copy(
                    stage.at[core, rows], covariance.at[rows, lanes[core]], sems.at[3 + core * 2 + half])
                copy.start()
                copies.append(copy)
    for copy in copies:
        copy.wait()


def covariances(*args):
    return pl.pallas_call(
        covariance_kernel,
        out_shape=(
            jax.ShapeDtypeStruct((FACTORS, ASSET_BLOCK), jnp.float32),
            jax.ShapeDtypeStruct((ASSET_BLOCK, 2 * ASSET_BLOCK), jnp.float32),
        ),
        in_specs=[pl.BlockSpec(memory_space=pltpu.VMEM)] * len(args),
        out_specs=(pl.BlockSpec(memory_space=pltpu.HBM),) * 2,
        scratch_shapes=[pltpu.VMEM((2, ASSET_BLOCK, SIDE_WIDTH[1]), jnp.float32), pltpu.SemaphoreType.DMA((7,))],
        compiler_params=pltpu.CompilerParams(vmem_limit_bytes=24 * 2**20),
        name="covariances",
    )(*args)


def per_device(factors, returns):
    factors = pltpu.with_memory_space_constraint(factors, pltpu.HBM)
    returns = pltpu.with_memory_space_constraint(returns, pltpu.HBM)
    return covariances(*gather(factors, returns))


def solution(mesh):
    in_specs = (P("days", None), P("days", "assets"))
    out_specs = (P(None, "assets"), P("assets", "days"))
    return jax.shard_map(
        per_device, mesh=mesh, in_specs=in_specs, out_specs=out_specs, check_vma=False
    )
```
